128 devices in a mesh: band: 8 (over y, core), pgroup: 16 (over z, x).
Axes of the slice: x: 4, y: 4, z: 4, core: 2. Of those that a mesh axis runs over, the one named last changes fastest.
Arguments:
- state: float32 [256, 512, 512], P('pgroup', 'band'), may hold values from -6 to 6
- forcing: float32 [512, 512], P('band'), may hold values from -3 to 3
- parents: int32 [128, 256], P('band'), may hold values from 0 to 255, as said below
- taper_index: int32 [512], P('band'), may hold values from 0 to 7
Outputs:
- analysis: float32 [256, 512, 512], P('pgroup', 'band')
The draws below stay inside these ranges and needn't reach their ends.
Inputs may be any that keep to these rules, and one draw needn't show every extreme that they name: In every patch, the parents of the 16 particles k with k // 16 = g are distinct and come from exactly 8 groups (a group holds the particles j with the same j // 16), exactly 2 from each of them, for every patch and every g.
All inputs are finite; a program needn't handle non-finite values.
Results may differ from the reference program's by a relative error of at most 0.000071.
Values sent between devices are 32-bit elements; how exact they have to be, the bound alone decides.
No kernel may reach another device: no remote copies, remote signals or barrier semaphores. Data moves between devices by JAX's collectives and lax.ppermute only.
A program may use at most 64 MiB of HBM per device.

```python
import jax
import jax.numpy as jnp
from jax import lax

NX = 512
PART_DEV = 16
PATCH_ROWS = 4
STEPS = 6
CAP = 2
NY = 512
PARTICLES = 256
PATCHES = 128


def draw_parents(key, part):
    groups = PARTICLES // PART_DEV
    sources = PART_DEV // CAP
    pairs = PATCHES * groups
    key_src, key_loc, key_mix = jax.random.split(key, 3)
    chosen_src = jax.vmap(lambda k: jax.random.permutation(k, groups))(jax.random.split(key_src, pairs))[:, :sources]
    chosen_loc = jax.vmap(lambda k: jax.random.permutation(k, PART_DEV))(jax.random.split(key_loc, pairs * sources)).reshape(pairs, sources, PART_DEV)
    slot = jnp.arange(PART_DEV, dtype=jnp.int32)
    position = slot // CAP
    order = slot % CAP
    owner = chosen_src[:, position]
    within = chosen_loc[:, position, order]
    parent = owner * PART_DEV + within
    shuffle = jax.vmap(lambda k: jax.random.permutation(k, PART_DEV))(jax.random.split(key_mix, pairs))
    parent = jnp.take_along_axis(parent, shuffle, axis=1)
    return parent.reshape(PATCHES, groups * PART_DEV).astype(jnp.int32)


def touch_ends(entries, rng, least, top_value):
    longest = entries.shape.index(max(entries.shape))
    spots = []
    for shift in (0, 1):
        where = [jax.random.randint(jax.random.fold_in(rng, axis), (), 0, length) for axis, length in enumerate(entries.shape)]
        where[longest] = (where[longest] + shift) % entries.shape[longest]
        spots.append(tuple(where))
    return entries.at[spots[0]].set(least).at[spots[1]].set(top_value)


def block_scale(rng, extent, pieces, least, high):
    level, own = 1.0, jax.random.fold_in(rng, 6)
    for dim, blocks in pieces:
        heights = jnp.exp(jax.random.uniform(jax.random.fold_in(own, dim), (blocks,), jnp.float32, least / len(pieces), high / len(pieces)))
        level = level * jnp.repeat(heights, extent[dim] // blocks).reshape([-1 if axis == dim else 1 for axis in range(len(extent))])
    return level


def normal_values(own_key, shape, deviation, reach, cuts=(), kind=jnp.bfloat16):
    drawn = deviation * jax.random.normal(own_key, shape, jnp.float32)
    if cuts:
        drawn = drawn * block_scale(own_key, shape, cuts, -0.22, 0.18)
    return jnp.clip(drawn, -reach, reach).astype(kind)


def setup_inputs(seed: int = 0) -> dict:
    arg_keys = jax.random.split(jax.random.key(seed), 5)
    state = normal_values(arg_keys[0], (PARTICLES, NY, NX), 1.0, 6.0, ((0, 16), (1, 8)), jnp.float32)
    forcing = normal_values(arg_keys[1], (NY, NX), 0.3, 3.0, ((0, 8),), jnp.float32)
    parents = draw_parents(jax.random.fold_in(arg_keys[4], 71), 0)
    taper_index = touch_ends(jax.random.randint(arg_keys[3], (NY,), 0, 8), jax.random.fold_in(arg_keys[3], 1), 0, 7).astype(jnp.int32)
    return {"state": state, "forcing": forcing, "parents": parents, "taper_index": taper_index}


advect_x = 0.05
advect_y = 0.1
diffuse = 0.15
taper_kinds = 8


def advect(padded, drive):
    center = padded[:, 1:-1]
    north = padded[:, 2:]
    south = padded[:, :-2]
    east = jnp.roll(center, -1, axis=2)
    west = jnp.roll(center, 1, axis=2)
    return center - advect_x * center * (east - west) - advect_y * (north - south) + diffuse * (east + west + north + south - 4.0 * center) + drive[None]


def taper_weights(taper_rows):
    offsets = jnp.arange(5, dtype=jnp.float32) - 2.0
    rates = 0.2 * (jnp.arange(taper_kinds, dtype=jnp.float32) + 1.0)
    raw_table = jnp.exp(-rates[:, None] * offsets[None, :] * offsets[None, :])
    table = raw_table / jnp.sum(raw_table, axis=1, keepdims=True)
    onehot = (taper_rows[:, None] == jnp.arange(taper_kinds, dtype=jnp.int32)[None, :]).astype(jnp.float32)
    return jnp.dot(onehot, table, precision=lax.Precision.HIGHEST)


def blend(padded, weights):
    rows = weights.shape[0]
    total = weights[:, 0][None, :, None] * padded[:, 0:rows]
    for offset in range(1, 5):
        total = total + weights[:, offset][None, :, None] * padded[:, offset:offset + rows]
    return total


def reference(state, forcing, parents, taper_index):
    field = state
    for repeat in range(STEPS):
        field = advect(jnp.pad(field, ((0, 0), (1, 1), (0, 0))), forcing)
    blocks = field.reshape(PARTICLES, PATCHES, PATCH_ROWS * NX)
    picked = blocks[parents.T, jnp.arange(PATCHES, dtype=jnp.int32)[None, :]]
    field = picked.reshape(PARTICLES, NY, NX)
    field = blend(jnp.pad(field, ((0, 0), (2, 2), (0, 0))), taper_weights(taper_index))
    for repeat in range(STEPS):
        field = advect(jnp.pad(field, ((0, 0), (1, 1), (0, 0))), forcing)
    return field
```

```python
import functools

import jax
import jax.numpy as jnp
from jax import lax
from jax.experimental import pallas as pl
from jax.experimental.pallas import tpu as pltpu
from jax.sharding import PartitionSpec as P

PATCH_ROWS = 4
STEPS = 6
CAP = 2
TILE = 8
SCALE = 0.05


def _sub(shape):
    return lax.broadcasted_iota(jnp.int32, shape, 0)


def _up(tiles, i, k):
    here = tiles[i]
    after = tiles[min(i + 1, len(tiles) - 1)]
    return pltpu.roll(jnp.where(_sub(here.shape) < k, after, here), TILE - k, 0)


def _down(tiles, i, k):
    here = tiles[i]
    before = tiles[max(i - 1, 0)]
    return pltpu.roll(jnp.where(_sub(here.shape) >= TILE - k, before, here), k, 0)


def _step(tiles, i, drive):
    m = tiles[i]
    width = m.shape[1]
    e = pltpu.roll(m, width - 1, 1)
    w = pltpu.roll(m, 1, 1)
    n = _up(tiles, i, 1)
    s = _down(tiles, i, 1)
    return (m * (0.4 - (e - w)) + 0.15 * (e + w)) + (0.05 * n + 0.25 * s) + drive


def _steps(tiles, drive, keep, outer, mask):
    for repeat in range(STEPS):
        todo = keep if repeat == STEPS - 1 else range(len(tiles))
        fresh = list(tiles)
        for i in todo:
            fresh[i] = _step(tiles, i, drive(i))
            if i == outer:
                fresh[i] = fresh[i] * mask
        tiles = fresh
    return [tiles[i] for i in keep]


def _blend(tiles, weights, outer, mask):
    fresh = []
    for i in range(len(tiles)):
        w0, w1, w2 = weights(i)
        total = w0 * tiles[i]
        total = total + w1 * (_up(tiles, i, 1) + _down(tiles, i, 1))
        total = total + w2 * (_up(tiles, i, 2) + _down(tiles, i, 2))
        if i == outer:
            total = total * mask
        fresh.append(total)
    return fresh


def _taper(kind, width):
    rate = 0.2 * (kind + 1.0)
    near = jnp.exp(-rate)
    far = jnp.exp(-4.0 * rate)
    inv = 1.0 / (far + near + 1.0 + near + far)
    rep = width // kind.shape[1]
    return [jnp.concatenate([v] * rep, axis=1) for v in (inv, near * inv, far * inv)]


def _halves(a, b):
    return jnp.where(_sub(a.shape) < PATCH_ROWS, a, b)


def _inner_kernel(table, state, drive, out, field, scaled, *, per, batch, ncomp, gpack, groups):
    i = pl.program_id(0)
    tiles = state.shape[1]

    @pl.when(i == 0)
    def _():
        scaled[...] = drive[...] * SCALE

    @pl.when(i < ncomp)
    def _():
        def body(k, carry):
            cur = [state[k, t] * SCALE for t in range(tiles)]
            res = _steps(cur, lambda t: scaled[t], range(1, tiles - 1), -1, None)
            for t, v in enumerate(res):
                field[i * batch + k, t] = v
            return carry

        lax.fori_loop(0, batch, body, 0)

    @pl.when(i >= ncomp)
    def _():
        def body(k, carry):
            g = (i - ncomp) * gpack + k
            for slot in range(CAP):
                for q in range(tiles - 2):
                    first = table[((2 * q + 2) * groups + g) * CAP + slot]
                    second = table[((2 * q + 3) * groups + g) * CAP + slot]
                    out[k, slot, q] = _halves(field[first, q], field[second, q])
            return carry

        lax.fori_loop(0, gpack, body, 0)


def _edge_kernel(table, mask, low_in, high_in, low, high, drive, drive_low, drive_high, out, field,
                 scaled, *, batch, ncomp, gpack, groups, last):
    i = pl.program_id(0)

    @pl.when(i == 0)
    def _():
        scaled[0, 0] = drive_low[0] * SCALE
        scaled[0, 1] = drive[0] * SCALE
        scaled[0, 2] = drive[1] * SCALE
        scaled[1, 0] = drive[last - 1] * SCALE
        scaled[1, 1] = drive[last] * SCALE
        scaled[1, 2] = drive_high[0] * SCALE

    @pl.when(i < ncomp)
    def _():
        def body(k, carry):
            cur = [low[k] * SCALE, low_in[k, 0] * SCALE, low_in[k, 1] * SCALE]
            res = _steps(cur, lambda t: scaled[0, t], [1], 0, mask[0])
            field[i * batch + k, 0] = res[0]
            cur = [high_in[k, 0] * SCALE, high_in[k, 1] * SCALE, high[k] * SCALE]
            res = _steps(cur, lambda t: scaled[1, t], [1], 2, mask[1])
            field[i * batch + k, 1] = res[0]
            return carry

        lax.fori_loop(0, batch, body, 0)

    @pl.when(i >= ncomp)
    def _():
        def body(k, carry):
            g = (i - ncomp) * gpack + k
            for slot in range(CAP):
                for q in range(2):
                    base = 2 * last * q
                    first = table[(base * groups + g) * CAP + slot]
                    second = table[((base + 1) * groups + g) * CAP + slot]
                    out[k, slot, q] = _halves(field[first, q], field[second, q])
            return carry

        lax.fori_loop(0, gpack, body, 0)


def _pick_kernel(table, incoming, first, final, *, per, last):
    def body(j, carry):
        first[j] = _halves(incoming[table[j], 0], incoming[table[per + j], 0])
        base = 2 * last * per
        final[j] = _halves(incoming[table[base + j], 1], incoming[table[base + per + j], 1])
        return carry

    lax.fori_loop(0, per, body, 0)


def _final_inner_kernel(table, incoming, first, final, drive, kinds, out, scaled, taper, *, per,
                        batch, tiles):
    i = pl.program_id(0)

    @pl.when(i == 0)
    def _():
        scaled[...] = drive[...] * SCALE
        for t in range(tiles):
            for c, v in enumerate(_taper(kinds[t], kinds.shape[2])):
                taper[c, t] = v

    width = drive.shape[2]

    def weights(t):
        return [jnp.concatenate([taper[c, t]] * (width // taper.shape[3]), axis=1) for c in range(3)]

    def body(k, carry):
        j = i * batch + k
        cur = [first[k]]
        for t in range(1, tiles - 1):
            a = incoming[table[(2 * t) * per + j], t - 1]
            b = incoming[table[(2 * t + 1) * per + j], t - 1]
            cur.append(_halves(a, b))
        cur.append(final[k])
        cur = _blend(cur, weights, -1, None)
        res = _steps(cur, lambda t: scaled[t], range(1, tiles - 1), -1, None)
        for t, v in enumerate(res):
            out[k, t + 1] = v * (1.0 / SCALE)
        return carry

    lax.fori_loop(0, batch, body, 0)


def _final_edge_kernel(table, mask, incoming, own, halo, drive3, kinds3, prior, out, scaled, taper, *,
                       per, batch, tiles):
    side = pl.program_id(0)
    i = pl.program_id(1)

    @pl.when(i == 0)
    def _():
        for t in range(3):
            scaled[t] = drive3[0, t] * SCALE
            for c, v in enumerate(_taper(kinds3[0, t], kinds3.shape[3])):
                taper[c, t] = v

    width = drive3.shape[3]

    def weights(t):
        return [jnp.concatenate([taper[c, t]] * (width // taper.shape[3]), axis=1) for c in range(3)]

    def run(which):
        def body(k, carry):
            j = i * batch + k
            t = 1 if which == 0 else tiles - 2
            a = incoming[table[(2 * t) * per + j], 0]
            b = incoming[table[(2 * t + 1) * per + j], 0]
            inner = _halves(a, b)
            cur = [halo[0, k], own[0, k], inner]
            if which:
                cur = [inner, own[0, k], halo[0, k]]
            outer = 2 if which else 0
            cur = _blend(cur, weights, outer, mask[which])
            res = _steps(cur, lambda t: scaled[t], [1], outer, mask[which])
            out[k, 0] = res[0] * (1.0 / SCALE)
            return carry

        lax.fori_loop(0, batch, body, 0)

    pl.when(side == 0)(lambda: run(0))
    pl.when(side == 1)(lambda: run(1))


def _cost(units, extra):
    return pl.CostEstimate(flops=units, transcendentals=0, bytes_accessed=extra)


def on_device(state, forcing, parents, taper_index):
    per, rows, width = state.shape
    tiles = rows // TILE
    last = tiles - 1
    patches = rows // PATCH_ROWS
    groups = lax.axis_size("pgroup")
    bands = lax.axis_size("band")
    me = lax.axis_index("pgroup")
    band = lax.axis_index("band")
    f32 = jnp.float32
    params = pltpu.CompilerParams(vmem_limit_bytes=48 * 1024 * 1024)
    forward = [(i, i + 1) for i in range(bands - 1)]
    backward = [(b, a) for a, b in forward]

    kinds = jnp.broadcast_to(taper_index.astype(f32)[:, None], (rows, width))
    tail = jnp.concatenate([state[:, rows - TILE:], forcing[None, rows - TILE:], kinds[None, rows - TILE:]], axis=0)
    head = jnp.concatenate([state[:, :TILE], forcing[None, :TILE], kinds[None, :TILE]], axis=0)
    low = lax.ppermute(tail, "band", forward)
    high = lax.ppermute(head, "band", backward)
    mask = jnp.stack([(band > 0).astype(f32), (band < bands - 1).astype(f32)])

    table = parents.reshape(patches, groups, per)
    within = jnp.where(table // per == me, table % per, per)
    lowest = jnp.min(within, axis=2)
    highest = jnp.max(jnp.where(within == per, -1, within), axis=2)
    chosen = jnp.stack([jnp.minimum(lowest, per - 1), jnp.maximum(highest, 0)], axis=2).reshape(-1)
    mine = lax.dynamic_index_in_dim(table, me, 1, keepdims=False)
    source = mine // per
    earlier = (source[:, :, None] == source[:, None, :]) & (mine[:, None, :] < mine[:, :, None])
    slots = (source * CAP + jnp.any(earlier, axis=2).astype(jnp.int32)).reshape(-1)

    state4 = state.reshape(per, tiles, TILE, width)
    drive = forcing.reshape(tiles, TILE, width)
    kinds4 = kinds.reshape(tiles, TILE, width)[:, :, :128]
    batch = 2
    ncomp = per // batch
    gpack = 4
    npack = groups // gpack
    inner = tiles - 2

    def comp(i):
        return jnp.minimum(i, ncomp - 1)

    def pack(i):
        return jnp.maximum(i - ncomp, 0)

    sent_inner = pl.pallas_call(
        functools.partial(_inner_kernel, per=per, batch=batch, ncomp=ncomp, gpack=gpack, groups=groups),
        grid_spec=pltpu.PrefetchScalarGridSpec(
            num_scalar_prefetch=1,
            grid=(ncomp + npack,),
            in_specs=[
                pl.BlockSpec((batch, tiles, TILE, width), lambda i, t: (comp(i), 0, 0, 0)),
                pl.BlockSpec((tiles, TILE, width), lambda i, t: (0, 0, 0)),
            ],
            out_specs=pl.BlockSpec((gpack, CAP, inner, TILE, width), lambda i, t: (pack(i), 0, 0, 0, 0)),
            scratch_shapes=[
                pltpu.VMEM((per, inner, TILE, width), f32),
                pltpu.VMEM((tiles, TILE, width), f32),
            ],
        ),
        out_shape=jax.ShapeDtypeStruct((groups, CAP, inner, TILE, width), f32),
        compiler_params=params,
        cost_estimate=_cost(400_000_000, 8_000_000),
        name="advance_inner",
    )(chosen, state4, drive)
    got_inner = lax.all_to_all(sent_inner, "pgroup", split_axis=0, concat_axis=0, tiled=True)

    sent_edge = pl.pallas_call(
        functools.partial(_edge_kernel, batch=batch, ncomp=ncomp, gpack=gpack, groups=groups, last=last),
        grid_spec=pltpu.PrefetchScalarGridSpec(
            num_scalar_prefetch=2,
            grid=(ncomp + npack,),
            in_specs=[
                pl.BlockSpec((batch, 2, TILE, width), lambda i, t, m: (comp(i), 0, 0, 0)),
                pl.BlockSpec((batch, 2, TILE, width), lambda i, t, m: (comp(i), tiles // 2 - 1, 0, 0)),
                pl.BlockSpec((batch, TILE, width), lambda i, t, m: (comp(i), 0, 0)),
                pl.BlockSpec((batch, TILE, width), lambda i, t, m: (comp(i), 0, 0)),
                pl.BlockSpec((tiles, TILE, width), lambda i, t, m: (0, 0, 0)),
                pl.BlockSpec((1, TILE, width), lambda i, t, m: (per, 0, 0)),
                pl.BlockSpec((1, TILE, width), lambda i, t, m: (per, 0, 0)),
            ],
            out_specs=pl.BlockSpec((gpack, CAP, 2, TILE, width), lambda i, t, m: (pack(i), 0, 0, 0, 0)),
            scratch_shapes=[
                pltpu.VMEM((per, 2, TILE, width), f32),
                pltpu.VMEM((2, 3, TILE, width), f32),
            ],
        ),
        out_shape=jax.ShapeDtypeStruct((groups, CAP, 2, TILE, width), f32),
        compiler_params=params,
        cost_estimate=_cost(300_000_000, 4_000_000),
        name="advance_edge",
    )(chosen, mask, state4, state4, low, high, drive, low, high)
    got_edge = lax.all_to_all(sent_edge, "pgroup", split_axis=0, concat_axis=0, tiled=True)

    entries = groups * CAP
    in_edge = got_edge.reshape(entries, 2, TILE, width)
    in_inner = got_inner.reshape(entries, inner, TILE, width)
    first, final = pl.pallas_call(
        functools.partial(_pick_kernel, per=per, last=last),
        grid_spec=pltpu.PrefetchScalarGridSpec(
            num_scalar_prefetch=1,
            grid=(1,),
            in_specs=[pl.BlockSpec((entries, 2, TILE, width), lambda i, t: (0, 0, 0, 0))],
            out_specs=[pl.BlockSpec((per, TILE, width), lambda i, t: (0, 0, 0))] * 2,
        ),
        out_shape=[jax.ShapeDtypeStruct((per, TILE, width), f32)] * 2,
        compiler_params=params,
        cost_estimate=_cost(50_000_000, 3_000_000),
        name="pick_edge",
    )(slots, in_edge)
    below = lax.ppermute(final, "band", forward)
    above = lax.ppermute(first, "band", backward)

    field = pl.pallas_call(
        functools.partial(_final_inner_kernel, per=per, batch=batch, tiles=tiles),
        grid_spec=pltpu.PrefetchScalarGridSpec(
            num_scalar_prefetch=1,
            grid=(ncomp,),
            in_specs=[
                pl.BlockSpec((entries, inner, TILE, width), lambda i, t: (0, 0, 0, 0)),
                pl.BlockSpec((batch, TILE, width), lambda i, t: (i, 0, 0)),
                pl.BlockSpec((batch, TILE, width), lambda i, t: (i, 0, 0)),
                pl.BlockSpec((tiles, TILE, width), lambda i, t: (0, 0, 0)),
                pl.BlockSpec((tiles, TILE, 128), lambda i, t: (0, 0, 0)),
            ],
            out_specs=pl.BlockSpec((batch, tiles, TILE, width), lambda i, t: (i, 0, 0, 0)),
            scratch_shapes=[
                pltpu.VMEM((tiles, TILE, width), f32),
                pltpu.VMEM((3, tiles, TILE, 128), f32),
            ],
        ),
        out_shape=jax.ShapeDtypeStruct((per, tiles, TILE, width), f32),
        compiler_params=params,
        cost_estimate=_cost(500_000_000, 8_000_000),
        name="final_inner",
    )(slots, in_inner, first, final, drive, kinds4)

    drive3 = jnp.stack([
        jnp.stack([low[per], drive[0], drive[1]]), jnp.stack([drive[last - 1], drive[last], high[per]])])
    kinds3 = jnp.stack([
        jnp.stack([low[per + 1, :, :128], kinds4[0], kinds4[1]]),
        jnp.stack([kinds4[last - 1], kinds4[last], high[per + 1, :, :128]])])
    own = jnp.stack([first, final])
    halo = jnp.stack([below, above])
    ebatch = 4
    field = pl.pallas_call(
        functools.partial(_final_edge_kernel, per=per, batch=ebatch, tiles=tiles),
        grid_spec=pltpu.PrefetchScalarGridSpec(
            num_scalar_prefetch=2,
            grid=(2, per // ebatch),
            in_specs=[
                pl.BlockSpec((entries, 1, TILE, width), lambda s, i, t, m: (0, (inner - 1) * s, 0, 0)),
                pl.BlockSpec((1, ebatch, TILE, width), lambda s, i, t, m: (s, i, 0, 0)),
                pl.BlockSpec((1, ebatch, TILE, width), lambda s, i, t, m: (s, i, 0, 0)),
                pl.BlockSpec((1, 3, TILE, width), lambda s, i, t, m: (s, 0, 0, 0)),
                pl.BlockSpec((1, 3, TILE, 128), lambda s, i, t, m: (s, 0, 0, 0)),
                pl.BlockSpec(memory_space=pl.ANY),
            ],
            out_specs=pl.BlockSpec((ebatch, 1, TILE, width), lambda s, i, t, m: (i, last * s, 0, 0)),
            scratch_shapes=[
                pltpu.VMEM((3, TILE, width), f32),
                pltpu.VMEM((3, 3, TILE, 128), f32),
            ],
        ),
        out_shape=jax.ShapeDtypeStruct((per, tiles, TILE, width), f32),
        input_output_aliases={7: 0},
        compiler_params=params,
        cost_estimate=_cost(300_000_000, 4_000_000),
        name="final_edge",
    )(slots, mask, in_inner, own, halo, drive3, kinds3, field)
    return field.reshape(per, rows, width)


def solution(mesh):
    return jax.shard_map(
        on_device,
        mesh=mesh,
        in_specs=(P("pgroup", "band", None), P("band", None), P("band", None), P("band")),
        out_specs=P("pgroup", "band", None),
        check_vma=False,
    )
```

```python
import functools

import jax
import jax.numpy as jnp
from jax import lax
from jax.experimental import pallas as pl
from jax.experimental.pallas import tpu as pltpu
from jax.sharding import PartitionSpec as P

PATCH_ROWS = 4
STEPS = 6
CAP = 2
TILE = 8
SCALE = 0.05


def _sub(shape):
    return lax.broadcasted_iota(jnp.int32, shape, 0)


def _up(tiles, i, k):
    here = tiles[i]
    after = tiles[min(i + 1, len(tiles) - 1)]
    return pltpu.roll(jnp.where(_sub(here.shape) < k, after, here), TILE - k, 0)


def _down(tiles, i, k):
    here = tiles[i]
    before = tiles[max(i - 1, 0)]
    return pltpu.roll(jnp.where(_sub(here.shape) >= TILE - k, before, here), k, 0)


def _step(tiles, i, drive):
    m = tiles[i]
    width = m.shape[1]
    e = pltpu.roll(m, width - 1, 1)
    w = pltpu.roll(m, 1, 1)
    n = _up(tiles, i, 1)
    s = _down(tiles, i, 1)
    return (m * (0.4 - (e - w)) + 0.15 * (e + w)) + (0.05 * n + 0.25 * s) + drive


def _steps(groups, drive, keep, outer, mask):
    for repeat in range(STEPS):
        todo = keep if repeat == STEPS - 1 else range(len(groups[0]))
        fresh = [list(tiles) for tiles in groups]
        for i in todo:
            source = drive(i)
            for tiles, new in zip(groups, fresh):
                v = _step(tiles, i, source)
                new[i] = v * mask if i == outer else v
        groups = fresh
    return [[tiles[i] for i in keep] for tiles in groups]


def _blend(tiles, weights, outer, mask):
    fresh = []
    for i in range(len(tiles)):
        w0, w1, w2 = weights(i)
        total = w0 * tiles[i]
        total = total + w1 * (_up(tiles, i, 1) + _down(tiles, i, 1))
        total = total + w2 * (_up(tiles, i, 2) + _down(tiles, i, 2))
        if i == outer:
            total = total * mask
        fresh.append(total)
    return fresh


def _taper(kind):
    rate = 0.2 * (kind + 1.0)
    near = jnp.exp(-rate)
    far = jnp.exp(-4.0 * rate)
    inv = 1.0 / (far + near + 1.0 + near + far)
    return inv, near * inv, far * inv


def _halves(a, b):
    return jnp.where(_sub(a.shape) < PATCH_ROWS, a, b)


def _widen(v, width):
    return jnp.concatenate([v] * (width // v.shape[1]), axis=1)


def _inner_kernel(table, state, drive, out, field, scaled, *, batch, mix, ncomp, gpack, groups):
    i = pl.program_id(0)
    tiles = state.shape[1]

    @pl.when(i == 0)
    def _():
        scaled[...] = drive[...] * SCALE

    @pl.when(i < ncomp)
    def _():
        def body(k, carry):
            cur = [[state[k * mix + u, t] * SCALE for t in range(tiles)] for u in range(mix)]
            res = _steps(cur, lambda t: scaled[t], range(1, tiles - 1), -1, None)
            for u in range(mix):
                for t, v in enumerate(res[u]):
                    field[i * batch + k * mix + u, t] = v
            return carry

        lax.fori_loop(0, batch // mix, body, 0)

    @pl.when(i >= ncomp)
    def _():
        def body(k, carry):
            g = (i - ncomp) * gpack + k
            for slot in range(CAP):
                for q in range(1, tiles - 1):
                    first = table[(2 * q * groups + g) * CAP + slot]
                    second = table[((2 * q + 1) * groups + g) * CAP + slot]
                    out[k, slot, q] = _halves(field[first, q - 1], field[second, q - 1])
            return carry

        lax.fori_loop(0, gpack, body, 0)


def _edge_kernel(table, mask, low_in, high_in, low, high, drive, drive_low, drive_high, prior, out,
                 field, scaled, *, batch, mix, ncomp, npack, gpack, groups, last):
    i = pl.program_id(0)

    @pl.when(i == 0)
    def _():
        scaled[0, 0] = drive_low[0] * SCALE
        scaled[0, 1] = drive[0] * SCALE
        scaled[0, 2] = drive[1] * SCALE
        scaled[1, 0] = drive[last - 1] * SCALE
        scaled[1, 1] = drive[last] * SCALE
        scaled[1, 2] = drive_high[0] * SCALE

    @pl.when(i < ncomp)
    def _():
        def body(k, carry):
            at = [k * mix + u for u in range(mix)]
            cur = [[low[j] * SCALE, low_in[j, 0] * SCALE, low_in[j, 1] * SCALE] for j in at]
            res = _steps(cur, lambda t: scaled[0, t], [1], 0, mask[0])
            for j, r in zip(at, res):
                field[0, i * batch + j] = r[0]
            cur = [[high_in[j, 0] * SCALE, high_in[j, 1] * SCALE, high[j] * SCALE] for j in at]
            res = _steps(cur, lambda t: scaled[1, t], [1], 2, mask[1])
            for j, r in zip(at, res):
                field[1, i * batch + j] = r[0]
            return carry

        lax.fori_loop(0, batch // mix, body, 0)

    @pl.when(i >= ncomp)
    def _():
        side = (i - ncomp) // npack
        base = 2 * last * side

        def body(k, carry):
            g = ((i - ncomp) % npack) * gpack + k
            for slot in range(CAP):
                first = table[(base * groups + g) * CAP + slot]
                second = table[((base + 1) * groups + g) * CAP + slot]
                out[k, slot, 0] = _halves(field[side, first], field[side, second])
            return carry

        lax.fori_loop(0, gpack, body, 0)


def _pick_kernel(table, incoming0, incoming1, first, final, *, per, last):
    def body(j, carry):
        first[j] = _halves(incoming0[table[j], 0], incoming0[table[per + j], 0])
        base = 2 * last * per
        final[j] = _halves(incoming1[table[base + j], 0], incoming1[table[base + per + j], 0])
        return carry

    lax.fori_loop(0, per, body, 0)


def _final_inner_kernel(table, incoming, drive, kinds, out, scaled, taper, *, per, batch, mix, tiles):
    i = pl.program_id(0)

    @pl.when(i == 0)
    def _():
        scaled[...] = drive[...] * SCALE
        for t in range(tiles):
            for c, v in enumerate(_taper(kinds[t])):
                taper[c, t] = v

    width = drive.shape[2]

    def weights(t):
        return [_widen(taper[c, t], width) for c in range(3)]

    def body(k, carry):
        cur = []
        for u in range(mix):
            j = i * batch + k * mix + u
            mine = []
            for t in range(tiles):
                a = incoming[table[(2 * t) * per + j], t]
                b = incoming[table[(2 * t + 1) * per + j], t]
                mine.append(_halves(a, b))
            cur.append(_blend(mine, weights, -1, None))
        res = _steps(cur, lambda t: scaled[t], range(1, tiles - 1), -1, None)
        for u in range(mix):
            for t, v in enumerate(res[u]):
                out[k * mix + u, t + 1] = v * (1.0 / SCALE)
        return carry

    lax.fori_loop(0, batch // mix, body, 0)


def _final_edge_kernel(table, mask, incoming, first, final, below, above, drive, drive_low, drive_high,
                       kinds, kinds_low, kinds_high, prior, out, scaled, taper, *, per, batch, mix, last):
    side = pl.program_id(0)
    i = pl.program_id(1)
    width = drive.shape[2]

    @pl.when((i == 0) & (side == 0))
    def _():
        both = [[(drive_low[0], kinds_low[0]), (drive[0], kinds[0]), (drive[1], kinds[1])],
                [(drive[last - 1], kinds[last - 1]), (drive[last], kinds[last]), (drive_high[0], kinds_high[0])]]
        for s in range(2):
            for t in range(3):
                scaled[s, t] = both[s][t][0] * SCALE
                for c, v in enumerate(_taper(both[s][t][1])):
                    taper[s, c, t] = v

    def run(s):
        def weights(t):
            return [_widen(taper[s, c, t], width) for c in range(3)]

        def body(k, carry):
            t = 1 if s == 0 else last - 1
            cur = []
            for u in range(mix):
                j = k * mix + u
                row = (2 * t) * per + i * batch + j
                inner = _halves(incoming[table[row], 0], incoming[table[row + per], 0])
                three = [below[j], first[j], inner] if s == 0 else [inner, final[j], above[j]]
                cur.append(_blend(three, weights, 2 * s, mask[s]))
            res = _steps(cur, lambda t: scaled[s, t], [1], 2 * s, mask[s])
            for u in range(mix):
                out[k * mix + u, 0] = res[u][0] * (1.0 / SCALE)
            return carry

        lax.fori_loop(0, batch // mix, body, 0)

    pl.when(side == 0)(lambda: run(0))
    pl.when(side == 1)(lambda: run(1))


def _cost(units, extra):
    return pl.CostEstimate(flops=units, transcendentals=0, bytes_accessed=extra)


def on_device(state, forcing, parents, taper_index):
    per, rows, width = state.shape
    tiles = rows // TILE
    last = tiles - 1
    patches = rows // PATCH_ROWS
    groups = lax.axis_size("pgroup")
    bands = lax.axis_size("band")
    me = lax.axis_index("pgroup")
    band = lax.axis_index("band")
    f32 = jnp.float32
    params = pltpu.CompilerParams(vmem_limit_bytes=48 * 1024 * 1024)
    forward = [(i, i + 1) for i in range(bands - 1)]
    backward = [(b, a) for a, b in forward]

    kinds = jnp.broadcast_to(taper_index.astype(f32)[:, None], (rows, width))
    tail = jnp.concatenate([state[:, rows - TILE:], forcing[None, rows - TILE:], kinds[None, rows - TILE:]], axis=0)
    head = jnp.concatenate([state[:, :TILE], forcing[None, :TILE], kinds[None, :TILE]], axis=0)
    low = lax.ppermute(tail, "band", forward)
    high = lax.ppermute(head, "band", backward)
    mask = jnp.stack([(band > 0).astype(f32), (band < bands - 1).astype(f32)])

    table = parents.reshape(patches, groups, per)
    within = jnp.where(table // per == me, table % per, per)
    lowest = jnp.min(within, axis=2)
    highest = jnp.max(jnp.where(within == per, -1, within), axis=2)
    chosen = jnp.stack([jnp.minimum(lowest, per - 1), jnp.maximum(highest, 0)], axis=2).reshape(-1)
    mine = lax.dynamic_index_in_dim(table, me, 1, keepdims=False)
    source = mine // per
    earlier = (source[:, :, None] == source[:, None, :]) & (mine[:, None, :] < mine[:, :, None])
    slots = (source * CAP + jnp.any(earlier, axis=2).astype(jnp.int32)).reshape(-1)

    state4 = state.reshape(per, tiles, TILE, width)
    drive = forcing.reshape(tiles, TILE, width)
    kinds4 = kinds.reshape(tiles, TILE, width)
    entries = groups * CAP

    batch, mix, gpack = 4, 2, 4
    ncomp, npack = per // batch, groups // gpack
    message = pl.pallas_call(
        functools.partial(_inner_kernel, batch=batch, mix=mix, ncomp=ncomp, gpack=gpack, groups=groups),
        grid_spec=pltpu.PrefetchScalarGridSpec(
            num_scalar_prefetch=1,
            grid=(ncomp + npack,),
            in_specs=[
                pl.BlockSpec((batch, tiles, TILE, width), lambda i, t: (jnp.minimum(i, ncomp - 1), 0, 0, 0)),
                pl.BlockSpec((tiles, TILE, width), lambda i, t: (0, 0, 0)),
            ],
            out_specs=pl.BlockSpec((gpack, CAP, tiles, TILE, width), lambda i, t: (jnp.maximum(i - ncomp, 0), 0, 0, 0, 0)),
            scratch_shapes=[
                pltpu.VMEM((per, tiles - 2, TILE, width), f32),
                pltpu.VMEM((tiles, TILE, width), f32),
            ],
        ),
        out_shape=jax.ShapeDtypeStruct((groups, CAP, tiles, TILE, width), f32),
        compiler_params=params,
        cost_estimate=_cost(400_000_000, 8_000_000),
        name="advance_inner",
    )(chosen, state4, drive)

    ebatch, emix, epack = 8, 4, 8
    ecomp, enp = per // ebatch, groups // epack

    def ecs(i):
        return jnp.minimum(i, ecomp - 1)

    def eout(i, t, m):
        k = jnp.maximum(i - ecomp, 0)
        return (k % enp, 0, last * (k // enp), 0, 0)

    message = pl.pallas_call(
        functools.partial(_edge_kernel, batch=ebatch, mix=emix, ncomp=ecomp, npack=enp, gpack=epack, groups=groups,
                          last=last),
        grid_spec=pltpu.PrefetchScalarGridSpec(
            num_scalar_prefetch=2,
            grid=(ecomp + 2 * enp,),
            in_specs=[
                pl.BlockSpec((ebatch, 2, TILE, width), lambda i, t, m: (ecs(i), 0, 0, 0)),
                pl.BlockSpec((ebatch, 2, TILE, width), lambda i, t, m: (ecs(i), tiles // 2 - 1, 0, 0)),
                pl.BlockSpec((ebatch, TILE, width), lambda i, t, m: (ecs(i), 0, 0)),
                pl.BlockSpec((ebatch, TILE, width), lambda i, t, m: (ecs(i), 0, 0)),
                pl.BlockSpec((tiles, TILE, width), lambda i, t, m: (0, 0, 0)),
                pl.BlockSpec((1, TILE, width), lambda i, t, m: (per, 0, 0)),
                pl.BlockSpec((1, TILE, width), lambda i, t, m: (per, 0, 0)),
                pl.BlockSpec(memory_space=pl.ANY),
            ],
            out_specs=pl.BlockSpec((epack, CAP, 1, TILE, width), eout),
            scratch_shapes=[
                pltpu.VMEM((2, per, TILE, width), f32),
                pltpu.VMEM((2, 3, TILE, width), f32),
            ],
        ),
        out_shape=jax.ShapeDtypeStruct((groups, CAP, tiles, TILE, width), f32),
        input_output_aliases={9: 0},
        compiler_params=params,
        cost_estimate=_cost(300_000_000, 4_000_000),
        name="advance_edge",
    )(chosen, mask, state4, state4, low, high, drive, low, high, message)
    incoming = lax.all_to_all(message, "pgroup", split_axis=0, concat_axis=0, tiled=True)
    incoming = incoming.reshape(entries, tiles, TILE, width)

    first, final = pl.pallas_call(
        functools.partial(_pick_kernel, per=per, last=last),
        grid_spec=pltpu.PrefetchScalarGridSpec(
            num_scalar_prefetch=1,
            grid=(1,),
            in_specs=[
                pl.BlockSpec((entries, 1, TILE, width), lambda i, t: (0, 0, 0, 0)),
                pl.BlockSpec((entries, 1, TILE, width), lambda i, t: (0, last, 0, 0)),
            ],
            out_specs=[pl.BlockSpec((per, TILE, width), lambda i, t: (0, 0, 0))] * 2,
        ),
        out_shape=[jax.ShapeDtypeStruct((per, TILE, width), f32)] * 2,
        compiler_params=params,
        cost_estimate=_cost(50_000_000, 3_000_000),
        name="pick_edge",
    )(slots, incoming, incoming)
    below = lax.ppermute(final, "band", forward)
    above = lax.ppermute(first, "band", backward)

    field = pl.pallas_call(
        functools.partial(_final_inner_kernel, per=per, batch=batch, mix=mix, tiles=tiles),
        grid_spec=pltpu.PrefetchScalarGridSpec(
            num_scalar_prefetch=1,
            grid=(per // batch,),
            in_specs=[
                pl.BlockSpec((entries, tiles, TILE, width), lambda i, t: (0, 0, 0, 0)),
                pl.BlockSpec((tiles, TILE, width), lambda i, t: (0, 0, 0)),
                pl.BlockSpec((tiles, TILE, 128), lambda i, t: (0, 0, 0)),
            ],
            out_specs=pl.BlockSpec((batch, tiles, TILE, width), lambda i, t: (i, 0, 0, 0)),
            scratch_shapes=[
                pltpu.VMEM((tiles, TILE, width), f32),
                pltpu.VMEM((3, tiles, TILE, 128), f32),
            ],
        ),
        out_shape=jax.ShapeDtypeStruct((per, tiles, TILE, width), f32),
        compiler_params=params,
        cost_estimate=_cost(500_000_000, 8_000_000),
        name="final_inner",
    )(slots, incoming, drive, kinds4)

    def lo(s, i, t, m):
        return (jnp.where(s == 0, i, per // ebatch - 1), 0, 0)

    def hi(s, i, t, m):
        return (jnp.where(s == 0, 0, i), 0, 0)

    field = pl.pallas_call(
        functools.partial(_final_edge_kernel, per=per, batch=ebatch, mix=emix, last=last),
        grid_spec=pltpu.PrefetchScalarGridSpec(
            num_scalar_prefetch=2,
            grid=(2, per // ebatch),
            in_specs=[
                pl.BlockSpec((entries, 1, TILE, width), lambda s, i, t, m: (0, 1 + (last - 2) * s, 0, 0)),
                pl.BlockSpec((ebatch, TILE, width), lo),
                pl.BlockSpec((ebatch, TILE, width), hi),
                pl.BlockSpec((ebatch, TILE, width), lo),
                pl.BlockSpec((ebatch, TILE, width), hi),
                pl.BlockSpec((tiles, TILE, width), lambda s, i, t, m: (0, 0, 0)),
                pl.BlockSpec((1, TILE, width), lambda s, i, t, m: (per, 0, 0)),
                pl.BlockSpec((1, TILE, width), lambda s, i, t, m: (per, 0, 0)),
                pl.BlockSpec((tiles, TILE, 128), lambda s, i, t, m: (0, 0, 0)),
                pl.BlockSpec((1, TILE, 128), lambda s, i, t, m: (per + 1, 0, 0)),
                pl.BlockSpec((1, TILE, 128), lambda s, i, t, m: (per + 1, 0, 0)),
                pl.BlockSpec(memory_space=pl.ANY),
            ],
            out_specs=pl.BlockSpec((ebatch, 1, TILE, width), lambda s, i, t, m: (i, last * s, 0, 0)),
            scratch_shapes=[
                pltpu.VMEM((2, 3, TILE, width), f32),
                pltpu.VMEM((2, 3, 3, TILE, 128), f32),
            ],
        ),
        out_shape=jax.ShapeDtypeStruct((per, tiles, TILE, width), f32),
        input_output_aliases={13: 0},
        compiler_params=params,
        cost_estimate=_cost(300_000_000, 4_000_000),
        name="final_edge",
    )(slots, mask, incoming, first, final, below, above, drive, low, high, kinds4, low, high, field)
    return field.reshape(per, rows, width)


def solution(mesh):
    return jax.shard_map(
        on_device,
        mesh=mesh,
        in_specs=(P("pgroup", "band", None), P("band", None), P("band", None), P("band")),
        out_specs=P("pgroup", "band", None),
        check_vma=False,
    )
```

```python
import functools

import jax
import jax.numpy as jnp
from jax import lax
from jax.experimental import pallas as pl
from jax.experimental.pallas import tpu as pltpu
from jax.sharding import PartitionSpec as P

PATCH_ROWS = 4
STEPS = 6
CAP = 2
TILE = 8
SCALE = 0.05


def _sub(shape):
    return lax.broadcasted_iota(jnp.int32, shape, 0)


def _up(tiles, i, k):
    here = tiles[i]
    after = tiles[min(i + 1, len(tiles) - 1)]
    return pltpu.roll(jnp.where(_sub(here.shape) < k, after, here), TILE - k, 0)


def _down(tiles, i, k):
    here = tiles[i]
    before = tiles[max(i - 1, 0)]
    return pltpu.roll(jnp.where(_sub(here.shape) >= TILE - k, before, here), k, 0)


def _step(tiles, i, drive):
    m = tiles[i]
    width = m.shape[1]
    e = pltpu.roll(m, width - 1, 1)
    w = pltpu.roll(m, 1, 1)
    n = _up(tiles, i, 1)
    s = _down(tiles, i, 1)
    return (m * (0.4 - (e - w)) + 0.15 * (e + w)) + (0.05 * n + 0.25 * s) + drive


def _steps(groups, drive, keep, outer, mask):
    for repeat in range(STEPS):
        todo = keep if repeat == STEPS - 1 else range(len(groups[0]))
        fresh = [list(tiles) for tiles in groups]
        for i in todo:
            source = drive(i)
            for tiles, new in zip(groups, fresh):
                v = _step(tiles, i, source)
                new[i] = v * mask if i == outer else v
        groups = fresh
    return [[tiles[i] for i in keep] for tiles in groups]


def _blend(tiles, weights, outer, mask):
    fresh = []
    for i in range(len(tiles)):
        w0, w1, w2 = weights(i)
        total = w0 * tiles[i]
        total = total + w1 * (_up(tiles, i, 1) + _down(tiles, i, 1))
        total = total + w2 * (_up(tiles, i, 2) + _down(tiles, i, 2))
        if i == outer:
            total = total * mask
        fresh.append(total)
    return fresh


def _taper(kind):
    rate = 0.2 * (kind + 1.0)
    near = jnp.exp(-rate)
    far = jnp.exp(-4.0 * rate)
    inv = 1.0 / (far + near + 1.0 + near + far)
    return inv, near * inv, far * inv


def _halves(a, b):
    return jnp.where(_sub(a.shape) < PATCH_ROWS, a, b)


def _widen(v, width):
    return jnp.concatenate([v] * (width // v.shape[1]), axis=1)


def _inner_kernel(table, state, drive, out, field, scaled, *, batch, mix, ncomp, gpack, groups):
    i = pl.program_id(0)
    tiles = state.shape[1]

    @pl.when(i == 0)
    def _():
        scaled[...] = drive[...] * SCALE

    @pl.when(i < ncomp)
    def _():
        def body(k, carry):
            cur = [[state[k * mix + u, t] * SCALE for t in range(tiles)] for u in range(mix)]
            res = _steps(cur, lambda t: scaled[t], range(1, tiles - 1), -1, None)
            for u in range(mix):
                for t, v in enumerate(res[u]):
                    field[i * batch + k * mix + u, t] = v
            return carry

        lax.fori_loop(0, batch // mix, body, 0)

    @pl.when(i >= ncomp)
    def _():
        def body(k, carry):
            g = (i - ncomp) * gpack + k
            for slot in range(CAP):
                for q in range(1, tiles - 1):
                    first = table[(2 * q * groups + g) * CAP + slot]
                    second = table[((2 * q + 1) * groups + g) * CAP + slot]
                    out[k, slot, q] = _halves(field[first, q - 1], field[second, q - 1])
            return carry

        lax.fori_loop(0, gpack, body, 0)


def _edge_kernel(table, mask, low_in, high_in, low, high, drive, drive_low, drive_high, prior, out,
                 field, scaled, *, batch, mix, ncomp, npack, gpack, groups, last):
    i = pl.program_id(0)

    @pl.when(i == 0)
    def _():
        scaled[0, 0] = drive_low[0] * SCALE
        scaled[0, 1] = drive[0] * SCALE
        scaled[0, 2] = drive[1] * SCALE
        scaled[1, 0] = drive[last - 1] * SCALE
        scaled[1, 1] = drive[last] * SCALE
        scaled[1, 2] = drive_high[0] * SCALE

    @pl.when(i < ncomp)
    def _():
        def body(k, carry):
            at = [k * mix + u for u in range(mix)]
            cur = [[low[j] * SCALE, low_in[j, 0] * SCALE, low_in[j, 1] * SCALE] for j in at]
            res = _steps(cur, lambda t: scaled[0, t], [1], 0, mask[0])
            for j, r in zip(at, res):
                field[0, i * batch + j] = r[0]
            cur = [[high_in[j, 0] * SCALE, high_in[j, 1] * SCALE, high[j] * SCALE] for j in at]
            res = _steps(cur, lambda t: scaled[1, t], [1], 2, mask[1])
            for j, r in zip(at, res):
                field[1, i * batch + j] = r[0]
            return carry

        lax.fori_loop(0, batch // mix, body, 0)

    @pl.when(i >= ncomp)
    def _():
        side = (i - ncomp) // npack
        base = 2 * last * side

        def body(k, carry):
            g = ((i - ncomp) % npack) * gpack + k
            for slot in range(CAP):
                first = table[(base * groups + g) * CAP + slot]
                second = table[((base + 1) * groups + g) * CAP + slot]
                out[k, slot, 0] = _halves(field[side, first], field[side, second])
            return carry

        lax.fori_loop(0, gpack, body, 0)


def _pick_kernel(table, incoming0, incoming1, first, final, *, per, last):
    def body(j, carry):
        first[j] = _halves(incoming0[table[j], 0], incoming0[table[per + j], 0])
        base = 2 * last * per
        final[j] = _halves(incoming1[table[base + j], 0], incoming1[table[base + per + j], 0])
        return carry

    lax.fori_loop(0, per, body, 0)


def _final_inner_kernel(table, incoming, drive, kinds, out, scaled, taper, *, per, batch, mix, tiles):
    i = pl.program_id(0)

    @pl.when(i == 0)
    def _():
        scaled[...] = drive[...] * SCALE
        for t in range(tiles):
            for c, v in enumerate(_taper(kinds[t])):
                taper[c, t] = v

    width = drive.shape[2]

    def weights(t):
        return [_widen(taper[c, t], width) for c in range(3)]

    def body(k, carry):
        cur = []
        for u in range(mix):
            j = i * batch + k * mix + u
            mine = []
            for t in range(tiles):
                a = incoming[table[(2 * t) * per + j], t]
                b = incoming[table[(2 * t + 1) * per + j], t]
                mine.append(_halves(a, b))
            cur.append(_blend(mine, weights, -1, None))
        res = _steps(cur, lambda t: scaled[t], range(1, tiles - 1), -1, None)
        for u in range(mix):
            for t, v in enumerate(res[u]):
                out[k * mix + u, t + 1] = v * (1.0 / SCALE)
        return carry

    lax.fori_loop(0, batch // mix, body, 0)


def _final_edge_kernel(table, mask, incoming, first, final, below, above, drive, drive_low, drive_high,
                       kinds, kinds_low, kinds_high, prior, out, scaled, taper, *, per, batch, mix, last):
    side = pl.program_id(0)
    i = pl.program_id(1)
    width = drive.shape[2]

    @pl.when((i == 0) & (side == 0))
    def _():
        both = [[(drive_low[0], kinds_low[0]), (drive[0], kinds[0]), (drive[1], kinds[1])],
                [(drive[last - 1], kinds[last - 1]), (drive[last], kinds[last]), (drive_high[0], kinds_high[0])]]
        for s in range(2):
            for t in range(3):
                scaled[s, t] = both[s][t][0] * SCALE
                for c, v in enumerate(_taper(both[s][t][1])):
                    taper[s, c, t] = v

    def run(s):
        def weights(t):
            return [_widen(taper[s, c, t], width) for c in range(3)]

        def body(k, carry):
            t = 1 if s == 0 else last - 1
            cur = []
            for u in range(mix):
                j = k * mix + u
                row = (2 * t) * per + i * batch + j
                inner = _halves(incoming[table[row], 0], incoming[table[row + per], 0])
                three = [below[j], first[j], inner] if s == 0 else [inner, final[j], above[j]]
                cur.append(_blend(three, weights, 2 * s, mask[s]))
            res = _steps(cur, lambda t: scaled[s, t], [1], 2 * s, mask[s])
            for u in range(mix):
                out[k * mix + u, 0] = res[u][0] * (1.0 / SCALE)
            return carry

        lax.fori_loop(0, batch // mix, body, 0)

    pl.when(side == 0)(lambda: run(0))
    pl.when(side == 1)(lambda: run(1))


def _cost(units, extra):
    return pl.CostEstimate(flops=units, transcendentals=0, bytes_accessed=extra)


def on_device(state, forcing, parents, taper_index):
    per, rows, width = state.shape
    tiles = rows // TILE
    last = tiles - 1
    patches = rows // PATCH_ROWS
    groups = lax.axis_size("pgroup")
    bands = lax.axis_size("band")
    me = lax.axis_index("pgroup")
    band = lax.axis_index("band")
    f32 = jnp.float32
    params = pltpu.CompilerParams(vmem_limit_bytes=48 * 1024 * 1024)
    forward = [(i, i + 1) for i in range(bands - 1)]
    backward = [(b, a) for a, b in forward]

    kinds = jnp.broadcast_to(taper_index.astype(f32)[:, None], (rows, width))
    tail = jnp.concatenate([state[:, rows - TILE:], forcing[None, rows - TILE:], kinds[None, rows - TILE:]], axis=0)
    head = jnp.concatenate([state[:, :TILE], forcing[None, :TILE], kinds[None, :TILE]], axis=0)
    low = lax.ppermute(tail, "band", forward)
    high = lax.ppermute(head, "band", backward)
    mask = jnp.stack([(band > 0).astype(f32), (band < bands - 1).astype(f32)])

    table = parents.reshape(patches, groups, per)
    within = jnp.where(table // per == me, table % per, per)
    lowest = jnp.min(within, axis=2)
    highest = jnp.max(jnp.where(within == per, -1, within), axis=2)
    chosen = jnp.stack([jnp.minimum(lowest, per - 1), jnp.maximum(highest, 0)], axis=2).reshape(-1)
    mine = lax.dynamic_index_in_dim(table, me, 1, keepdims=False)
    source = mine // per
    earlier = (source[:, :, None] == source[:, None, :]) & (mine[:, None, :] < mine[:, :, None])
    slots = (source * CAP + jnp.any(earlier, axis=2).astype(jnp.int32)).reshape(-1)

    state4 = state.reshape(per, tiles, TILE, width)
    drive = forcing.reshape(tiles, TILE, width)
    kinds4 = kinds.reshape(tiles, TILE, width)
    entries = groups * CAP

    batch, mix, gpack = 4, 2, 4
    ncomp, npack = per // batch, groups // gpack
    message = pl.pallas_call(
        functools.partial(_inner_kernel, batch=batch, mix=mix, ncomp=ncomp, gpack=gpack, groups=groups),
        grid_spec=pltpu.PrefetchScalarGridSpec(
            num_scalar_prefetch=1,
            grid=(ncomp + npack,),
            in_specs=[
                pl.BlockSpec((batch, tiles, TILE, width), lambda i, t: (jnp.minimum(i, ncomp - 1), 0, 0, 0)),
                pl.BlockSpec((tiles, TILE, width), lambda i, t: (0, 0, 0)),
            ],
            out_specs=pl.BlockSpec((gpack, CAP, tiles, TILE, width), lambda i, t: (jnp.maximum(i - ncomp, 0), 0, 0, 0, 0)),
            scratch_shapes=[
                pltpu.VMEM((per, tiles - 2, TILE, width), f32),
                pltpu.VMEM((tiles, TILE, width), f32),
            ],
        ),
        out_shape=jax.ShapeDtypeStruct((groups, CAP, tiles, TILE, width), f32),
        compiler_params=params,
        cost_estimate=_cost(400_000_000, 8_000_000),
        name="advance_inner",
    )(chosen, state4, drive)

    ebatch, emix, epack = 8, 4, 8
    ecomp, enp = per // ebatch, groups // epack

    def ecs(i):
        return jnp.minimum(i, ecomp - 1)

    def eout(i, t, m):
        k = jnp.maximum(i - ecomp, 0)
        return (k % enp, 0, last * (k // enp), 0, 0)

    message = pl.pallas_call(
        functools.partial(_edge_kernel, batch=ebatch, mix=emix, ncomp=ecomp, npack=enp, gpack=epack, groups=groups,
                          last=last),
        grid_spec=pltpu.PrefetchScalarGridSpec(
            num_scalar_prefetch=2,
            grid=(ecomp + 2 * enp,),
            in_specs=[
                pl.BlockSpec((ebatch, 2, TILE, width), lambda i, t, m: (ecs(i), 0, 0, 0)),
                pl.BlockSpec((ebatch, 2, TILE, width), lambda i, t, m: (ecs(i), tiles // 2 - 1, 0, 0)),
                pl.BlockSpec((ebatch, TILE, width), lambda i, t, m: (ecs(i), 0, 0)),
                pl.BlockSpec((ebatch, TILE, width), lambda i, t, m: (ecs(i), 0, 0)),
                pl.BlockSpec((tiles, TILE, width), lambda i, t, m: (0, 0, 0)),
                pl.BlockSpec((1, TILE, width), lambda i, t, m: (per, 0, 0)),
                pl.BlockSpec((1, TILE, width), lambda i, t, m: (per, 0, 0)),
                pl.BlockSpec(memory_space=pl.ANY),
            ],
            out_specs=pl.BlockSpec((epack, CAP, 1, TILE, width), eout),
            scratch_shapes=[
                pltpu.VMEM((2, per, TILE, width), f32),
                pltpu.VMEM((2, 3, TILE, width), f32),
            ],
        ),
        out_shape=jax.ShapeDtypeStruct((groups, CAP, tiles, TILE, width), f32),
        input_output_aliases={9: 0},
        compiler_params=params,
        cost_estimate=_cost(300_000_000, 4_000_000),
        name="advance_edge",
    )(chosen, mask, state4, state4, low, high, drive, low, high, message)
    message, slots, kinds4 = lax.optimization_barrier((message, slots, kinds4))
    incoming = lax.all_to_all(message, "pgroup", split_axis=0, concat_axis=0, tiled=True)
    incoming = incoming.reshape(entries, tiles, TILE, width)

    first, final = pl.pallas_call(
        functools.partial(_pick_kernel, per=per, last=last),
        grid_spec=pltpu.PrefetchScalarGridSpec(
            num_scalar_prefetch=1,
            grid=(1,),
            in_specs=[
                pl.BlockSpec((entries, 1, TILE, width), lambda i, t: (0, 0, 0, 0)),
                pl.BlockSpec((entries, 1, TILE, width), lambda i, t: (0, last, 0, 0)),
            ],
            out_specs=[pl.BlockSpec((per, TILE, width), lambda i, t: (0, 0, 0))] * 2,
        ),
        out_shape=[jax.ShapeDtypeStruct((per, TILE, width), f32)] * 2,
        compiler_params=params,
        cost_estimate=_cost(50_000_000, 3_000_000),
        name="pick_edge",
    )(slots, incoming, incoming)
    below = lax.ppermute(final, "band", forward)
    above = lax.ppermute(first, "band", backward)

    field = pl.pallas_call(
        functools.partial(_final_inner_kernel, per=per, batch=batch, mix=mix, tiles=tiles),
        grid_spec=pltpu.PrefetchScalarGridSpec(
            num_scalar_prefetch=1,
            grid=(per // batch,),
            in_specs=[
                pl.BlockSpec((entries, tiles, TILE, width), lambda i, t: (0, 0, 0, 0)),
                pl.BlockSpec((tiles, TILE, width), lambda i, t: (0, 0, 0)),
                pl.BlockSpec((tiles, TILE, 128), lambda i, t: (0, 0, 0)),
            ],
            out_specs=pl.BlockSpec((batch, tiles, TILE, width), lambda i, t: (i, 0, 0, 0)),
            scratch_shapes=[
                pltpu.VMEM((tiles, TILE, width), f32),
                pltpu.VMEM((3, tiles, TILE, 128), f32),
            ],
        ),
        out_shape=jax.ShapeDtypeStruct((per, tiles, TILE, width), f32),
        compiler_params=params,
        cost_estimate=_cost(500_000_000, 8_000_000),
        name="final_inner",
    )(slots, incoming, drive, kinds4)

    def lo(s, i, t, m):
        return (jnp.where(s == 0, i, per // ebatch - 1), 0, 0)

    def hi(s, i, t, m):
        return (jnp.where(s == 0, 0, i), 0, 0)

    field = pl.pallas_call(
        functools.partial(_final_edge_kernel, per=per, batch=ebatch, mix=emix, last=last),
        grid_spec=pltpu.PrefetchScalarGridSpec(
            num_scalar_prefetch=2,
            grid=(2, per // ebatch),
            in_specs=[
                pl.BlockSpec((entries, 1, TILE, width), lambda s, i, t, m: (0, 1 + (last - 2) * s, 0, 0)),
                pl.BlockSpec((ebatch, TILE, width), lo),
                pl.BlockSpec((ebatch, TILE, width), hi),
                pl.BlockSpec((ebatch, TILE, width), lo),
                pl.BlockSpec((ebatch, TILE, width), hi),
                pl.BlockSpec((tiles, TILE, width), lambda s, i, t, m: (0, 0, 0)),
                pl.BlockSpec((1, TILE, width), lambda s, i, t, m: (per, 0, 0)),
                pl.BlockSpec((1, TILE, width), lambda s, i, t, m: (per, 0, 0)),
                pl.BlockSpec((tiles, TILE, 128), lambda s, i, t, m: (0, 0, 0)),
                pl.BlockSpec((1, TILE, 128), lambda s, i, t, m: (per + 1, 0, 0)),
                pl.BlockSpec((1, TILE, 128), lambda s, i, t, m: (per + 1, 0, 0)),
                pl.BlockSpec(memory_space=pl.ANY),
            ],
            out_specs=pl.BlockSpec((ebatch, 1, TILE, width), lambda s, i, t, m: (i, last * s, 0, 0)),
            scratch_shapes=[
                pltpu.VMEM((2, 3, TILE, width), f32),
                pltpu.VMEM((2, 3, 3, TILE, 128), f32),
            ],
        ),
        out_shape=jax.ShapeDtypeStruct((per, tiles, TILE, width), f32),
        input_output_aliases={13: 0},
        compiler_params=params,
        cost_estimate=_cost(300_000_000, 4_000_000),
        name="final_edge",
    )(slots, mask, incoming, first, final, below, above, drive, low, high, kinds4, low, high, field)
    return field.reshape(per, rows, width)


def solution(mesh):
    return jax.shard_map(
        on_device,
        mesh=mesh,
        in_specs=(P("pgroup", "band", None), P("band", None), P("band", None), P("band")),
        out_specs=P("pgroup", "band", None),
        check_vma=False,
    )
```

```python
import functools

import jax
import jax.numpy as jnp
from jax import lax
from jax.experimental import pallas as pl
from jax.experimental.pallas import tpu as pltpu
from jax.sharding import PartitionSpec as P

PATCH_ROWS = 4
STEPS = 6
CAP = 2
TILE = 8
SCALE = 0.05


def _sub(shape):
    return lax.broadcasted_iota(jnp.int32, shape, 0)


def _up(tiles, i, k):
    here = tiles[i]
    after = tiles[min(i + 1, len(tiles) - 1)]
    return pltpu.roll(jnp.where(_sub(here.shape) < k, after, here), TILE - k, 0)


def _down(tiles, i, k):
    here = tiles[i]
    before = tiles[max(i - 1, 0)]
    return pltpu.roll(jnp.where(_sub(here.shape) >= TILE - k, before, here), k, 0)


def _step(tiles, i, drive):
    m = tiles[i]
    width = m.shape[1]
    e = pltpu.roll(m, width - 1, 1)
    w = pltpu.roll(m, 1, 1)
    n = _up(tiles, i, 1)
    s = _down(tiles, i, 1)
    return (m * (0.4 - (e - w)) + 0.15 * (e + w)) + (0.05 * n + 0.25 * s) + drive


def _steps(groups, drive, keep, outer, mask):
    for repeat in range(STEPS):
        todo = keep if repeat == STEPS - 1 else range(len(groups[0]))
        fresh = [list(tiles) for tiles in groups]
        for i in todo:
            source = drive(i)
            for tiles, new in zip(groups, fresh):
                v = _step(tiles, i, source)
                new[i] = v * mask if i == outer else v
        groups = fresh
    return [[tiles[i] for i in keep] for tiles in groups]


def _blend(tiles, weights, outer, mask):
    fresh = []
    for i in range(len(tiles)):
        w0, w1, w2 = weights(i)
        total = w0 * tiles[i]
        total = total + w1 * (_up(tiles, i, 1) + _down(tiles, i, 1))
        total = total + w2 * (_up(tiles, i, 2) + _down(tiles, i, 2))
        if i == outer:
            total = total * mask
        fresh.append(total)
    return fresh


def _taper(kind):
    rate = 0.2 * (kind + 1.0)
    near = jnp.exp(-rate)
    far = jnp.exp(-4.0 * rate)
    inv = 1.0 / (far + near + 1.0 + near + far)
    return inv, near * inv, far * inv


def _halves(a, b):
    return jnp.where(_sub(a.shape) < PATCH_ROWS, a, b)


def _widen(v, width):
    return jnp.concatenate([v] * (width // v.shape[1]), axis=1)


def _prep_kernel(info, taper, state, forcing, parents, head, tail, kinds, lowest, highest, slots, local, drive, sems,
                 *, per, tiles):
    last = tiles - 1
    copies = [
        pltpu.make_async_copy(state.at[:, 0], head.at[pl.ds(0, per)], sems.at[0]),
        pltpu.make_async_copy(state.at[:, last], tail.at[pl.ds(0, per)], sems.at[1]),
        pltpu.make_async_copy(forcing.at[0], head.at[per], sems.at[2]),
        pltpu.make_async_copy(forcing.at[last], tail.at[per], sems.at[3]),
        pltpu.make_async_copy(forcing, drive, sems.at[4]),
        pltpu.make_async_copy(state, local, sems.at[5]),
    ]
    for c in copies:
        c.start()
    width = head.shape[2]
    for t in range(tiles):
        for r in range(TILE):
            value = taper[t * TILE + r].astype(jnp.float32)
            kinds[t, r:r + 1, :] = jnp.full((1, kinds.shape[2]), value, jnp.float32)
            if t == 0:
                head[per + 1, r:r + 1, :] = jnp.full((1, width), value, jnp.float32)
            if t == last:
                tail[per + 1, r:r + 1, :] = jnp.full((1, width), value, jnp.float32)
    p = parents[...]
    count = p.shape[1]
    owner = p // per
    inside = p - owner * per
    mine = owner == info[0]
    lo = jnp.where(mine, inside, per - 1)
    hi = jnp.where(mine, inside, 0)
    shift = 1
    while shift < per:
        lo = jnp.minimum(lo, pltpu.roll(lo, count - shift, 1))
        hi = jnp.maximum(hi, pltpu.roll(hi, count - shift, 1))
        shift *= 2
    lowest[...] = lo
    highest[...] = hi
    lane = lax.broadcasted_iota(jnp.int32, p.shape, 1) % per
    rank = jnp.zeros_like(p)
    for shift in range(1, per):
        other = jnp.where(lane + shift < per, pltpu.roll(p, count - shift, 1), pltpu.roll(p, per - shift, 1))
        rank = jnp.where((other // per == owner) & (other < p), 1, rank)
    slots[...] = owner * CAP + rank
    for c in copies:
        c.wait()


def _inner_kernel(lowest, highest, state, drive, out, field, scaled, *, mix, groups):
    per, tiles = state.shape[0], state.shape[1]
    scaled[...] = drive[...] * SCALE

    def body(k, carry):
        cur = [[state[k * mix + u, t] * SCALE for t in range(tiles)] for u in range(mix)]
        res = _steps(cur, lambda t: scaled[t], range(1, tiles - 1), -1, None)
        for u in range(mix):
            for t, v in enumerate(res[u]):
                field[k * mix + u, t] = v
        return carry

    lax.fori_loop(0, per // mix, body, 0)

    def pack(g, carry):
        for q in range(1, tiles - 1):
            for slot, table in enumerate((lowest, highest)):
                first = table[2 * q, g * per]
                second = table[2 * q + 1, g * per]
                out[g, slot, q] = _halves(field[first, q - 1], field[second, q - 1])
        return carry

    lax.fori_loop(0, groups, pack, 0)


def _edge_kernel(info, lowest, highest, state, low, high, drive, prior, out, field, scaled, *, mix, groups, bands):
    per, tiles = state.shape[0], state.shape[1]
    last = tiles - 1
    scaled[0, 0] = low[per] * SCALE
    scaled[0, 1] = drive[0] * SCALE
    scaled[0, 2] = drive[1] * SCALE
    scaled[1, 0] = drive[last - 1] * SCALE
    scaled[1, 1] = drive[last] * SCALE
    scaled[1, 2] = high[per] * SCALE
    mask = _masks(info, bands)

    def body(k, carry):
        at = [k * mix + u for u in range(mix)]
        cur = [[low[j] * SCALE, state[j, 0] * SCALE, state[j, 1] * SCALE] for j in at]
        res = _steps(cur, lambda t: scaled[0, t], [1], 0, mask[0])
        for j, r in zip(at, res):
            field[0, j] = r[0]
        cur = [[state[j, last - 1] * SCALE, state[j, last] * SCALE, high[j] * SCALE] for j in at]
        res = _steps(cur, lambda t: scaled[1, t], [1], 2, mask[1])
        for j, r in zip(at, res):
            field[1, j] = r[0]
        return carry

    lax.fori_loop(0, per // mix, body, 0)

    def pack(g, carry):
        for side in range(2):
            q = last * side
            for slot, table in enumerate((lowest, highest)):
                first = table[2 * q, g * per]
                second = table[2 * q + 1, g * per]
                out[g, slot, q] = _halves(field[side, first], field[side, second])
        return carry

    lax.fori_loop(0, groups, pack, 0)


def _masks(info, bands):
    one = jnp.float32(1.0)
    zero = jnp.float32(0.0)
    return [jnp.where(info[1] > 0, one, zero), jnp.where(info[1] < bands - 1, one, zero)]


def _choose(slots, incoming, column, q):
    a = incoming[slots[2 * q, column], q]
    b = incoming[slots[2 * q + 1, column], q]
    return _halves(a, b)


def _pick_kernel(info, slots, incoming, first, final):
    per, tiles = first.shape[0], incoming.shape[1]

    def body(j, carry):
        column = info[0] * per + j
        first[j] = _choose(slots, incoming, column, 0)
        final[j] = _choose(slots, incoming, column, tiles - 1)
        return carry

    lax.fori_loop(0, per, body, 0)


def _final_inner_kernel(info, slots, incoming, drive, kinds, out, buffer, scaled, taper, sems, *, per, mix):
    tiles, width = drive.shape[0], drive.shape[2]
    scaled[...] = drive[...] * SCALE
    for t in range(tiles):
        for c, v in enumerate(_taper(kinds[t])):
            taper[c, t] = v

    def weights(t):
        return [_widen(taper[c, t], width) for c in range(3)]

    def copy(k, hold):
        return pltpu.make_async_copy(
            buffer.at[hold], out.at[pl.ds(k * mix, mix), pl.ds(1, tiles - 2)], sems.at[hold])

    def body(k, carry):
        hold = k % 2
        cur = []
        for u in range(mix):
            column = info[0] * per + k * mix + u
            cur.append(_blend([_choose(slots, incoming, column, t) for t in range(tiles)], weights, -1, None))
        res = _steps(cur, lambda t: scaled[t], range(1, tiles - 1), -1, None)

        @pl.when(k >= 2)
        def _():
            copy(k - 2, hold).wait()

        for u in range(mix):
            for t, v in enumerate(res[u]):
                buffer[hold, u, t] = v * (1.0 / SCALE)
        copy(k, hold).start()
        return carry

    steps = per // mix
    lax.fori_loop(0, steps, body, 0)
    for k in range(steps - 2, steps):
        copy(k, k % 2).wait()


def _final_edge_kernel(info, slots, incoming, first, final, low, high, below, above, drive, kinds, prior, out,
                       buffer, scaled, taper, sems, *, per, mix, bands):
    tiles, width = drive.shape[0], drive.shape[2]
    last = tiles - 1
    both = [[(low[per], low[per + 1, :, :128]), (drive[0], kinds[0]), (drive[1], kinds[1])],
            [(drive[last - 1], kinds[last - 1]), (drive[last], kinds[last]), (high[per], high[per + 1, :, :128])]]
    for s in range(2):
        for t in range(3):
            scaled[s, t] = both[s][t][0] * SCALE
            for c, v in enumerate(_taper(both[s][t][1])):
                taper[s, c, t] = v
    mask = _masks(info, bands)

    def copy(k, hold, s):
        return pltpu.make_async_copy(buffer.at[s, hold], out.at[pl.ds(k * mix, mix), last * s], sems.at[s, hold])

    def body(k, carry):
        hold = k % 2
        for s in range(2):
            def weights(t):
                return [_widen(taper[s, c, t], width) for c in range(3)]

            cur = []
            for u in range(mix):
                j = k * mix + u
                inner = _choose(slots, incoming, info[0] * per + j, 1 if s == 0 else last - 1)
                three = [below[j], first[j], inner] if s == 0 else [inner, final[j], above[j]]
                cur.append(_blend(three, weights, 2 * s, mask[s]))
            res = _steps(cur, lambda t: scaled[s, t], [1], 2 * s, mask[s])

            @pl.when(k >= 2)
            def _():
                copy(k - 2, hold, s).wait()

            for u in range(mix):
                buffer[s, hold, u] = res[u][0] * (1.0 / SCALE)
            copy(k, hold, s).start()
        return carry

    steps = per // mix
    lax.fori_loop(0, steps, body, 0)
    for k in range(steps - 2, steps):
        for s in range(2):
            copy(k, k % 2, s).wait()


def _call(kernel, name, outs, scratch, spaces, out_spaces, alias=None):
    def spec(kind):
        return pl.BlockSpec(memory_space={"v": pltpu.VMEM, "s": pltpu.SMEM, "a": pl.ANY, "h": pltpu.HBM}[kind])

    specs = [spec(k) for k in out_spaces]
    single = len(outs) == 1
    return pl.pallas_call(
        kernel,
        in_specs=[spec(k) for k in spaces],
        out_specs=specs[0] if single else specs,
        out_shape=outs[0] if single else outs,
        scratch_shapes=scratch,
        input_output_aliases=alias or {},
        compiler_params=pltpu.CompilerParams(vmem_limit_bytes=40 * 1024 * 1024),
        name=name,
    )


def on_device(state, forcing, parents, taper_index):
    per, rows, width = state.shape
    tiles = rows // TILE
    groups = lax.axis_size("pgroup")
    bands = lax.axis_size("band")
    f32 = jnp.float32
    forward = [(i, i + 1) for i in range(bands - 1)]
    backward = [(b, a) for a, b in forward]
    info = jnp.stack([lax.axis_index("pgroup"), lax.axis_index("band")]).astype(jnp.int32)
    state4 = state.reshape(per, tiles, TILE, width)
    pinned = pltpu.with_memory_space_constraint(state4, pltpu.HBM)
    drive = forcing.reshape(tiles, TILE, width)
    entries = groups * CAP
    dma = pltpu.SemaphoreType.DMA
    vmem = pltpu.VMEM

    def shape(*dims, dtype=f32):
        return jax.ShapeDtypeStruct(dims, dtype)

    patches, count = parents.shape
    i32 = jnp.int32
    head, tail, kinds, lowest, highest, slots, state4, drive = _call(
        functools.partial(_prep_kernel, per=per, tiles=tiles), "prepare",
        [shape(per + 2, TILE, width), shape(per + 2, TILE, width), shape(tiles, TILE, 128),
         shape(patches, count, dtype=i32), shape(patches, count, dtype=i32), shape(patches, count, dtype=i32),
         shape(per, tiles, TILE, width), shape(tiles, TILE, width)],
        [dma((6,))], "sshhv", "vvvvvvvv",
    )(info, taper_index, pinned, pltpu.with_memory_space_constraint(drive, pltpu.HBM), parents)
    low = lax.ppermute(tail, "band", forward)
    high = lax.ppermute(head, "band", backward)

    message = _call(
        functools.partial(_inner_kernel, mix=2, groups=groups), "advance_inner",
        [shape(groups, CAP, tiles, TILE, width)],
        [vmem((per, tiles - 2, TILE, width), f32), vmem((tiles, TILE, width), f32)], "ssvv", "v",
    )(lowest, highest, state4, drive)
    message = _call(
        functools.partial(_edge_kernel, mix=4, groups=groups, bands=bands), "advance_edge",
        [shape(groups, CAP, tiles, TILE, width)],
        [vmem((2, per, TILE, width), f32), vmem((2, 3, TILE, width), f32)], "sssvvvvv", "v", {7: 0},
    )(info, lowest, highest, state4, low, high, drive, message)

    incoming = lax.all_to_all(message, "pgroup", split_axis=0, concat_axis=0, tiled=True)
    incoming = incoming.reshape(entries, tiles, TILE, width)

    first, final = _call(
        _pick_kernel, "pick_edge", [shape(per, TILE, width), shape(per, TILE, width)], [], "ssv", "vv",
    )(info, slots, incoming)
    below = lax.ppermute(final, "band", forward)
    above = lax.ppermute(first, "band", backward)

    field = _call(
        functools.partial(_final_inner_kernel, per=per, mix=2), "final_inner",
        [shape(per, tiles, TILE, width)],
        [vmem((2, 2, tiles - 2, TILE, width), f32), vmem((tiles, TILE, width), f32),
         vmem((3, tiles, TILE, 128), f32), dma((2,))], "ssvvv", "a",
    )(info, slots, incoming, drive, kinds)
    field = _call(
        functools.partial(_final_edge_kernel, per=per, mix=4, bands=bands), "final_edge",
        [shape(per, tiles, TILE, width)],
        [vmem((2, 2, 4, TILE, width), f32), vmem((2, 3, TILE, width), f32),
         vmem((2, 3, 3, TILE, 128), f32), dma((2, 2))], "ssvvvvvvvvva", "a", {11: 0},
    )(info, slots, incoming, first, final, low, high, below, above, drive, kinds, field)
    return field.reshape(per, rows, width)


def solution(mesh):
    return jax.shard_map(
        on_device,
        mesh=mesh,
        in_specs=(P("pgroup", "band", None), P("band", None), P("band", None), P("band")),
        out_specs=P("pgroup", "band", None),
        check_vma=False,
    )
```

```python
import functools

import jax
import jax.numpy as jnp
from jax import lax
from jax.experimental import pallas as pl
from jax.experimental.pallas import tpu as pltpu
from jax.sharding import PartitionSpec as P

PATCH_ROWS = 4
STEPS = 6
CAP = 2
TILE = 8
SCALE = 0.05


def _sub(shape):
    return lax.broadcasted_iota(jnp.int32, shape, 0)


def _up(tiles, i, k):
    here = tiles[i]
    after = tiles[min(i + 1, len(tiles) - 1)]
    return pltpu.roll(jnp.where(_sub(here.shape) < k, after, here), TILE - k, 0)


def _down(tiles, i, k):
    here = tiles[i]
    before = tiles[max(i - 1, 0)]
    return pltpu.roll(jnp.where(_sub(here.shape) >= TILE - k, before, here), k, 0)


def _step(tiles, i, drive):
    m = tiles[i]
    width = m.shape[1]
    e = pltpu.roll(m, width - 1, 1)
    w = pltpu.roll(m, 1, 1)
    n = _up(tiles, i, 1)
    s = _down(tiles, i, 1)
    return (m * (0.4 - (e - w)) + 0.15 * (e + w)) + (0.05 * n + 0.25 * s) + drive


def _steps(groups, drive, keep, masks):
    for repeat in range(STEPS):
        todo = keep if repeat == STEPS - 1 else range(len(groups[0]))
        fresh = [list(tiles) for tiles in groups]
        for i in todo:
            source = drive(i)
            for tiles, new in zip(groups, fresh):
                v = _step(tiles, i, source)
                new[i] = v * masks[i] if i in masks else v
        groups = fresh
    return [[tiles[i] for i in keep] for tiles in groups]


def _blend(tiles, weights, masks):
    fresh = []
    for i in range(len(tiles)):
        w0, w1, w2 = weights(i)
        total = w0 * tiles[i]
        total = total + w1 * (_up(tiles, i, 1) + _down(tiles, i, 1))
        total = total + w2 * (_up(tiles, i, 2) + _down(tiles, i, 2))
        fresh.append(total * masks[i] if i in masks else total)
    return fresh


def _taper(kind):
    rate = 0.2 * (kind + 1.0)
    near = jnp.exp(-rate)
    far = jnp.exp(-4.0 * rate)
    inv = 1.0 / (far + near + 1.0 + near + far)
    return inv, near * inv, far * inv


def _halves(a, b):
    return jnp.where(_sub(a.shape) < PATCH_ROWS, a, b)


def _widen(v, width):
    return jnp.concatenate([v] * (width // v.shape[1]), axis=1)


def _prep_kernel(info, taper, state, forcing, parents, head, tail, kinds, ends, slots, local, drive, sems,
                 *, per, tiles):
    last = tiles - 1
    copies = [
        pltpu.make_async_copy(state.at[:, 0], head.at[pl.ds(0, per)], sems.at[0]),
        pltpu.make_async_copy(state.at[:, last], tail.at[pl.ds(0, per)], sems.at[1]),
        pltpu.make_async_copy(forcing.at[0], head.at[per], sems.at[2]),
        pltpu.make_async_copy(forcing.at[last], tail.at[per], sems.at[3]),
        pltpu.make_async_copy(forcing, drive, sems.at[4]),
        pltpu.make_async_copy(state, local, sems.at[5]),
    ]
    for c in copies:
        c.start()
    width = head.shape[2]
    for t in range(tiles):
        for r in range(TILE):
            value = taper[t * TILE + r].astype(jnp.float32)
            kinds[t, r:r + 1, :] = jnp.full((1, kinds.shape[2]), value, jnp.float32)
            if t == 0:
                head[per + 1, r:r + 1, :] = jnp.full((1, width), value, jnp.float32)
            if t == last:
                tail[per + 1, r:r + 1, :] = jnp.full((1, width), value, jnp.float32)
    p = parents[...]
    count = p.shape[1]
    owner = p // per
    inside = p - owner * per
    mine = owner == info[0]
    lo = jnp.where(mine, inside, per - 1)
    hi = jnp.where(mine, inside, 0)
    shift = 1
    while shift < per:
        lo = jnp.minimum(lo, pltpu.roll(lo, count - shift, 1))
        hi = jnp.maximum(hi, pltpu.roll(hi, count - shift, 1))
        shift *= 2
    ends[0] = lo
    ends[1] = hi
    lane = lax.broadcasted_iota(jnp.int32, p.shape, 1) % per
    rank = jnp.zeros_like(p)
    for shift in range(1, per):
        other = jnp.where(lane + shift < per, pltpu.roll(p, count - shift, 1), pltpu.roll(p, per - shift, 1))
        rank = jnp.where((other // per == owner) & (other < p), 1, rank)
    slots[...] = owner * CAP + rank
    for c in copies:
        c.wait()


def _inner_kernel(ends, state, drive, out, field, scaled, *, mix, groups):
    per, tiles = state.shape[0], state.shape[1]
    scaled[...] = drive[...] * SCALE

    def body(k, carry):
        cur = [[state[k * mix + u, t] * SCALE for t in range(tiles)] for u in range(mix)]
        res = _steps(cur, lambda t: scaled[t], range(1, tiles - 1), {})
        for u in range(mix):
            for t, v in enumerate(res[u]):
                field[k * mix + u, t] = v
        return carry

    lax.fori_loop(0, per // mix, body, 0)

    def pack(g, carry):
        for q in range(1, tiles - 1):
            for slot in range(CAP):
                first = ends[slot, 2 * q, g * per]
                second = ends[slot, 2 * q + 1, g * per]
                out[g, slot, q - 1] = _halves(field[first, q - 1], field[second, q - 1])
        return carry

    lax.fori_loop(0, groups, pack, 0)


def _edge_kernel(info, ends, state, low, high, forcing, kinds, after, *rest, mix, side, bands):
    outs, (scaled, taper), (field, near, sems) = rest[:-5], rest[-5:-3], rest[-3:]
    per, tiles = state.shape[0], state.shape[1]
    last = tiles - 1
    count = tiles + 2
    loads = [
        pltpu.make_async_copy(state.at[:, pl.ds(0, 2)], near.at[0], sems.at[0]),
        pltpu.make_async_copy(state.at[:, pl.ds(last - 1, 2)], near.at[1], sems.at[1]),
        pltpu.make_async_copy(forcing, scaled.at[pl.ds(1, tiles)], sems.at[2]),
    ]
    for c in loads:
        c.start()
    scaled[0] = low[per]
    scaled[count - 1] = high[per]
    for t in range(count):
        kind = low[per + 1, :, :128] if t == 0 else high[per + 1, :, :128] if t == count - 1 else kinds[t - 1]
        for c, v in enumerate(_taper(kind)):
            taper[c, t] = v
    for c in loads:
        c.wait()
    scaled[...] = scaled[...] * SCALE
    mask = _masks(info, bands)

    def body(k, carry):
        at = [k * mix + u for u in range(mix)]
        cur = [[low[j] * SCALE, near[0, j, 0] * SCALE, near[0, j, 1] * SCALE] for j in at]
        res = _steps(cur, lambda t: scaled[t], [1], {0: mask[0]})
        for j, r in zip(at, res):
            field[0, j] = r[0]
        cur = [[near[1, j, 0] * SCALE, near[1, j, 1] * SCALE, high[j] * SCALE] for j in at]
        res = _steps(cur, lambda t: scaled[last + t], [1], {2: mask[1]})
        for j, r in zip(at, res):
            field[1, j] = r[0]
        return carry

    lax.fori_loop(0, per // mix, body, 0)

    for k, out in enumerate(outs):
        g = _peer(info, k, side, 1)
        for end in range(2):
            q = last * end
            for slot in range(CAP):
                first = ends[slot, 2 * q, g * per]
                second = ends[slot, 2 * q + 1, g * per]
                out[slot, end] = _halves(field[end, first], field[end, second])


def _peer(info, k, side, sign):
    row, column = k // side, k % side
    mine_row, mine_column = info[0] // side, info[0] % side
    return ((mine_row + sign * row + side) % side) * side + (mine_column + sign * column + side) % side


def _masks(info, bands):
    one = jnp.float32(1.0)
    zero = jnp.float32(0.0)
    return [jnp.where(info[1] > 0, one, zero), jnp.where(info[1] < bands - 1, one, zero)]


def _choose(slots, incoming, column, patch, q):
    a = incoming[slots[2 * patch, column], q]
    b = incoming[slots[2 * patch + 1, column], q]
    return _halves(a, b)


def _pick_kernel(info, slots, *rest, last, side):
    received, (first, final, incoming) = rest[:-3], rest[-3:]
    per = first.shape[0]
    for k, block in enumerate(received):
        g = _peer(info, k, side, -1)
        for slot in range(CAP):
            incoming[g * CAP + slot] = block[slot]

    def body(j, carry):
        column = info[0] * per + j
        first[j] = _choose(slots, incoming, column, 0, 0)
        final[j] = _choose(slots, incoming, column, last, 1)
        return carry

    lax.fori_loop(0, per, body, 0)


def _final_kernel(info, slots, incoming, first_in, final_in, below_in, above_in, scaled_in, taper_in, out,
                  buffer, ends, scaled, taper, sems, *, per, tiles, mix, bands):
    count = tiles + 2
    width = scaled.shape[2]
    loads = [pltpu.make_async_copy(source, ends.at[n], sems.at[2 + n])
             for n, source in enumerate((below_in, first_in, final_in, above_in))]
    loads += [pltpu.make_async_copy(scaled_in, scaled, sems.at[6]), pltpu.make_async_copy(taper_in, taper, sems.at[7])]
    for c in loads:
        c.start()
    for c in loads:
        c.wait()
    mask = _masks(info, bands)
    masks = {0: mask[0], count - 1: mask[1]}

    def weights(t):
        return [_widen(taper[c, t], width) for c in range(3)]

    def copy(k, hold):
        return pltpu.make_async_copy(buffer.at[hold], out.at[pl.ds(k * mix, mix)], sems.at[hold])

    def body(k, carry):
        hold = k % 2
        cur = []
        for u in range(mix):
            j = k * mix + u
            column = info[0] * per + j
            mine = [ends[0, j], ends[1, j]]
            mine += [_choose(slots, incoming, column, t, t - 1) for t in range(1, tiles - 1)]
            mine += [ends[2, j], ends[3, j]]
            cur.append(_blend(mine, weights, masks))
        res = _steps(cur, lambda t: scaled[t], range(1, count - 1), masks)

        @pl.when(k >= 2)
        def _():
            copy(k - 2, hold).wait()

        for u in range(mix):
            for t, v in enumerate(res[u]):
                buffer[hold, u, t] = v * (1.0 / SCALE)
        copy(k, hold).start()
        return carry

    steps = per // mix
    lax.fori_loop(0, steps, body, 0)
    for k in range(steps - 2, steps):
        copy(k, k % 2).wait()


def _pin(x):
    return pltpu.with_memory_space_constraint(x, pltpu.HBM)


def _call(kernel, name, outs, scratch, spaces, out_spaces, alias=None):
    def spec(kind):
        return pl.BlockSpec(memory_space={"v": pltpu.VMEM, "s": pltpu.SMEM, "a": pl.ANY, "h": pltpu.HBM}[kind])

    specs = [spec(k) for k in out_spaces]
    single = len(outs) == 1
    return pl.pallas_call(
        kernel,
        in_specs=[spec(k) for k in spaces],
        out_specs=specs[0] if single else specs,
        out_shape=outs[0] if single else outs,
        scratch_shapes=scratch,
        input_output_aliases=alias or {},
        compiler_params=pltpu.CompilerParams(vmem_limit_bytes=40 * 1024 * 1024),
        name=name,
    )


def on_device(state, forcing, parents, taper_index):
    per, rows, width = state.shape
    tiles = rows // TILE
    groups = lax.axis_size("pgroup")
    bands = lax.axis_size("band")
    f32 = jnp.float32
    forward = [(i, i + 1) for i in range(bands - 1)]
    backward = [(b, a) for a, b in forward]
    info = jnp.stack([lax.axis_index("pgroup"), lax.axis_index("band")]).astype(jnp.int32)
    state4 = _pin(state.reshape(per, tiles, TILE, width))
    forcing4 = _pin(forcing.reshape(tiles, TILE, width))
    entries = groups * CAP
    dma = pltpu.SemaphoreType.DMA
    vmem = pltpu.VMEM

    def shape(*dims, dtype=f32):
        return jax.ShapeDtypeStruct(dims, dtype)

    patches, count = parents.shape
    i32 = jnp.int32
    head, tail, kinds, ends, slots, local, drive = _call(
        functools.partial(_prep_kernel, per=per, tiles=tiles), "prepare",
        [shape(per + 2, TILE, width), shape(per + 2, TILE, width), shape(tiles, TILE, 128),
         shape(CAP, patches, count, dtype=i32), shape(patches, count, dtype=i32),
         shape(per, tiles, TILE, width), shape(tiles, TILE, width)],
        [dma((6,))], "sshhv", "vvvvvvv",
    )(info, taper_index, state4, forcing4, parents)
    low = lax.ppermute(tail, "band", forward)
    high = lax.ppermute(head, "band", backward)

    inner = tiles - 2
    message = _call(
        functools.partial(_inner_kernel, mix=2, groups=groups), "advance_inner",
        [shape(groups, CAP, inner, TILE, width)],
        [vmem((per, inner, TILE, width), f32), vmem((tiles, TILE, width), f32)], "svv", "v",
    )(ends, local, drive)
    message, low, high = lax.optimization_barrier((message, low, high))
    incoming = lax.all_to_all(message, "pgroup", split_axis=0, concat_axis=0, tiled=True)
    incoming = incoming.reshape(entries, inner, TILE, width)

    side = int(groups ** 0.5)
    *edges, scaled, taper = _call(
        functools.partial(_edge_kernel, mix=4, side=side, bands=bands), "advance_edge",
        [shape(CAP, 2, TILE, width)] * groups + [shape(tiles + 2, TILE, width), shape(3, tiles + 2, TILE, 128)],
        [vmem((2, per, TILE, width), f32), vmem((2, per, 2, TILE, width), f32), dma((3,))],
        "sshvvhva", "v" * (groups + 2),
    )(info, _pin(ends), state4, low, high, forcing4, kinds, message)
    received = [edges[0]]
    for k in range(1, groups):
        pairs = []
        for g in range(groups):
            row, column = (g // side + k // side) % side, (g % side + k % side) % side
            pairs.append((g, row * side + column))
        received.append(lax.ppermute(edges[k], "pgroup", pairs))

    first, final = _call(
        functools.partial(_pick_kernel, last=tiles - 1, side=side), "pick_edge",
        [shape(per, TILE, width), shape(per, TILE, width)],
        [vmem((entries, 2, TILE, width), f32)], "ss" + "v" * groups, "vv",
    )(info, _pin(slots), *received)
    below = lax.ppermute(final, "band", forward)
    above = lax.ppermute(first, "band", backward)

    field = _call(
        functools.partial(_final_kernel, per=per, tiles=tiles, mix=2, bands=bands), "final",
        [shape(per, tiles, TILE, width)],
        [vmem((2, 2, tiles, TILE, width), f32), vmem((4, per, TILE, width), f32), vmem((tiles + 2, TILE, width), f32),
         vmem((3, tiles + 2, TILE, 128), f32), dma((8,))], "ssvhhhhhh", "a",
    )(info, _pin(slots), incoming, *[_pin(x) for x in (first, final, below, above, scaled, taper)])
    return field.reshape(per, rows, width)


def solution(mesh):
    return jax.shard_map(
        on_device,
        mesh=mesh,
        in_specs=(P("pgroup", "band", None), P("band", None), P("band", None), P("band")),
        out_specs=P("pgroup", "band", None),
        check_vma=False,
    )
```

```python
import functools

import jax
import jax.numpy as jnp
from jax import lax
from jax.experimental import pallas as pl
from jax.experimental.pallas import tpu as pltpu
from jax.sharding import PartitionSpec as P

PATCH_ROWS = 4
STEPS = 6
CAP = 2
TILE = 8
SCALE = 0.05


def _sub(shape):
    return lax.broadcasted_iota(jnp.int32, shape, 0)


def _up(tiles, i, k):
    here = tiles[i]
    after = tiles[min(i + 1, len(tiles) - 1)]
    return pltpu.roll(jnp.where(_sub(here.shape) < k, after, here), TILE - k, 0)


def _down(tiles, i, k):
    here = tiles[i]
    before = tiles[max(i - 1, 0)]
    return pltpu.roll(jnp.where(_sub(here.shape) >= TILE - k, before, here), k, 0)


def _step(tiles, i, drive):
    m = tiles[i]
    width = m.shape[1]
    e = pltpu.roll(m, width - 1, 1)
    w = pltpu.roll(m, 1, 1)
    n = _up(tiles, i, 1)
    s = _down(tiles, i, 1)
    return (m * (0.4 - (e - w)) + 0.15 * (e + w)) + (0.05 * n + 0.25 * s) + drive


def _steps(groups, drive, keep, masks):
    for repeat in range(STEPS):
        todo = keep if repeat == STEPS - 1 else range(len(groups[0]))
        fresh = [list(tiles) for tiles in groups]
        for i in todo:
            source = drive(i)
            for tiles, new in zip(groups, fresh):
                v = _step(tiles, i, source)
                new[i] = v * masks[i] if i in masks else v
        groups = fresh
    return [[tiles[i] for i in keep] for tiles in groups]


def _blend(tiles, weights, masks):
    fresh = []
    for i in range(len(tiles)):
        w0, w1, w2 = weights(i)
        total = w0 * tiles[i]
        total = total + w1 * (_up(tiles, i, 1) + _down(tiles, i, 1))
        total = total + w2 * (_up(tiles, i, 2) + _down(tiles, i, 2))
        fresh.append(total * masks[i] if i in masks else total)
    return fresh


def _taper(kind):
    rate = 0.2 * (kind + 1.0)
    near = jnp.exp(-rate)
    far = jnp.exp(-4.0 * rate)
    inv = 1.0 / (far + near + 1.0 + near + far)
    return inv, near * inv, far * inv


def _halves(a, b):
    return jnp.where(_sub(a.shape) < PATCH_ROWS, a, b)


def _widen(v, width):
    return jnp.concatenate([v] * (width // v.shape[1]), axis=1)


def _prep_kernel(info, taper_in, state, forcing, parents_in, head, tail, kinds, lowest, highest, slots, local, drive,
                 taper, parents, sems, *, per, tiles):
    last = tiles - 1
    copies = [
        pltpu.make_async_copy(state.at[:, 0], head.at[pl.ds(0, per)], sems.at[0]),
        pltpu.make_async_copy(state.at[:, last], tail.at[pl.ds(0, per)], sems.at[1]),
        pltpu.make_async_copy(forcing.at[0], head.at[per], sems.at[2]),
        pltpu.make_async_copy(forcing.at[last], tail.at[per], sems.at[3]),
        pltpu.make_async_copy(forcing, drive, sems.at[4]),
        pltpu.make_async_copy(state, local, sems.at[5]),
    ]
    first = [pltpu.make_async_copy(parents_in, parents, sems.at[6]), pltpu.make_async_copy(taper_in, taper, sems.at[7])]
    for c in first + copies:
        c.start()
    for c in first:
        c.wait()
    width = head.shape[2]
    for t in range(tiles):
        for r in range(TILE):
            value = taper[t * TILE + r].astype(jnp.float32)
            kinds[t, r:r + 1, :] = jnp.full((1, kinds.shape[2]), value, jnp.float32)
            if t == 0:
                head[per + 1, r:r + 1, :] = jnp.full((1, width), value, jnp.float32)
            if t == last:
                tail[per + 1, r:r + 1, :] = jnp.full((1, width), value, jnp.float32)
    p = parents[...]
    count = p.shape[1]
    owner = p // per
    inside = p - owner * per
    mine = owner == info[0]
    lo = jnp.where(mine, inside, per - 1)
    hi = jnp.where(mine, inside, 0)
    shift = 1
    while shift < per:
        lo = jnp.minimum(lo, pltpu.roll(lo, count - shift, 1))
        hi = jnp.maximum(hi, pltpu.roll(hi, count - shift, 1))
        shift *= 2
    lowest[...] = lo
    highest[...] = hi
    lane = lax.broadcasted_iota(jnp.int32, p.shape, 1) % per
    rank = jnp.zeros_like(p)
    for shift in range(1, per):
        other = jnp.where(lane + shift < per, pltpu.roll(p, count - shift, 1), pltpu.roll(p, per - shift, 1))
        rank = jnp.where((other // per == owner) & (other < p), 1, rank)
    slots[...] = owner * CAP + rank
    for c in copies:
        c.wait()


def _inner_kernel(state, drive, field, scaled, *, mix, half):
    tiles = state.shape[1]
    scaled[...] = drive[...] * SCALE

    def body(k, carry):
        cur = [[state[k * mix + u, t] * SCALE for t in range(tiles)] for u in range(mix)]
        res = _steps(cur, lambda t: scaled[t], range(1, tiles - 1), {})
        for u in range(mix):
            for t, v in enumerate(res[u]):
                field[k * mix + u, t + 1] = v
        return carry

    lax.fori_loop(0, half // mix, body, 0)


def _rest_kernel(info, lowest, highest, state, low, high, drive, prior, out, field, scaled, *, mix, edge_mix, half,
                 groups, bands):
    per, tiles = state.shape[0], state.shape[1]
    last = tiles - 1
    count = tiles + 2
    scaled[0] = low[per] * SCALE
    scaled[count - 1] = high[per] * SCALE
    for t in range(tiles):
        scaled[t + 1] = drive[t] * SCALE
    mask = _masks(info, bands)

    def edge(k, carry):
        at = [k * edge_mix + u for u in range(edge_mix)]
        cur = [[low[j] * SCALE, state[j, 0] * SCALE, state[j, 1] * SCALE] for j in at]
        res = _steps(cur, lambda t: scaled[t], [1], {0: mask[0]})
        for j, r in zip(at, res):
            field[j, 0] = r[0]
        cur = [[state[j, last - 1] * SCALE, state[j, last] * SCALE, high[j] * SCALE] for j in at]
        res = _steps(cur, lambda t: scaled[last + t], [1], {2: mask[1]})
        for j, r in zip(at, res):
            field[j, last] = r[0]
        return carry

    def whole(k, carry):
        at = [half + k * mix + u for u in range(mix)]
        cur = [[low[j] * SCALE] + [state[j, t] * SCALE for t in range(tiles)] + [high[j] * SCALE] for j in at]
        res = _steps(cur, lambda t: scaled[t], range(1, count - 1), {0: mask[0], count - 1: mask[1]})
        for j, r in zip(at, res):
            for t, v in enumerate(r):
                field[j, t] = v
        return carry

    lax.fori_loop(0, half // edge_mix, edge, 0)
    for j in range(half):
        for t in range(1, last):
            field[j, t] = prior[j, t]
    lax.fori_loop(0, (per - half) // mix, whole, 0)

    def pack(g, carry):
        for q in range(tiles):
            for slot, table in enumerate((lowest, highest)):
                first = table[2 * q, g * per]
                second = table[2 * q + 1, g * per]
                out[g, slot, q] = _halves(field[first, q], field[second, q])
        return carry

    lax.fori_loop(0, groups, pack, 0)


def _masks(info, bands):
    one = jnp.float32(1.0)
    zero = jnp.float32(0.0)
    return [jnp.where(info[1] > 0, one, zero), jnp.where(info[1] < bands - 1, one, zero)]


def _choose(slots, incoming, column, q):
    a = incoming[slots[2 * q, column], q]
    b = incoming[slots[2 * q + 1, column], q]
    return _halves(a, b)


def _pick_kernel(info, slots, incoming, first, final):
    per, tiles = first.shape[0], incoming.shape[1]

    def body(j, carry):
        column = info[0] * per + j
        first[j] = _choose(slots, incoming, column, 0)
        final[j] = _choose(slots, incoming, column, tiles - 1)
        return carry

    lax.fori_loop(0, per, body, 0)


def _final_inner_kernel(info, slots, incoming, drive, kinds, out, buffer, scaled, taper, sems, *, per, half, mix):
    tiles, width = drive.shape[0], drive.shape[2]
    scaled[...] = drive[...] * SCALE
    for t in range(tiles):
        for c, v in enumerate(_taper(kinds[t])):
            taper[c, t] = v

    def weights(t):
        return [_widen(taper[c, t], width) for c in range(3)]

    def copy(k, hold):
        return pltpu.make_async_copy(
            buffer.at[hold], out.at[pl.ds(k * mix, mix), pl.ds(1, tiles - 2)], sems.at[hold])

    def body(k, carry):
        hold = k % 2
        cur = []
        for u in range(mix):
            column = info[0] * per + k * mix + u
            cur.append(_blend([_choose(slots, incoming, column, t) for t in range(tiles)], weights, {}))
        res = _steps(cur, lambda t: scaled[t], range(1, tiles - 1), {})

        @pl.when(k >= 2)
        def _():
            copy(k - 2, hold).wait()

        for u in range(mix):
            for t, v in enumerate(res[u]):
                buffer[hold, u, t] = v * (1.0 / SCALE)
        copy(k, hold).start()
        return carry

    steps = half // mix
    lax.fori_loop(0, steps, body, 0)
    for k in range(steps - 2, steps):
        copy(k, k % 2).wait()


def _final_rest_kernel(info, slots, incoming, first, final, low, high, below, above, drive, kinds, prior, out,
                       edges, buffer, scaled, taper, sems, *, per, half, mix, edge_mix, bands):
    tiles, width = drive.shape[0], drive.shape[2]
    last = tiles - 1
    count = tiles + 2
    scaled[0] = low[per] * SCALE
    scaled[count - 1] = high[per] * SCALE
    for t in range(tiles):
        scaled[t + 1] = drive[t] * SCALE
    for t in range(count):
        kind = low[per + 1, :, :128] if t == 0 else high[per + 1, :, :128] if t == count - 1 else kinds[t - 1]
        for c, v in enumerate(_taper(kind)):
            taper[c, t] = v
    mask = _masks(info, bands)

    def weights_from(start):
        return lambda t: [_widen(taper[c, start + t], width) for c in range(3)]

    def ends(s):
        return pltpu.make_async_copy(edges.at[s], out.at[pl.ds(0, half), last * s], sems.at[2 + s])

    def edge(k, carry):
        for s in range(2):
            start = last * s
            cur = []
            for u in range(edge_mix):
                j = k * edge_mix + u
                inner = _choose(slots, incoming, info[0] * per + j, 1 if s == 0 else last - 1)
                three = [below[j], first[j], inner] if s == 0 else [inner, final[j], above[j]]
                cur.append(_blend(three, weights_from(start), {2 * s: mask[s]}))
            res = _steps(cur, lambda t: scaled[start + t], [1], {2 * s: mask[s]})
            for u in range(edge_mix):
                edges[s, k * edge_mix + u] = res[u][0] * (1.0 / SCALE)
        return carry

    lax.fori_loop(0, half // edge_mix, edge, 0)
    for s in range(2):
        ends(s).start()

    masks = {0: mask[0], count - 1: mask[1]}

    def copy(k, hold):
        return pltpu.make_async_copy(buffer.at[hold], out.at[pl.ds(half + k * mix, mix)], sems.at[hold])

    def whole(k, carry):
        hold = k % 2
        cur = []
        for u in range(mix):
            j = half + k * mix + u
            column = info[0] * per + j
            mine = [below[j], first[j]]
            mine += [_choose(slots, incoming, column, t) for t in range(1, last)]
            mine += [final[j], above[j]]
            cur.append(_blend(mine, weights_from(0), masks))
        res = _steps(cur, lambda t: scaled[t], range(1, count - 1), masks)

        @pl.when(k >= 2)
        def _():
            copy(k - 2, hold).wait()

        for u in range(mix):
            for t, v in enumerate(res[u]):
                buffer[hold, u, t] = v * (1.0 / SCALE)
        copy(k, hold).start()
        return carry

    steps = (per - half) // mix
    lax.fori_loop(0, steps, whole, 0)
    for k in range(steps - 2, steps):
        copy(k, k % 2).wait()
    for s in range(2):
        ends(s).wait()


def _pin(x):
    return pltpu.with_memory_space_constraint(x, pltpu.HBM)


def _call(kernel, name, outs, scratch, spaces, out_spaces, alias=None):
    def spec(kind):
        return pl.BlockSpec(memory_space={"v": pltpu.VMEM, "s": pltpu.SMEM, "a": pl.ANY, "h": pltpu.HBM}[kind])

    specs = [spec(k) for k in out_spaces]
    single = len(outs) == 1
    return pl.pallas_call(
        kernel,
        in_specs=[spec(k) for k in spaces],
        out_specs=specs[0] if single else specs,
        out_shape=outs[0] if single else outs,
        scratch_shapes=scratch,
        input_output_aliases=alias or {},
        compiler_params=pltpu.CompilerParams(vmem_limit_bytes=40 * 1024 * 1024),
        name=name,
    )


def on_device(state, forcing, parents, taper_index):
    per, rows, width = state.shape
    tiles = rows // TILE
    groups = lax.axis_size("pgroup")
    bands = lax.axis_size("band")
    f32 = jnp.float32
    forward = [(i, i + 1) for i in range(bands - 1)]
    backward = [(b, a) for a, b in forward]
    info = jnp.stack([lax.axis_index("pgroup"), lax.axis_index("band")]).astype(jnp.int32)
    state4 = state.reshape(per, tiles, TILE, width)
    pinned = _pin(state4)
    drive = forcing.reshape(tiles, TILE, width)
    entries = groups * CAP
    dma = pltpu.SemaphoreType.DMA
    vmem = pltpu.VMEM

    def shape(*dims, dtype=f32):
        return jax.ShapeDtypeStruct(dims, dtype)

    patches, count = parents.shape
    i32 = jnp.int32
    head, tail, kinds, lowest, highest, slots, state4, drive = _call(
        functools.partial(_prep_kernel, per=per, tiles=tiles), "prepare",
        [shape(per + 2, TILE, width), shape(per + 2, TILE, width), shape(tiles, TILE, 128),
         shape(patches, count, dtype=i32), shape(patches, count, dtype=i32), shape(patches, count, dtype=i32),
         shape(per, tiles, TILE, width), shape(tiles, TILE, width)],
        [pltpu.SMEM((rows,), i32), vmem((patches, count), i32), dma((8,))], "shhhh", "vvvvvvvv",
    )(info, _pin(taper_index), pinned, _pin(drive), _pin(parents))
    low = lax.ppermute(tail, "band", forward)
    high = lax.ppermute(head, "band", backward)

    half = per // 2
    field = _call(
        functools.partial(_inner_kernel, mix=2, half=half), "advance_inner",
        [shape(half, tiles, TILE, width)], [vmem((tiles, TILE, width), f32)], "vv", "v",
    )(state4, drive)
    message = _call(
        functools.partial(_rest_kernel, mix=2, edge_mix=4, half=half, groups=groups, bands=bands), "advance_rest",
        [shape(groups, CAP, tiles, TILE, width)],
        [vmem((per, tiles, TILE, width), f32), vmem((tiles + 2, TILE, width), f32)], "sssvvvvv", "v",
    )(info, lowest, highest, state4, low, high, drive, field)

    incoming = lax.all_to_all(message, "pgroup", split_axis=0, concat_axis=0, tiled=True)
    incoming = incoming.reshape(entries, tiles, TILE, width)

    first, final = _call(
        _pick_kernel, "pick_edge", [shape(per, TILE, width), shape(per, TILE, width)], [], "ssv", "vv",
    )(info, slots, incoming)
    below = lax.ppermute(final, "band", forward)
    above = lax.ppermute(first, "band", backward)

    field = _call(
        functools.partial(_final_inner_kernel, per=per, half=half, mix=2), "final_inner",
        [shape(per, tiles, TILE, width)],
        [vmem((2, 2, tiles - 2, TILE, width), f32), vmem((tiles, TILE, width), f32),
         vmem((3, tiles, TILE, 128), f32), dma((2,))], "ssvvv", "a",
    )(info, slots, incoming, drive, kinds)
    field = _call(
        functools.partial(_final_rest_kernel, per=per, half=half, mix=2, edge_mix=4, bands=bands), "final_rest",
        [shape(per, tiles, TILE, width)],
        [vmem((2, half, TILE, width), f32), vmem((2, 2, tiles, TILE, width), f32), vmem((tiles + 2, TILE, width), f32),
         vmem((3, tiles + 2, TILE, 128), f32), dma((4,))], "ssvvvvvvvvva", "a", {11: 0},
    )(info, slots, incoming, first, final, low, high, below, above, drive, kinds, field)
    return field.reshape(per, rows, width)


def solution(mesh):
    return jax.shard_map(
        on_device,
        mesh=mesh,
        in_specs=(P("pgroup", "band", None), P("band", None), P("band", None), P("band")),
        out_specs=P("pgroup", "band", None),
        check_vma=False,
    )
```

```python
import functools

import jax
import jax.numpy as jnp
from jax import lax
from jax.experimental import pallas as pl
from jax.experimental.pallas import tpu as pltpu
from jax.sharding import PartitionSpec as P

PATCH_ROWS = 4
STEPS = 6
CAP = 2
TILE = 8
SCALE = 0.05
LATE = (5, 6)


def _sub(shape):
    return lax.broadcasted_iota(jnp.int32, shape, 0)


def _up(tiles, i, k):
    here = tiles[i]
    after = tiles[min(i + 1, len(tiles) - 1)]
    return pltpu.roll(jnp.where(_sub(here.shape) < k, after, here), TILE - k, 0)


def _down(tiles, i, k):
    here = tiles[i]
    before = tiles[max(i - 1, 0)]
    return pltpu.roll(jnp.where(_sub(here.shape) >= TILE - k, before, here), k, 0)


def _step(tiles, i, drive):
    m = tiles[i]
    width = m.shape[1]
    e = pltpu.roll(m, width - 1, 1)
    w = pltpu.roll(m, 1, 1)
    n = _up(tiles, i, 1)
    s = _down(tiles, i, 1)
    return (m * (0.4 - (e - w)) + 0.15 * (e + w)) + (0.05 * n + 0.25 * s) + drive


def _steps(groups, drive, keep, masks):
    for repeat in range(STEPS):
        todo = keep if repeat == STEPS - 1 else range(len(groups[0]))
        fresh = [list(tiles) for tiles in groups]
        for i in todo:
            source = drive(i)
            for tiles, new in zip(groups, fresh):
                v = _step(tiles, i, source)
                new[i] = v * masks[i] if i in masks else v
        groups = fresh
    return [[tiles[i] for i in keep] for tiles in groups]


def _blend(tiles, weights, masks):
    fresh = []
    for i in range(len(tiles)):
        w0, w1, w2 = weights(i)
        total = w0 * tiles[i]
        total = total + w1 * (_up(tiles, i, 1) + _down(tiles, i, 1))
        total = total + w2 * (_up(tiles, i, 2) + _down(tiles, i, 2))
        fresh.append(total * masks[i] if i in masks else total)
    return fresh


def _taper(kind):
    rate = 0.2 * (kind + 1.0)
    near = jnp.exp(-rate)
    far = jnp.exp(-4.0 * rate)
    inv = 1.0 / (far + near + 1.0 + near + far)
    return inv, near * inv, far * inv


def _halves(a, b):
    return jnp.where(_sub(a.shape) < PATCH_ROWS, a, b)


def _widen(v, width):
    return jnp.concatenate([v] * (width // v.shape[1]), axis=1)


def _prep_kernel(info, taper_in, state, forcing, parents_in, head, tail, kinds, lowest, highest, slots, local, drive,
                 taper, parents, sems, *, per, tiles):
    last = tiles - 1
    copies = [
        pltpu.make_async_copy(state.at[:, 0], head.at[pl.ds(0, per)], sems.at[0]),
        pltpu.make_async_copy(state.at[:, last], tail.at[pl.ds(0, per)], sems.at[1]),
        pltpu.make_async_copy(forcing.at[0], head.at[per], sems.at[2]),
        pltpu.make_async_copy(forcing.at[last], tail.at[per], sems.at[3]),
        pltpu.make_async_copy(forcing, drive, sems.at[4]),
        pltpu.make_async_copy(state, local, sems.at[5]),
    ]
    first = [pltpu.make_async_copy(parents_in, parents, sems.at[6]), pltpu.make_async_copy(taper_in, taper, sems.at[7])]
    for c in first + copies:
        c.start()
    for c in first:
        c.wait()
    width = head.shape[2]
    for t in range(tiles):
        for r in range(TILE):
            value = taper[t * TILE + r].astype(jnp.float32)
            kinds[t, r:r + 1, :] = jnp.full((1, kinds.shape[2]), value, jnp.float32)
            if t == 0:
                head[per + 1, r:r + 1, :] = jnp.full((1, width), value, jnp.float32)
            if t == last:
                tail[per + 1, r:r + 1, :] = jnp.full((1, width), value, jnp.float32)
    p = parents[...]
    count = p.shape[1]
    owner = p // per
    inside = p - owner * per
    mine = owner == info[0]
    lo = jnp.where(mine, inside, per - 1)
    hi = jnp.where(mine, inside, 0)
    shift = 1
    while shift < per:
        lo = jnp.minimum(lo, pltpu.roll(lo, count - shift, 1))
        hi = jnp.maximum(hi, pltpu.roll(hi, count - shift, 1))
        shift *= 2
    lowest[...] = lo
    highest[...] = hi
    lane = lax.broadcasted_iota(jnp.int32, p.shape, 1) % per
    rank = jnp.zeros_like(p)
    for shift in range(1, per):
        other = jnp.where(lane + shift < per, pltpu.roll(p, count - shift, 1), pltpu.roll(p, per - shift, 1))
        rank = jnp.where((other // per == owner) & (other < p), 1, rank)
    slots[...] = owner * CAP + rank
    for c in copies:
        c.wait()


def _inner_kernel(state, drive, field, scaled, *, mix, half):
    tiles = state.shape[1]
    scaled[...] = drive[...] * SCALE

    def body(k, carry):
        cur = [[state[k * mix + u, t] * SCALE for t in range(tiles)] for u in range(mix)]
        res = _steps(cur, lambda t: scaled[t], range(1, tiles - 1), {})
        for u in range(mix):
            for t, v in enumerate(res[u]):
                field[k * mix + u, t + 1] = v
        return carry

    lax.fori_loop(0, half // mix, body, 0)


def _rest_kernel(info, lowest, highest, state, low, high, drive, kinds, prior, out, late, scaled, taper, field, *, mix,
                 edge_mix, half, groups, bands):
    per, tiles = state.shape[0], state.shape[1]
    last = tiles - 1
    count = tiles + 2
    scaled[0] = low[per] * SCALE
    scaled[count - 1] = high[per] * SCALE
    for t in range(tiles):
        scaled[t + 1] = drive[t] * SCALE
    for t in range(count):
        kind = low[per + 1, :, :128] if t == 0 else high[per + 1, :, :128] if t == count - 1 else kinds[t - 1]
        for c, v in enumerate(_taper(kind)):
            taper[c, t] = v
    mask = _masks(info, bands)

    def edge(k, carry):
        at = [k * edge_mix + u for u in range(edge_mix)]
        cur = [[low[j] * SCALE, state[j, 0] * SCALE, state[j, 1] * SCALE] for j in at]
        res = _steps(cur, lambda t: scaled[t], [1], {0: mask[0]})
        for j, r in zip(at, res):
            field[j, 0] = r[0]
        cur = [[state[j, last - 1] * SCALE, state[j, last] * SCALE, high[j] * SCALE] for j in at]
        res = _steps(cur, lambda t: scaled[last + t], [1], {2: mask[1]})
        for j, r in zip(at, res):
            field[j, last] = r[0]
        return carry

    def whole(k, carry):
        at = [half + k * mix + u for u in range(mix)]
        cur = [[low[j] * SCALE] + [state[j, t] * SCALE for t in range(tiles)] + [high[j] * SCALE] for j in at]
        res = _steps(cur, lambda t: scaled[t], range(1, count - 1), {0: mask[0], count - 1: mask[1]})
        for j, r in zip(at, res):
            for t, v in enumerate(r):
                field[j, t] = v
        return carry

    lax.fori_loop(0, half // edge_mix, edge, 0)
    for j in range(half):
        for t in range(1, last):
            field[j, t] = prior[j, t]
    lax.fori_loop(0, (per - half) // mix, whole, 0)

    def pack(g, carry):
        for q in range(tiles):
            for slot, table in enumerate((lowest, highest)):
                first = table[2 * q, g * per]
                second = table[2 * q + 1, g * per]
                value = _halves(field[first, q], field[second, q])
                if q in LATE:
                    late[g, slot, q - LATE[0]] = value
                else:
                    out[g, slot, q - len(LATE) if q > LATE[-1] else q] = value
        return carry

    lax.fori_loop(0, groups, pack, 0)


def _masks(info, bands):
    one = jnp.float32(1.0)
    zero = jnp.float32(0.0)
    return [jnp.where(info[1] > 0, one, zero), jnp.where(info[1] < bands - 1, one, zero)]


def _choose(slots, incoming, column, patch, q):
    a = incoming[slots[2 * patch, column], q]
    b = incoming[slots[2 * patch + 1, column], q]
    return _halves(a, b)


def _pick_kernel(info, slots, early, first, final, one, two, sems, *, last):
    per = first.shape[0]
    loads = [pltpu.make_async_copy(early.at[:, 0], one, sems.at[0]),
             pltpu.make_async_copy(early.at[:, early.shape[1] - 1], two, sems.at[1])]
    for c in loads:
        c.start()
    for c in loads:
        c.wait()

    def body(j, carry):
        column = info[0] * per + j
        first[j] = _halves(one[slots[0, column]], one[slots[1, column]])
        final[j] = _halves(two[slots[2 * last, column]], two[slots[2 * last + 1, column]])
        return carry

    lax.fori_loop(0, per, body, 0)


def _advance_part(pieces, store, out, column, buffer, sems, scaled, taper, masks, *, per, mix):
    count, width = scaled.shape[0], scaled.shape[2]

    def weights(t):
        return [_widen(taper[c, t], width) for c in range(3)]

    def copy(k, hold):
        return pltpu.make_async_copy(
            buffer.at[hold], out.at[pl.ds(k * mix, mix), pl.ds(store, count - 2)], sems.at[hold])

    def body(k, carry):
        hold = k % 2
        cur = [_blend(pieces(k * mix + u), weights, masks) for u in range(mix)]
        res = _steps(cur, lambda t: scaled[t], range(1, count - 1), masks)

        @pl.when(k >= 2)
        def _():
            copy(k - 2, hold).wait()

        for u in range(mix):
            for t, v in enumerate(res[u]):
                buffer[hold, u, t] = v * (1.0 / SCALE)
        copy(k, hold).start()
        return carry

    steps = per // mix
    lax.fori_loop(0, steps, body, 0)
    for k in range(steps - 2, steps):
        copy(k, k % 2).wait()


def _lower_kernel(info, slots, early, first, below, scaled_in, taper_in, out, kept, buffer, inner, ends, scaled, taper,
                  sems, *, per, mix, bands):
    count = scaled.shape[0]
    loads = [
        pltpu.make_async_copy(early.at[:, pl.ds(1, count - 2)], inner, sems.at[2]),
        pltpu.make_async_copy(first, ends.at[1], sems.at[3]),
        pltpu.make_async_copy(below, ends.at[0], sems.at[4]),
        pltpu.make_async_copy(scaled_in.at[pl.ds(0, count)], scaled, sems.at[5]),
        pltpu.make_async_copy(taper_in.at[:, pl.ds(0, count)], taper, sems.at[6]),
    ]
    for c in loads:
        c.start()
    for c in loads:
        c.wait()

    def pieces(j):
        column = info[0] * per + j
        mine = [_choose(slots, inner, column, t, t - 1) for t in range(1, count - 1)]
        kept[j, 0] = mine[-2]
        kept[j, 1] = mine[-1]
        return [ends[0, j], ends[1, j]] + mine

    _advance_part(pieces, 0, out, None, buffer, sems, scaled, taper, {0: _masks(info, bands)[0]}, per=per, mix=mix)


def _upper_kernel(info, slots, late, kept_in, final, above, scaled_in, taper_in, prior, out, buffer, kept, ends, scaled,
                  taper, sems, *, per, tiles, mix, bands):
    count = scaled.shape[0]
    start = tiles + 2 - count
    loads = [
        pltpu.make_async_copy(kept_in, kept, sems.at[2]),
        pltpu.make_async_copy(final, ends.at[0], sems.at[3]),
        pltpu.make_async_copy(above, ends.at[1], sems.at[4]),
        pltpu.make_async_copy(scaled_in.at[pl.ds(start, count)], scaled, sems.at[5]),
        pltpu.make_async_copy(taper_in.at[:, pl.ds(start, count)], taper, sems.at[6]),
    ]
    for c in loads:
        c.start()
    for c in loads:
        c.wait()

    def pieces(j):
        column = info[0] * per + j
        mine = [_choose(slots, late, column, t, t - LATE[0]) for t in LATE]
        return [kept[j, 0], kept[j, 1]] + mine + [ends[0, j], ends[1, j]]

    _advance_part(pieces, start, out, None, buffer, sems, scaled, taper, {count - 1: _masks(info, bands)[1]}, per=per,
                  mix=mix)


def _pin(x):
    return pltpu.with_memory_space_constraint(x, pltpu.HBM)


def _call(kernel, name, outs, scratch, spaces, out_spaces, alias=None):
    def spec(kind):
        return pl.BlockSpec(memory_space={"v": pltpu.VMEM, "s": pltpu.SMEM, "a": pl.ANY, "h": pltpu.HBM}[kind])

    specs = [spec(k) for k in out_spaces]
    single = len(outs) == 1
    return pl.pallas_call(
        kernel,
        in_specs=[spec(k) for k in spaces],
        out_specs=specs[0] if single else specs,
        out_shape=outs[0] if single else outs,
        scratch_shapes=scratch,
        input_output_aliases=alias or {},
        compiler_params=pltpu.CompilerParams(vmem_limit_bytes=40 * 1024 * 1024),
        name=name,
    )


def on_device(state, forcing, parents, taper_index):
    per, rows, width = state.shape
    tiles = rows // TILE
    groups = lax.axis_size("pgroup")
    bands = lax.axis_size("band")
    f32 = jnp.float32
    forward = [(i, i + 1) for i in range(bands - 1)]
    backward = [(b, a) for a, b in forward]
    info = jnp.stack([lax.axis_index("pgroup"), lax.axis_index("band")]).astype(jnp.int32)
    state4 = state.reshape(per, tiles, TILE, width)
    pinned = _pin(state4)
    drive = forcing.reshape(tiles, TILE, width)
    entries = groups * CAP
    dma = pltpu.SemaphoreType.DMA
    vmem = pltpu.VMEM

    def shape(*dims, dtype=f32):
        return jax.ShapeDtypeStruct(dims, dtype)

    patches, count = parents.shape
    i32 = jnp.int32
    head, tail, kinds, lowest, highest, slots, state4, drive = _call(
        functools.partial(_prep_kernel, per=per, tiles=tiles), "prepare",
        [shape(per + 2, TILE, width), shape(per + 2, TILE, width), shape(tiles, TILE, 128),
         shape(patches, count, dtype=i32), shape(patches, count, dtype=i32), shape(patches, count, dtype=i32),
         shape(per, tiles, TILE, width), shape(tiles, TILE, width)],
        [pltpu.SMEM((rows,), i32), vmem((patches, count), i32), dma((8,))], "shhhh", "vvvvvvvv",
    )(info, _pin(taper_index), pinned, _pin(drive), _pin(parents))
    low = lax.ppermute(tail, "band", forward)
    high = lax.ppermute(head, "band", backward)

    half = per // 2
    field = _call(
        functools.partial(_inner_kernel, mix=2, half=half), "advance_inner",
        [shape(half, tiles, TILE, width)], [vmem((tiles, TILE, width), f32)], "vv", "v",
    )(state4, drive)
    early = tiles - len(LATE)
    count = len(LATE) + 4
    message, later, scaled, taper = _call(
        functools.partial(_rest_kernel, mix=2, edge_mix=4, half=half, groups=groups, bands=bands), "advance_rest",
        [shape(groups, CAP, early, TILE, width), shape(groups, CAP, len(LATE), TILE, width),
         shape(tiles + 2, TILE, width), shape(3, tiles + 2, TILE, 128)],
        [vmem((per, tiles, TILE, width), f32)], "sssvvvvvv", "vvvv",
    )(info, lowest, highest, state4, low, high, drive, kinds, field)

    incoming = lax.all_to_all(message, "pgroup", split_axis=0, concat_axis=0, tiled=True)
    incoming, later = lax.optimization_barrier((incoming, later))
    late = lax.all_to_all(later, "pgroup", split_axis=0, concat_axis=0, tiled=True)
    incoming = _pin(incoming.reshape(entries, early, TILE, width))
    late = late.reshape(entries, len(LATE), TILE, width)
    slots, scaled, taper = _pin(slots), _pin(scaled), _pin(taper)

    first, final = _call(
        functools.partial(_pick_kernel, last=tiles - 1), "pick_edge", [shape(per, TILE, width)] * 2,
        [vmem((entries, TILE, width), f32), vmem((entries, TILE, width), f32), dma((2,))], "ssh", "vv",
    )(info, slots, incoming)
    below = lax.ppermute(final, "band", forward)
    above = lax.ppermute(first, "band", backward)

    field, kept = _call(
        functools.partial(_lower_kernel, per=per, mix=2, bands=bands), "final_lower",
        [shape(per, tiles, TILE, width), shape(per, 2, TILE, width)],
        [vmem((2, 2, count - 2, TILE, width), f32), vmem((entries, count - 2, TILE, width), f32),
         vmem((2, per, TILE, width), f32), vmem((count, TILE, width), f32), vmem((3, count, TILE, 128), f32),
         dma((7,))], "sshhhhh", "av",
    )(info, slots, incoming, _pin(first), _pin(below), scaled, taper)
    field = _call(
        functools.partial(_upper_kernel, per=per, tiles=tiles, mix=2, bands=bands), "final_upper",
        [shape(per, tiles, TILE, width)],
        [vmem((2, 2, count - 2, TILE, width), f32), vmem((per, 2, TILE, width), f32),
         vmem((2, per, TILE, width), f32), vmem((count, TILE, width), f32), vmem((3, count, TILE, 128), f32),
         dma((7,))], "ssvhhhhha", "a", {8: 0},
    )(info, slots, late, _pin(kept), _pin(final), _pin(above), scaled, taper, field)
    return field.reshape(per, rows, width)


def solution(mesh):
    return jax.shard_map(
        on_device,
        mesh=mesh,
        in_specs=(P("pgroup", "band", None), P("band", None), P("band", None), P("band")),
        out_specs=P("pgroup", "band", None),
        check_vma=False,
    )
```

```python
import functools

import jax
import jax.numpy as jnp
from jax import lax
from jax.experimental import pallas as pl
from jax.experimental.pallas import tpu as pltpu
from jax.sharding import PartitionSpec as P

PATCH_ROWS = 4
STEPS = 6
CAP = 2
TILE = 8
SCALE = 0.05


def _sub(shape):
    return lax.broadcasted_iota(jnp.int32, shape, 0)


def _north(tiles, i, k):
    count = len(tiles)
    return tiles[i + k] if i + k < count else pltpu.roll(tiles[i + k - count], TILE - 1, 0)


def _south(tiles, i, k):
    return tiles[i - k] if i >= k else pltpu.roll(tiles[i - k + len(tiles)], 1, 0)


def _step(tiles, i, drive):
    m = tiles[i]
    width = m.shape[1]
    e = pltpu.roll(m, width - 1, 1)
    w = pltpu.roll(m, 1, 1)
    n = _north(tiles, i, 1)
    s = _south(tiles, i, 1)
    return (m * (0.4 - (e - w)) + 0.15 * (e + w)) + (0.05 * n + 0.25 * s) + drive


def _steps(groups, drive, masks):
    for repeat in range(STEPS):
        fresh = [list(tiles) for tiles in groups]
        for i in range(len(groups[0])):
            source = drive(i)
            for tiles, new in zip(groups, fresh):
                v = _step(tiles, i, source)
                new[i] = v if masks is None else v * masks(i)
        groups = fresh
    return groups


def _blend(tiles, weights, masks):
    fresh = []
    for i in range(len(tiles)):
        w0, w1, w2 = weights(i)
        total = w0 * tiles[i]
        total = total + w1 * (_north(tiles, i, 1) + _south(tiles, i, 1))
        total = total + w2 * (_north(tiles, i, 2) + _south(tiles, i, 2))
        fresh.append(total if masks is None else total * masks(i))
    return fresh


LANES = 128


def _spread(scratch, u, natural):
    count = len(natural)
    chunks = natural[0].shape[1] // LANES
    for t, v in enumerate(natural):
        for c in range(chunks):
            scratch[u, c, t * TILE:(t + 1) * TILE, :] = v[:, c * LANES:(c + 1) * LANES]
    return [jnp.concatenate([scratch[u, c, pl.ds(i, TILE, count), :] for c in range(chunks)], axis=1)
            for i in range(count)]


def _collect(scratch, u, tiles, keep):
    count = len(tiles)
    chunks = tiles[0].shape[1] // LANES
    for i, v in enumerate(tiles):
        for c in range(chunks):
            scratch[u, c, pl.ds(i, TILE, count), :] = v[:, c * LANES:(c + 1) * LANES]
    return [jnp.concatenate([scratch[u, c, t * TILE:(t + 1) * TILE, :] for c in range(chunks)], axis=1) for t in keep]


def _row_masks(ref, count, rows, first, low, high):
    for i in range(count):
        row = _sub((TILE, LANES)) * count + i + first
        ref[i] = jnp.where(row < 0, low, jnp.where(row >= rows, high, jnp.float32(1.0)))


def _taper(kind):
    rate = 0.2 * (kind + 1.0)
    near = jnp.exp(-rate)
    far = jnp.exp(-4.0 * rate)
    inv = 1.0 / (far + near + 1.0 + near + far)
    return inv, near * inv, far * inv


def _halves(a, b):
    return jnp.where(_sub(a.shape) < PATCH_ROWS, a, b)


def _widen(v, width):
    return jnp.concatenate([v] * (width // v.shape[1]), axis=1)


def _prep_kernel(info, taper_in, state, forcing, parents_in, head, tail, kinds, lowest, highest, slots, local, drive,
                 taper, parents, sems, *, per, tiles):
    last = tiles - 1
    copies = [
        pltpu.make_async_copy(state.at[:, 0], head.at[pl.ds(0, per)], sems.at[0]),
        pltpu.make_async_copy(state.at[:, last], tail.at[pl.ds(0, per)], sems.at[1]),
        pltpu.make_async_copy(forcing.at[0], head.at[per], sems.at[2]),
        pltpu.make_async_copy(forcing.at[last], tail.at[per], sems.at[3]),
        pltpu.make_async_copy(forcing, drive, sems.at[4]),
        pltpu.make_async_copy(state, local, sems.at[5]),
    ]
    first = [pltpu.make_async_copy(parents_in, parents, sems.at[6]), pltpu.make_async_copy(taper_in, taper, sems.at[7])]
    for c in first + copies:
        c.start()
    for c in first:
        c.wait()
    width = head.shape[2]
    for t in range(tiles):
        for r in range(TILE):
            value = taper[t * TILE + r].astype(jnp.float32)
            kinds[t, r:r + 1, :] = jnp.full((1, kinds.shape[2]), value, jnp.float32)
            if t == 0:
                head[per + 1, r:r + 1, :] = jnp.full((1, width), value, jnp.float32)
            if t == last:
                tail[per + 1, r:r + 1, :] = jnp.full((1, width), value, jnp.float32)
    p = parents[...]
    count = p.shape[1]
    owner = p // per
    inside = p - owner * per
    mine = owner == info[0]
    lo = jnp.where(mine, inside, per - 1)
    hi = jnp.where(mine, inside, 0)
    shift = 1
    while shift < per:
        lo = jnp.minimum(lo, pltpu.roll(lo, count - shift, 1))
        hi = jnp.maximum(hi, pltpu.roll(hi, count - shift, 1))
        shift *= 2
    lowest[...] = lo
    highest[...] = hi
    lane = lax.broadcasted_iota(jnp.int32, p.shape, 1) % per
    rank = jnp.zeros_like(p)
    for shift in range(1, per):
        other = jnp.where(lane + shift < per, pltpu.roll(p, count - shift, 1), pltpu.roll(p, per - shift, 1))
        rank = jnp.where((other // per == owner) & (other < p), 1, rank)
    slots[...] = owner * CAP + rank
    for c in copies:
        c.wait()


def _inner_kernel(state, drive, field, scaled, work, *, mix, half):
    tiles = state.shape[1]
    for t, v in enumerate(_spread(work, 0, [drive[t] * SCALE for t in range(tiles)])):
        scaled[t] = v

    def body(k, carry):
        cur = [_spread(work, u, [state[k * mix + u, t] * SCALE for t in range(tiles)]) for u in range(mix)]
        res = _steps(cur, lambda t: scaled[t], None)
        keep = range(1, tiles - 1)
        for u in range(mix):
            for t, v in zip(keep, _collect(work, u, res[u], keep)):
                field[k * mix + u, t] = v
        return carry

    lax.fori_loop(0, half // mix, body, 0)


def _rest_kernel(info, lowest, highest, state, low, high, drive, prior, out, field, scaled, ends, masks, masks3, work, *,
                 mix, edge_mix, half, groups, bands):
    per, tiles = state.shape[0], state.shape[1]
    last = tiles - 1
    count = tiles + 2
    rows = tiles * TILE
    width = state.shape[3]
    natural = [low[per] * SCALE] + [drive[t] * SCALE for t in range(tiles)] + [high[per] * SCALE]
    for s in range(2):
        for t, v in enumerate(_spread(work, s, natural[last * s:last * s + 3])):
            ends[s, t] = v
    for t, v in enumerate(_spread(work, 2, natural)):
        scaled[t] = v
    mask = _masks(info, bands)
    _row_masks(masks, count, rows, -TILE, mask[0], mask[1])
    for s in range(2):
        _row_masks(masks3.at[s], 3, rows, (last * s - 1) * TILE, mask[0], mask[1])

    def edge(k, carry):
        at = [k * edge_mix + u for u in range(edge_mix)]
        for s in range(2):
            cur = []
            for u, j in enumerate(at):
                three = [low[j], state[j, 0], state[j, 1]] if s == 0 else [state[j, last - 1], state[j, last], high[j]]
                cur.append(_spread(work, u, [v * SCALE for v in three]))
            res = _steps(cur, lambda t: ends[s, t], lambda t: _widen(masks3[s, t], width))
            for u, j in enumerate(at):
                field[j, last * s] = _collect(work, u, res[u], [1])[0]
        return carry

    def whole(k, carry):
        at = [half + k * mix + u for u in range(mix)]
        cur = [_spread(work, u, [low[j] * SCALE] + [state[j, t] * SCALE for t in range(tiles)] + [high[j] * SCALE])
               for u, j in enumerate(at)]
        res = _steps(cur, lambda t: scaled[t], lambda t: _widen(masks[t], width))
        keep = range(1, count - 1)
        for u, j in enumerate(at):
            for t, v in zip(keep, _collect(work, u, res[u], keep)):
                field[j, t - 1] = v
        return carry

    lax.fori_loop(0, half // edge_mix, edge, 0)
    for j in range(half):
        for t in range(1, last):
            field[j, t] = prior[j, t]
    lax.fori_loop(0, (per - half) // mix, whole, 0)

    def pack(g, carry):
        for q in range(tiles):
            for slot, table in enumerate((lowest, highest)):
                first = table[2 * q, g * per]
                second = table[2 * q + 1, g * per]
                out[g, slot, q] = _halves(field[first, q], field[second, q])
        return carry

    lax.fori_loop(0, groups, pack, 0)


def _masks(info, bands):
    one = jnp.float32(1.0)
    zero = jnp.float32(0.0)
    return [jnp.where(info[1] > 0, one, zero), jnp.where(info[1] < bands - 1, one, zero)]


def _choose(slots, incoming, column, q):
    a = incoming[slots[2 * q, column], q]
    b = incoming[slots[2 * q + 1, column], q]
    return _halves(a, b)


def _pick_kernel(info, slots, incoming, first, final):
    per, tiles = first.shape[0], incoming.shape[1]

    def body(j, carry):
        column = info[0] * per + j
        first[j] = _choose(slots, incoming, column, 0)
        final[j] = _choose(slots, incoming, column, tiles - 1)
        return carry

    lax.fori_loop(0, per, body, 0)


def _spread_kinds(scratch, kinds, taper):
    for t, v in enumerate(_spread(scratch, 0, kinds)):
        for c, part in enumerate(_taper(v)):
            taper[c, t] = part


def _final_inner_kernel(info, slots, incoming, drive, kinds, out, buffer, scaled, taper, work, sems, *, per, half, mix):
    tiles, width = drive.shape[0], drive.shape[2]
    for t, v in enumerate(_spread(work, 0, [drive[t] * SCALE for t in range(tiles)])):
        scaled[t] = v
    _spread_kinds(work, [kinds[t] for t in range(tiles)], taper)

    def weights(t):
        return [_widen(taper[c, t], width) for c in range(3)]

    def copy(k, hold):
        return pltpu.make_async_copy(
            buffer.at[hold], out.at[pl.ds(k * mix, mix), pl.ds(1, tiles - 2)], sems.at[hold])

    def body(k, carry):
        hold = k % 2
        cur = []
        for u in range(mix):
            column = info[0] * per + k * mix + u
            mine = _spread(work, u, [_choose(slots, incoming, column, t) for t in range(tiles)])
            cur.append(_blend(mine, weights, None))
        res = _steps(cur, lambda t: scaled[t], None)

        @pl.when(k >= 2)
        def _():
            copy(k - 2, hold).wait()

        for u in range(mix):
            for t, v in enumerate(_collect(work, u, res[u], range(1, tiles - 1))):
                buffer[hold, u, t] = v * (1.0 / SCALE)
        copy(k, hold).start()
        return carry

    steps = half // mix
    lax.fori_loop(0, steps, body, 0)
    for k in range(steps - 2, steps):
        copy(k, k % 2).wait()


def _final_rest_kernel(info, slots, incoming, first, final, low, high, below, above, drive, kinds, prior, out,
                       edges, buffer, scaled, taper, ends, taper3, masks, masks3, work, sems, *, per, half, mix,
                       edge_mix, bands):
    tiles, width = drive.shape[0], drive.shape[2]
    last = tiles - 1
    count = tiles + 2
    rows = tiles * TILE
    natural = [low[per] * SCALE] + [drive[t] * SCALE for t in range(tiles)] + [high[per] * SCALE]
    every = [low[per + 1, :, :LANES]] + [kinds[t] for t in range(tiles)] + [high[per + 1, :, :LANES]]
    for s in range(2):
        for t, v in enumerate(_spread(work, s, natural[last * s:last * s + 3])):
            ends[s, t] = v
        _spread_kinds(work, every[last * s:last * s + 3], taper3.at[s])
    for t, v in enumerate(_spread(work, 2, natural)):
        scaled[t] = v
    _spread_kinds(work, every, taper)
    mask = _masks(info, bands)
    _row_masks(masks, count, rows, -TILE, mask[0], mask[1])
    for s in range(2):
        _row_masks(masks3.at[s], 3, rows, (last * s - 1) * TILE, mask[0], mask[1])

    def finish(s):
        return pltpu.make_async_copy(edges.at[s], out.at[pl.ds(0, half), last * s], sems.at[2 + s])

    def edge(k, carry):
        for s in range(2):
            def mask3(t):
                return _widen(masks3[s, t], width)

            cur = []
            for u in range(edge_mix):
                j = k * edge_mix + u
                inner = _choose(slots, incoming, info[0] * per + j, 1 if s == 0 else last - 1)
                three = [below[j], first[j], inner] if s == 0 else [inner, final[j], above[j]]
                cur.append(_blend(_spread(work, u, three),
                                  lambda t: [_widen(taper3[s, c, t], width) for c in range(3)], mask3))
            res = _steps(cur, lambda t: ends[s, t], mask3)
            for u in range(edge_mix):
                edges[s, k * edge_mix + u] = _collect(work, u, res[u], [1])[0] * (1.0 / SCALE)
        return carry

    lax.fori_loop(0, half // edge_mix, edge, 0)
    for s in range(2):
        finish(s).start()

    def copy(k, hold):
        return pltpu.make_async_copy(buffer.at[hold], out.at[pl.ds(half + k * mix, mix)], sems.at[hold])

    def whole(k, carry):
        hold = k % 2
        cur = []
        for u in range(mix):
            j = half + k * mix + u
            column = info[0] * per + j
            mine = [below[j], first[j]]
            mine += [_choose(slots, incoming, column, t) for t in range(1, last)]
            mine += [final[j], above[j]]
            cur.append(_blend(_spread(work, u, mine), lambda t: [_widen(taper[c, t], width) for c in range(3)],
                              lambda t: _widen(masks[t], width)))
        res = _steps(cur, lambda t: scaled[t], lambda t: _widen(masks[t], width))

        @pl.when(k >= 2)
        def _():
            copy(k - 2, hold).wait()

        for u in range(mix):
            for t, v in enumerate(_collect(work, u, res[u], range(1, count - 1))):
                buffer[hold, u, t] = v * (1.0 / SCALE)
        copy(k, hold).start()
        return carry

    steps = (per - half) // mix
    lax.fori_loop(0, steps, whole, 0)
    for k in range(steps - 2, steps):
        copy(k, k % 2).wait()
    for s in range(2):
        finish(s).wait()


def _pin(x):
    return pltpu.with_memory_space_constraint(x, pltpu.HBM)


def _call(kernel, name, outs, scratch, spaces, out_spaces, alias=None):
    def spec(kind):
        return pl.BlockSpec(memory_space={"v": pltpu.VMEM, "s": pltpu.SMEM, "a": pl.ANY, "h": pltpu.HBM}[kind])

    specs = [spec(k) for k in out_spaces]
    single = len(outs) == 1
    return pl.pallas_call(
        kernel,
        in_specs=[spec(k) for k in spaces],
        out_specs=specs[0] if single else specs,
        out_shape=outs[0] if single else outs,
        scratch_shapes=scratch,
        input_output_aliases=alias or {},
        compiler_params=pltpu.CompilerParams(vmem_limit_bytes=40 * 1024 * 1024),
        name=name,
    )


def on_device(state, forcing, parents, taper_index):
    per, rows, width = state.shape
    tiles = rows // TILE
    groups = lax.axis_size("pgroup")
    bands = lax.axis_size("band")
    f32 = jnp.float32
    forward = [(i, i + 1) for i in range(bands - 1)]
    backward = [(b, a) for a, b in forward]
    info = jnp.stack([lax.axis_index("pgroup"), lax.axis_index("band")]).astype(jnp.int32)
    state4 = state.reshape(per, tiles, TILE, width)
    pinned = _pin(state4)
    drive = forcing.reshape(tiles, TILE, width)
    entries = groups * CAP
    dma = pltpu.SemaphoreType.DMA
    vmem = pltpu.VMEM

    def shape(*dims, dtype=f32):
        return jax.ShapeDtypeStruct(dims, dtype)

    patches, count = parents.shape
    i32 = jnp.int32
    head, tail, kinds, lowest, highest, slots, state4, drive = _call(
        functools.partial(_prep_kernel, per=per, tiles=tiles), "prepare",
        [shape(per + 2, TILE, width), shape(per + 2, TILE, width), shape(tiles, TILE, 128),
         shape(patches, count, dtype=i32), shape(patches, count, dtype=i32), shape(patches, count, dtype=i32),
         shape(per, tiles, TILE, width), shape(tiles, TILE, width)],
        [pltpu.SMEM((rows,), i32), vmem((patches, count), i32), dma((8,))], "shhhh", "vvvvvvvv",
    )(info, _pin(taper_index), pinned, _pin(drive), _pin(parents))
    low = lax.ppermute(tail, "band", forward)
    high = lax.ppermute(head, "band", backward)

    half = per // 2

    def work(count, height):
        return vmem((count, width // LANES, height * TILE, LANES), f32)

    extra = [vmem((tiles + 2, TILE, width), f32), vmem((2, 3, TILE, width), f32),
             vmem((tiles + 2, TILE, LANES), f32), vmem((2, 3, TILE, LANES), f32)]
    field = _call(
        functools.partial(_inner_kernel, mix=2, half=half), "advance_inner",
        [shape(half, tiles, TILE, width)], [vmem((tiles, TILE, width), f32), work(2, tiles)], "vv", "v",
    )(state4, drive)
    message = _call(
        functools.partial(_rest_kernel, mix=2, edge_mix=4, half=half, groups=groups, bands=bands), "advance_rest",
        [shape(groups, CAP, tiles, TILE, width)],
        [vmem((per, tiles, TILE, width), f32), *extra, work(4, tiles + 2)], "sssvvvvv", "v",
    )(info, lowest, highest, state4, low, high, drive, field)

    incoming = lax.all_to_all(message, "pgroup", split_axis=0, concat_axis=0, tiled=True)
    incoming = incoming.reshape(entries, tiles, TILE, width)

    first, final = _call(
        _pick_kernel, "pick_edge", [shape(per, TILE, width), shape(per, TILE, width)], [], "ssv", "vv",
    )(info, slots, incoming)
    below = lax.ppermute(final, "band", forward)
    above = lax.ppermute(first, "band", backward)

    field = _call(
        functools.partial(_final_inner_kernel, per=per, half=half, mix=2), "final_inner",
        [shape(per, tiles, TILE, width)],
        [vmem((2, 2, tiles - 2, TILE, width), f32), vmem((tiles, TILE, width), f32),
         vmem((3, tiles, TILE, LANES), f32), work(2, tiles), dma((2,))], "ssvvv", "a",
    )(info, slots, incoming, drive, kinds)
    field = _call(
        functools.partial(_final_rest_kernel, per=per, half=half, mix=2, edge_mix=4, bands=bands), "final_rest",
        [shape(per, tiles, TILE, width)],
        [vmem((2, half, TILE, width), f32), vmem((2, 2, tiles, TILE, width), f32), extra[0],
         vmem((3, tiles + 2, TILE, LANES), f32), extra[1], vmem((2, 3, 3, TILE, LANES), f32), *extra[2:],
         work(4, tiles + 2), dma((4,))], "ssvvvvvvvvva", "a", {11: 0},
    )(info, slots, incoming, first, final, low, high, below, above, drive, kinds, field)
    return field.reshape(per, rows, width)


def solution(mesh):
    return jax.shard_map(
        on_device,
        mesh=mesh,
        in_specs=(P("pgroup", "band", None), P("band", None), P("band", None), P("band")),
        out_specs=P("pgroup", "band", None),
        check_vma=False,
    )
```

```python
import functools

import jax
import jax.numpy as jnp
from jax import lax
from jax.experimental import pallas as pl
from jax.experimental.pallas import tpu as pltpu
from jax.sharding import PartitionSpec as P

PATCH_ROWS = 4
STEPS = 6
CAP = 2
TILE = 8
SCALE = 0.05


def _sub(shape):
    return lax.broadcasted_iota(jnp.int32, shape, 0)


def _north(tiles, i, k):
    count = len(tiles)
    return tiles[i + k] if i + k < count else pltpu.roll(tiles[i + k - count], TILE - 1, 0)


def _south(tiles, i, k):
    return tiles[i - k] if i >= k else pltpu.roll(tiles[i - k + len(tiles)], 1, 0)


def _step(tiles, i, drive):
    m = tiles[i]
    width = m.shape[1]
    e = jnp.concatenate([m[:, LANES:], pltpu.roll(m[:, :LANES], LANES - 1, 1)], axis=1)
    w = jnp.concatenate([pltpu.roll(m[:, width - LANES:], 1, 1), m[:, :width - LANES]], axis=1)
    n = _north(tiles, i, 1)
    s = _south(tiles, i, 1)
    return (m * (0.4 - (e - w)) + 0.15 * (e + w)) + (0.05 * n + 0.25 * s) + drive


def _steps(groups, drive, masks):
    for repeat in range(STEPS):
        fresh = [list(tiles) for tiles in groups]
        for i in range(len(groups[0])):
            source = drive(i)
            for tiles, new in zip(groups, fresh):
                v = _step(tiles, i, source)
                new[i] = v if masks is None else v * masks(i)
        groups = fresh
    return groups


def _blend(tiles, weights, masks):
    fresh = []
    for i in range(len(tiles)):
        w0, w1, w2 = weights(i)
        total = w0 * tiles[i]
        total = total + w1 * (_north(tiles, i, 1) + _south(tiles, i, 1))
        total = total + w2 * (_north(tiles, i, 2) + _south(tiles, i, 2))
        fresh.append(total if masks is None else total * masks(i))
    return fresh


LANES = 128


def _fill_order(ref, back):
    size = ref.shape[0]
    chunks = size // LANES
    step = 64
    for r in range(0, size, step):
        row = lax.broadcasted_iota(jnp.int32, (step, size), 0) + r
        column = lax.broadcasted_iota(jnp.int32, (step, size), 1)
        natural, mixed = (column, row) if back else (row, column)
        hit = natural == chunks * (mixed % LANES) + mixed // LANES
        ref[r:r + step, :] = jnp.where(hit, 1.0, 0.0).astype(jnp.bfloat16)


def _reorder(v, order):
    rows = v.shape[0]
    high = v.astype(jnp.bfloat16)
    rest = (v - high.astype(jnp.float32)).astype(jnp.bfloat16)
    both = jnp.dot(jnp.concatenate([high, rest], axis=0), order[...], preferred_element_type=jnp.float32)
    return both[:rows] + both[rows:]


def _spread(scratch, u, natural):
    count = len(natural)
    chunks = natural[0].shape[1] // LANES
    for t, v in enumerate(natural):
        for c in range(chunks):
            scratch[u, c, t * TILE:(t + 1) * TILE, :] = v[:, c * LANES:(c + 1) * LANES]
    return [jnp.concatenate([scratch[u, c, pl.ds(i, TILE, count), :] for c in range(chunks)], axis=1)
            for i in range(count)]


def _collect(scratch, u, tiles, keep):
    count = len(tiles)
    chunks = tiles[0].shape[1] // LANES
    for i, v in enumerate(tiles):
        for c in range(chunks):
            scratch[u, c, pl.ds(i, TILE, count), :] = v[:, c * LANES:(c + 1) * LANES]
    return [jnp.concatenate([scratch[u, c, t * TILE:(t + 1) * TILE, :] for c in range(chunks)], axis=1) for t in keep]


def _row_masks(ref, count, rows, first, low, high):
    for i in range(count):
        row = _sub((TILE, LANES)) * count + i + first
        ref[i] = jnp.where(row < 0, low, jnp.where(row >= rows, high, jnp.float32(1.0)))


def _taper(kind):
    rate = 0.2 * (kind + 1.0)
    near = jnp.exp(-rate)
    far = jnp.exp(-4.0 * rate)
    inv = 1.0 / (far + near + 1.0 + near + far)
    return inv, near * inv, far * inv


def _halves(a, b):
    return jnp.where(_sub(a.shape) < PATCH_ROWS, a, b)


def _widen(v, width):
    return jnp.concatenate([v] * (width // v.shape[1]), axis=1)


def _prep_kernel(info, taper_in, state, forcing, parents_in, head, tail, kinds, lowest, highest, slots, local, drive,
                 taper, parents, sems, *, per, tiles):
    last = tiles - 1
    copies = [
        pltpu.make_async_copy(state.at[:, 0], head.at[pl.ds(0, per)], sems.at[0]),
        pltpu.make_async_copy(state.at[:, last], tail.at[pl.ds(0, per)], sems.at[1]),
        pltpu.make_async_copy(forcing.at[0], head.at[per], sems.at[2]),
        pltpu.make_async_copy(forcing.at[last], tail.at[per], sems.at[3]),
        pltpu.make_async_copy(forcing, drive, sems.at[4]),
        pltpu.make_async_copy(state, local, sems.at[5]),
    ]
    first = [pltpu.make_async_copy(parents_in, parents, sems.at[6]), pltpu.make_async_copy(taper_in, taper, sems.at[7])]
    for c in first + copies:
        c.start()
    for c in first:
        c.wait()
    width = head.shape[2]
    for t in range(tiles):
        for r in range(TILE):
            value = taper[t * TILE + r].astype(jnp.float32)
            kinds[t, r:r + 1, :] = jnp.full((1, kinds.shape[2]), value, jnp.float32)
            if t == 0:
                head[per + 1, r:r + 1, :] = jnp.full((1, width), value, jnp.float32)
            if t == last:
                tail[per + 1, r:r + 1, :] = jnp.full((1, width), value, jnp.float32)
    p = parents[...]
    count = p.shape[1]
    owner = p // per
    inside = p - owner * per
    mine = owner == info[0]
    lo = jnp.where(mine, inside, per - 1)
    hi = jnp.where(mine, inside, 0)
    shift = 1
    while shift < per:
        lo = jnp.minimum(lo, pltpu.roll(lo, count - shift, 1))
        hi = jnp.maximum(hi, pltpu.roll(hi, count - shift, 1))
        shift *= 2
    lowest[...] = lo
    highest[...] = hi
    lane = lax.broadcasted_iota(jnp.int32, p.shape, 1) % per
    rank = jnp.zeros_like(p)
    for shift in range(1, per):
        other = jnp.where(lane + shift < per, pltpu.roll(p, count - shift, 1), pltpu.roll(p, per - shift, 1))
        rank = jnp.where((other // per == owner) & (other < p), 1, rank)
    slots[...] = owner * CAP + rank
    for c in copies:
        c.wait()


def _order_kernel(state, out, order, *, mix):
    per, tiles, _, width = state.shape
    _fill_order(order, False)

    def body(k, carry):
        v = jnp.concatenate([state[k * mix + u, t] for u in range(mix) for t in range(tiles)], axis=0) * SCALE
        v = _reorder(v, order)
        for u in range(mix):
            for t in range(tiles):
                at = (u * tiles + t) * TILE
                out[k * mix + u, t] = v[at:at + TILE]
        return carry

    lax.fori_loop(0, per // mix, body, 0)


def _advance_kernel(info, lowest, highest, state, low_in, high_in, drive, kinds, out, natural, every, field, low, high,
                    scaled, masks, work, order, *, mix, groups, bands):
    per, tiles = state.shape[0], state.shape[1]
    count = tiles + 2
    rows = tiles * TILE
    width = state.shape[3]
    _fill_order(order, False)
    both = [low_in[j] for j in range(per + 1)] + [high_in[j] for j in range(per + 1)] + [drive[t] for t in range(tiles)]
    v = _reorder(jnp.concatenate(both, axis=0) * SCALE, order)
    for j in range(per + 1):
        low[j] = v[j * TILE:(j + 1) * TILE]
        high[j] = v[(per + 1 + j) * TILE:(per + 2 + j) * TILE]
    natural[0] = low[per]
    natural[count - 1] = high[per]
    every[0] = low_in[per + 1, :, :LANES]
    every[count - 1] = high_in[per + 1, :, :LANES]
    for t in range(tiles):
        at = (2 * per + 2 + t) * TILE
        natural[t + 1] = v[at:at + TILE]
        every[t + 1] = kinds[t]
    for t, v in enumerate(_spread(work, 0, [natural[t] for t in range(count)])):
        scaled[t] = v
    mask = _masks(info, bands)
    _row_masks(masks, count, rows, -TILE, mask[0], mask[1])

    def whole(k, carry):
        at = [k * mix + u for u in range(mix)]
        cur = [_spread(work, u, [low[j]] + [state[j, t] for t in range(tiles)] + [high[j]]) for u, j in enumerate(at)]
        res = _steps(cur, lambda t: scaled[t], lambda t: _widen(masks[t], width))
        keep = range(1, count - 1)
        for u, j in enumerate(at):
            for t, v in zip(keep, _collect(work, u, res[u], keep)):
                field[j, t - 1] = v
        return carry

    lax.fori_loop(0, per // mix, whole, 0)

    def pack(g, carry):
        for q in range(tiles):
            for slot, table in enumerate((lowest, highest)):
                first = table[2 * q, g * per]
                second = table[2 * q + 1, g * per]
                out[g, slot, q] = _halves(field[first, q], field[second, q])
        return carry

    lax.fori_loop(0, groups, pack, 0)


def _masks(info, bands):
    one = jnp.float32(1.0)
    zero = jnp.float32(0.0)
    return [jnp.where(info[1] > 0, one, zero), jnp.where(info[1] < bands - 1, one, zero)]


def _choose(slots, incoming, column, q):
    a = incoming[slots[2 * q, column], q]
    b = incoming[slots[2 * q + 1, column], q]
    return _halves(a, b)


def _pick_kernel(info, slots, incoming, first, final):
    per, tiles = first.shape[0], incoming.shape[1]

    def body(j, carry):
        column = info[0] * per + j
        first[j] = _choose(slots, incoming, column, 0)
        final[j] = _choose(slots, incoming, column, tiles - 1)
        return carry

    lax.fori_loop(0, per, body, 0)


def _spread_kinds(scratch, kinds, taper):
    for t, v in enumerate(_spread(scratch, 0, kinds)):
        for c, part in enumerate(_taper(v)):
            taper[c, t] = part


def _natural(pend, hold, order):
    mix, count = pend.shape[1], pend.shape[2]
    v = jnp.concatenate([pend[hold, u, t] for u in range(mix) for t in range(count)], axis=0)
    v = _reorder(v, order) * (1.0 / SCALE)
    return [[v[(u * count + t) * TILE:(u * count + t + 1) * TILE] for t in range(count)] for u in range(mix)]


def _pipeline(steps, mix, compute, pend, order, done, copy):
    def flush(k):
        for u, column in enumerate(_natural(pend, k % 2, order)):
            for t, v in enumerate(column):
                done[k * mix + u, t] = v

    def first(k):
        for u, column in enumerate(compute(k)):
            for t, v in enumerate(column):
                pend[k % 2, u, t] = v

    first(0)

    def body(k, carry):
        flush(k - 1)
        first(k)
        copy(k - 1).start()
        return carry

    lax.fori_loop(1, steps, body, 0)
    flush(steps - 1)
    copy(steps - 1).start()
    for k in range(steps):
        copy(k).wait()


def _final_inner_kernel(info, slots, incoming, natural, every, out, done, pend, scaled, taper, work, order, sems, *, per,
                        half, mix):
    tiles, width = natural.shape[0] - 2, natural.shape[2]
    _fill_order(order, True)
    for t, v in enumerate(_spread(work, 0, [natural[t + 1] for t in range(tiles)])):
        scaled[t] = v
    _spread_kinds(work, [every[t + 1] for t in range(tiles)], taper)

    def weights(t):
        return [_widen(taper[c, t], width) for c in range(3)]

    def copy(k):
        return pltpu.make_async_copy(
            done.at[pl.ds(k * mix, mix)], out.at[pl.ds(k * mix, mix), pl.ds(1, tiles - 2)], sems.at[k])

    def compute(k):
        cur = []
        for u in range(mix):
            column = info[0] * per + k * mix + u
            mine = _spread(work, u, [_choose(slots, incoming, column, t) for t in range(tiles)])
            cur.append(_blend(mine, weights, None))
        res = _steps(cur, lambda t: scaled[t], None)
        return [_collect(work, u, res[u], range(1, tiles - 1)) for u in range(mix)]

    _pipeline(half // mix, mix, compute, pend, order, done, copy)


def _final_rest_kernel(info, slots, incoming, first, final, below, above, natural, every, prior, out,
                       edges, done, pend, scaled, taper, ends, taper3, masks, masks3, work, order, sems, *, per, half,
                       mix, edge_mix, bands):
    count, width = natural.shape[0], natural.shape[2]
    tiles = count - 2
    last = tiles - 1
    rows = tiles * TILE
    _fill_order(order, True)
    for s in range(2):
        for t, v in enumerate(_spread(work, s, [natural[last * s + t] for t in range(3)])):
            ends[s, t] = v
        _spread_kinds(work, [every[last * s + t] for t in range(3)], taper3.at[s])
    for t, v in enumerate(_spread(work, 2, [natural[t] for t in range(count)])):
        scaled[t] = v
    _spread_kinds(work, [every[t] for t in range(count)], taper)
    mask = _masks(info, bands)
    _row_masks(masks, count, rows, -TILE, mask[0], mask[1])
    for s in range(2):
        _row_masks(masks3.at[s], 3, rows, (last * s - 1) * TILE, mask[0], mask[1])
    steps = (per - half) // mix

    def finish(s):
        return pltpu.make_async_copy(edges.at[s], out.at[pl.ds(0, half), last * s], sems.at[steps + s])

    def edge(k, carry):
        for s in range(2):
            def mask3(t):
                return _widen(masks3[s, t], width)

            cur = []
            for u in range(edge_mix):
                j = k * edge_mix + u
                inner = _choose(slots, incoming, info[0] * per + j, 1 if s == 0 else last - 1)
                three = [below[j], first[j], inner] if s == 0 else [inner, final[j], above[j]]
                cur.append(_blend(_spread(work, u, three),
                                  lambda t: [_widen(taper3[s, c, t], width) for c in range(3)], mask3))
            res = _steps(cur, lambda t: ends[s, t], mask3)
            for u in range(edge_mix):
                edges[s, k * edge_mix + u] = _collect(work, u, res[u], [1])[0]
        return carry

    lax.fori_loop(0, half // edge_mix, edge, 0)
    v = jnp.concatenate([edges[s, j] for s in range(2) for j in range(half)], axis=0)
    v = _reorder(v, order) * (1.0 / SCALE)
    for s in range(2):
        for j in range(half):
            at = (s * half + j) * TILE
            edges[s, j] = v[at:at + TILE]
    for s in range(2):
        finish(s).start()

    def copy(k):
        return pltpu.make_async_copy(
            done.at[pl.ds(k * mix, mix)], out.at[pl.ds(half + k * mix, mix)], sems.at[k])

    def compute(k):
        cur = []
        for u in range(mix):
            j = half + k * mix + u
            column = info[0] * per + j
            mine = [below[j], first[j]]
            mine += [_choose(slots, incoming, column, t) for t in range(1, last)]
            mine += [final[j], above[j]]
            cur.append(_blend(_spread(work, u, mine), lambda t: [_widen(taper[c, t], width) for c in range(3)],
                              lambda t: _widen(masks[t], width)))
        res = _steps(cur, lambda t: scaled[t], lambda t: _widen(masks[t], width))
        return [_collect(work, u, res[u], range(1, count - 1)) for u in range(mix)]

    _pipeline(steps, mix, compute, pend, order, done, copy)
    for s in range(2):
        finish(s).wait()


def _pin(x):
    return pltpu.with_memory_space_constraint(x, pltpu.HBM)


def _call(kernel, name, outs, scratch, spaces, out_spaces, alias=None):
    def spec(kind):
        return pl.BlockSpec(memory_space={"v": pltpu.VMEM, "s": pltpu.SMEM, "a": pl.ANY, "h": pltpu.HBM}[kind])

    specs = [spec(k) for k in out_spaces]
    single = len(outs) == 1
    return pl.pallas_call(
        kernel,
        in_specs=[spec(k) for k in spaces],
        out_specs=specs[0] if single else specs,
        out_shape=outs[0] if single else outs,
        scratch_shapes=scratch,
        input_output_aliases=alias or {},
        compiler_params=pltpu.CompilerParams(vmem_limit_bytes=40 * 1024 * 1024),
        name=name,
    )


def on_device(state, forcing, parents, taper_index):
    per, rows, width = state.shape
    tiles = rows // TILE
    groups = lax.axis_size("pgroup")
    bands = lax.axis_size("band")
    f32 = jnp.float32
    forward = [(i, i + 1) for i in range(bands - 1)]
    backward = [(b, a) for a, b in forward]
    info = jnp.stack([lax.axis_index("pgroup"), lax.axis_index("band")]).astype(jnp.int32)
    state4 = state.reshape(per, tiles, TILE, width)
    pinned = _pin(state4)
    drive = forcing.reshape(tiles, TILE, width)
    entries = groups * CAP
    dma = pltpu.SemaphoreType.DMA
    vmem = pltpu.VMEM

    def shape(*dims, dtype=f32):
        return jax.ShapeDtypeStruct(dims, dtype)

    patches, count = parents.shape
    i32 = jnp.int32
    head, tail, kinds, lowest, highest, slots, state4, drive = _call(
        functools.partial(_prep_kernel, per=per, tiles=tiles), "prepare",
        [shape(per + 2, TILE, width), shape(per + 2, TILE, width), shape(tiles, TILE, 128),
         shape(patches, count, dtype=i32), shape(patches, count, dtype=i32), shape(patches, count, dtype=i32),
         shape(per, tiles, TILE, width), shape(tiles, TILE, width)],
        [pltpu.SMEM((rows,), i32), vmem((patches, count), i32), dma((8,))], "shhhh", "vvvvvvvv",
    )(info, _pin(taper_index), pinned, _pin(drive), _pin(parents))
    low = lax.ppermute(tail, "band", forward)
    high = lax.ppermute(head, "band", backward)

    half = per // 2

    def work(count, height):
        return vmem((count, width // LANES, height * TILE, LANES), f32)

    extra = [vmem((tiles + 2, TILE, width), f32), vmem((2, 3, TILE, width), f32),
             vmem((tiles + 2, TILE, LANES), f32), vmem((2, 3, TILE, LANES), f32)]
    square = vmem((width, width), jnp.bfloat16)
    state4 = _call(
        functools.partial(_order_kernel, mix=4), "reorder", [shape(per, tiles, TILE, width)], [square], "v", "v",
    )(state4)
    message, natural, every = _call(
        functools.partial(_advance_kernel, mix=2, groups=groups, bands=bands), "advance",
        [shape(groups, CAP, tiles, TILE, width), shape(tiles + 2, TILE, width), shape(tiles + 2, TILE, LANES)],
        [vmem((per, tiles, TILE, width), f32), vmem((per + 1, TILE, width), f32), vmem((per + 1, TILE, width), f32),
         extra[0], extra[2], work(2, tiles + 2), square], "sssvvvvv", "vvv",
    )(info, lowest, highest, state4, low, high, drive, kinds)

    incoming = lax.all_to_all(message, "pgroup", split_axis=0, concat_axis=0, tiled=True)
    incoming = incoming.reshape(entries, tiles, TILE, width)

    first, final = _call(
        _pick_kernel, "pick_edge", [shape(per, TILE, width), shape(per, TILE, width)], [], "ssv", "vv",
    )(info, slots, incoming)
    below = lax.ppermute(final, "band", forward)
    above = lax.ppermute(first, "band", backward)

    pairs = half // 2
    field = _call(
        functools.partial(_final_inner_kernel, per=per, half=half, mix=2), "final_inner",
        [shape(per, tiles, TILE, width)],
        [vmem((half, tiles - 2, TILE, width), f32), vmem((2, 2, tiles - 2, TILE, width), f32),
         vmem((tiles, TILE, width), f32), vmem((3, tiles, TILE, LANES), f32), work(2, tiles), square,
         dma((pairs,))], "ssvvv", "a",
    )(info, slots, incoming, natural, every)
    field = _call(
        functools.partial(_final_rest_kernel, per=per, half=half, mix=2, edge_mix=4, bands=bands), "final_rest",
        [shape(per, tiles, TILE, width)],
        [vmem((2, half, TILE, width), f32), vmem((per - half, tiles, TILE, width), f32),
         vmem((2, 2, tiles, TILE, width), f32), extra[0], vmem((3, tiles + 2, TILE, LANES), f32), extra[1],
         vmem((2, 3, 3, TILE, LANES), f32), *extra[2:], work(4, tiles + 2), square, dma((pairs + 2,))],
        "ssvvvvvvva", "a", {9: 0},
    )(info, slots, incoming, first, final, below, above, natural, every, field)
    return field.reshape(per, rows, width)


def solution(mesh):
    return jax.shard_map(
        on_device,
        mesh=mesh,
        in_specs=(P("pgroup", "band", None), P("band", None), P("band", None), P("band")),
        out_specs=P("pgroup", "band", None),
        check_vma=False,
    )
```

```python
import functools

import jax
import jax.numpy as jnp
from jax import lax
from jax.experimental import pallas as pl
from jax.experimental.pallas import tpu as pltpu
from jax.sharding import PartitionSpec as P

PATCH_ROWS = 4
STEPS = 6
CAP = 2
TILE = 8
SCALE = 0.05


def _sub(shape):
    return lax.broadcasted_iota(jnp.int32, shape, 0)


def _north(tiles, i, k):
    count = len(tiles)
    return tiles[i + k] if i + k < count else pltpu.roll(tiles[i + k - count], TILE - 1, 0)


def _south(tiles, i, k):
    return tiles[i - k] if i >= k else pltpu.roll(tiles[i - k + len(tiles)], 1, 0)


def _step(tiles, i, drive):
    m = tiles[i]
    width = m.shape[1]
    e = jnp.concatenate([m[:, LANES:], pltpu.roll(m[:, :LANES], LANES - 1, 1)], axis=1)
    w = jnp.concatenate([pltpu.roll(m[:, width - LANES:], 1, 1), m[:, :width - LANES]], axis=1)
    n = _north(tiles, i, 1)
    s = _south(tiles, i, 1)
    return (m * (0.4 - (e - w)) + 0.15 * (e + w)) + (0.05 * n + 0.25 * s) + drive


def _steps(groups, drive, masks):
    for repeat in range(STEPS):
        fresh = [list(tiles) for tiles in groups]
        for i in range(len(groups[0])):
            source = drive(i)
            for tiles, new in zip(groups, fresh):
                v = _step(tiles, i, source)
                new[i] = v * masks[i] if i in masks else v
        groups = fresh
    return groups


def _blend(tiles, weights, masks):
    fresh = []
    for i in range(len(tiles)):
        w0, w1, w2 = weights(i)
        total = w0 * tiles[i]
        total = total + w1 * (_north(tiles, i, 1) + _south(tiles, i, 1))
        total = total + w2 * (_north(tiles, i, 2) + _south(tiles, i, 2))
        fresh.append(total * masks[i] if i in masks else total)
    return fresh


LANES = 128


def _fill_order(ref, back):
    size = ref.shape[0]
    chunks = size // LANES
    step = 64
    for r in range(0, size, step):
        row = lax.broadcasted_iota(jnp.int32, (step, size), 0) + r
        column = lax.broadcasted_iota(jnp.int32, (step, size), 1)
        natural, mixed = (column, row) if back else (row, column)
        hit = natural == chunks * (mixed % LANES) + mixed // LANES
        ref[r:r + step, :] = jnp.where(hit, 1.0, 0.0).astype(jnp.bfloat16)


def _reorder(v, order):
    rows = v.shape[0]
    high = v.astype(jnp.bfloat16)
    rest = (v - high.astype(jnp.float32)).astype(jnp.bfloat16)
    both = jnp.dot(jnp.concatenate([high, rest], axis=0), order[...], preferred_element_type=jnp.float32)
    return both[:rows] + both[rows:]


def _spread(scratch, u, natural):
    count = len(natural)
    chunks = natural[0].shape[1] // LANES
    for t, v in enumerate(natural):
        for c in range(chunks):
            scratch[u, c, t * TILE:(t + 1) * TILE, :] = v[:, c * LANES:(c + 1) * LANES]
    return [jnp.concatenate([scratch[u, c, pl.ds(i, TILE, count), :] for c in range(chunks)], axis=1)
            for i in range(count)]


def _collect(scratch, u, tiles, keep):
    count = len(tiles)
    chunks = tiles[0].shape[1] // LANES
    for i, v in enumerate(tiles):
        for c in range(chunks):
            scratch[u, c, pl.ds(i, TILE, count), :] = v[:, c * LANES:(c + 1) * LANES]
    return [jnp.concatenate([scratch[u, c, t * TILE:(t + 1) * TILE, :] for c in range(chunks)], axis=1) for t in keep]


def _border(count, width, *rows):
    return {at % count: jnp.where(_sub((TILE, width)) == at // count, factor, jnp.float32(1.0)) for at, factor in rows}


def _taper(kind):
    rate = 0.2 * (kind + 1.0)
    near = jnp.exp(-rate)
    far = jnp.exp(-4.0 * rate)
    inv = 1.0 / (far + near + 1.0 + near + far)
    return inv, near * inv, far * inv


def _halves(a, b):
    return jnp.where(_sub(a.shape) < PATCH_ROWS, a, b)


def _widen(v, width):
    return jnp.concatenate([v] * (width // v.shape[1]), axis=1)


def _prep_kernel(info, taper_in, state, forcing, parents_in, head, tail, kinds, ends, own, local, drive,
                 taper, parents, sems, *, per, tiles):
    last = tiles - 1
    copies = [
        pltpu.make_async_copy(state.at[:, 0], head.at[pl.ds(0, per)], sems.at[0]),
        pltpu.make_async_copy(state.at[:, last], tail.at[pl.ds(0, per)], sems.at[1]),
        pltpu.make_async_copy(forcing.at[0], head.at[per], sems.at[2]),
        pltpu.make_async_copy(forcing.at[last], tail.at[per], sems.at[3]),
        pltpu.make_async_copy(forcing, drive, sems.at[4]),
        pltpu.make_async_copy(state, local, sems.at[5]),
    ]
    first = [pltpu.make_async_copy(parents_in, parents, sems.at[6]), pltpu.make_async_copy(taper_in, taper, sems.at[7])]
    for c in first + copies:
        c.start()
    for c in first:
        c.wait()
    width = head.shape[2]
    for t in range(tiles):
        for r in range(TILE):
            value = taper[t * TILE + r].astype(jnp.float32)
            kinds[t, r:r + 1, :] = jnp.full((1, kinds.shape[2]), value, jnp.float32)
            if t == 0:
                head[per + 1, r:r + 1, :] = jnp.full((1, width), value, jnp.float32)
            if t == last:
                tail[per + 1, r:r + 1, :] = jnp.full((1, width), value, jnp.float32)
    p = parents[...]
    count = p.shape[1]
    owner = p // per
    inside = p - owner * per
    mine = owner == info[0]
    lo = jnp.where(mine, inside, per - 1)
    hi = jnp.where(mine, inside, 0)
    shift = 1
    while shift < per:
        lo = jnp.minimum(lo, pltpu.roll(lo, count - shift, 1))
        hi = jnp.maximum(hi, pltpu.roll(hi, count - shift, 1))
        shift *= 2
    patches = p.shape[0]
    for slot, v in enumerate((lo, hi)):
        ends[slot, pl.ds(0, patches), :] = v
        ends[slot, pl.ds(patches, TILE), :] = jnp.full((TILE, count), info[1], jnp.int32)
    lane = lax.broadcasted_iota(jnp.int32, p.shape, 1) % per
    rank = jnp.zeros_like(p)
    for shift in range(1, per):
        other = jnp.where(lane + shift < per, pltpu.roll(p, count - shift, 1), pltpu.roll(p, per - shift, 1))
        rank = jnp.where((other // per == owner) & (other < p), 1, rank)
    turn = (count - info[0] * per) % count
    own[pl.ds(0, patches), :] = pltpu.roll(owner * CAP + rank, turn, 1)[:, :LANES]
    own[pl.ds(patches, TILE), :] = jnp.full((TILE, LANES), info[1], jnp.int32)
    for c in copies:
        c.wait()


def _order_kernel(state, out, order, back, *, mix):
    per, tiles, _, width = state.shape
    _fill_order(order, False)
    _fill_order(back, True)

    def body(k, carry):
        v = jnp.concatenate([state[k * mix + u, t] for u in range(mix) for t in range(tiles)], axis=0) * SCALE
        v = _reorder(v, order)
        for u in range(mix):
            for t in range(tiles):
                at = (u * tiles + t) * TILE
                out[k * mix + u, t] = v[at:at + TILE]
        return carry

    lax.fori_loop(0, per // mix, body, 0)


def _advance_kernel(table, state, low_in, high_in, drive, kinds, order, out, natural, every, field, low, high,
                    scaled, work, *, mix, groups, bands):
    per, tiles = state.shape[0], state.shape[1]
    count = tiles + 2
    rows = tiles * TILE
    width = state.shape[3]
    both = [low_in[j] for j in range(per + 1)] + [high_in[j] for j in range(per + 1)] + [drive[t] for t in range(tiles)]
    v = _reorder(jnp.concatenate(both, axis=0) * SCALE, order)
    for j in range(per + 1):
        low[j] = v[j * TILE:(j + 1) * TILE]
        high[j] = v[(per + 1 + j) * TILE:(per + 2 + j) * TILE]
    natural[0] = low[per]
    natural[count - 1] = high[per]
    every[0] = low_in[per + 1, :, :LANES]
    every[count - 1] = high_in[per + 1, :, :LANES]
    for t in range(tiles):
        at = (2 * per + 2 + t) * TILE
        natural[t + 1] = v[at:at + TILE]
        every[t + 1] = kinds[t]
    for t, v in enumerate(_spread(work, 0, [natural[t] for t in range(count)])):
        scaled[t] = v
    mask = _masks(table[0, table.shape[1] - 1, 0], bands)

    def whole(k, carry):
        masks = _border(count, width, (TILE - 1, mask[0]), (TILE + rows, mask[1]))
        at = [k * mix + u for u in range(mix)]
        cur = [_spread(work, u, [low[j]] + [state[j, t] for t in range(tiles)] + [high[j]]) for u, j in enumerate(at)]
        res = _steps(cur, lambda t: scaled[t], masks)
        keep = range(1, count - 1)
        for u, j in enumerate(at):
            for t, v in zip(keep, _collect(work, u, res[u], keep)):
                field[j, t - 1] = v
        return carry

    lax.fori_loop(0, per // mix, whole, 0)

    def pack(g, carry):
        for q in range(tiles):
            for slot in range(CAP):
                first = table[slot, 2 * q, g * per]
                second = table[slot, 2 * q + 1, g * per]
                out[g, slot, q] = _halves(field[first, q], field[second, q])
        return carry

    lax.fori_loop(0, groups, pack, 0)


def _masks(band, bands):
    one = jnp.float32(1.0)
    zero = jnp.float32(0.0)
    return [jnp.where(band > 0, one, zero), jnp.where(band < bands - 1, one, zero)]


def _choose(slots, incoming, column, q):
    a = incoming[slots[2 * q, column], q]
    b = incoming[slots[2 * q + 1, column], q]
    return _halves(a, b)


def _pick_kernel(slots, incoming, first, final):
    per, tiles = first.shape[0], incoming.shape[1]

    def body(j, carry):
        first[j] = _choose(slots, incoming, j, 0)
        final[j] = _choose(slots, incoming, j, tiles - 1)
        return carry

    lax.fori_loop(0, per, body, 0)


def _spread_kinds(scratch, kinds, taper):
    for t, v in enumerate(_spread(scratch, 0, kinds)):
        for c, part in enumerate(_taper(v)):
            taper[c, t] = part


def _natural(pend, hold, order):
    mix, count = pend.shape[1], pend.shape[2]
    v = jnp.concatenate([pend[hold, u, t] for u in range(mix) for t in range(count)], axis=0)
    v = _reorder(v, order) * (1.0 / SCALE)
    return [[v[(u * count + t) * TILE:(u * count + t + 1) * TILE] for t in range(count)] for u in range(mix)]


def _pipeline(steps, mix, compute, pend, order, done, copy):
    def flush(k):
        for u, column in enumerate(_natural(pend, k % 2, order)):
            for t, v in enumerate(column):
                done[k * mix + u, t] = v

    def first(k):
        for u, column in enumerate(compute(k)):
            for t, v in enumerate(column):
                pend[k % 2, u, t] = v

    first(0)

    def body(k, carry):
        flush(k - 1)
        first(k)
        copy(k - 1).start()
        return carry

    lax.fori_loop(1, steps, body, 0)
    flush(steps - 1)
    copy(steps - 1).start()
    for k in range(steps):
        copy(k).wait()


def _final_inner_kernel(slots, incoming, natural, every, order, out, done, pend, scaled, taper, work, sems, *, half, mix):
    tiles, width = natural.shape[0] - 2, natural.shape[2]
    for t, v in enumerate(_spread(work, 0, [natural[t + 1] for t in range(tiles)])):
        scaled[t] = v
    _spread_kinds(work, [every[t + 1] for t in range(tiles)], taper)

    def weights(t):
        return [_widen(taper[c, t], width) for c in range(3)]

    def copy(k):
        return pltpu.make_async_copy(
            done.at[pl.ds(k * mix, mix)], out.at[pl.ds(k * mix, mix), pl.ds(1, tiles - 2)], sems.at[k])

    def compute(k):
        cur = []
        for u in range(mix):
            mine = _spread(work, u, [_choose(slots, incoming, k * mix + u, t) for t in range(tiles)])
            cur.append(_blend(mine, weights, {}))
        res = _steps(cur, lambda t: scaled[t], {})
        return [_collect(work, u, res[u], range(1, tiles - 1)) for u in range(mix)]

    _pipeline(half // mix, mix, compute, pend, order, done, copy)


def _final_rest_kernel(slots, incoming, first, final, below, above, natural, every, order, prior, out,
                       edges, done, pend, scaled, taper, ends, taper3, work, sems, *, per, half, mix, edge_mix, bands):
    count, width = natural.shape[0], natural.shape[2]
    tiles = count - 2
    last = tiles - 1
    rows = tiles * TILE
    for s in range(2):
        for t, v in enumerate(_spread(work, s, [natural[last * s + t] for t in range(3)])):
            ends[s, t] = v
        _spread_kinds(work, [every[last * s + t] for t in range(3)], taper3.at[s])
    for t, v in enumerate(_spread(work, 2, [natural[t] for t in range(count)])):
        scaled[t] = v
    _spread_kinds(work, [every[t] for t in range(count)], taper)
    mask = _masks(slots[slots.shape[0] - 1, 0], bands)
    steps = (per - half) // mix

    def finish(s):
        return pltpu.make_async_copy(edges.at[s], out.at[pl.ds(0, half), last * s], sems.at[steps + s])

    def edge(k, carry):
        for s in range(2):
            mask3 = _border(3, width, (TILE - 1, mask[0]) if s == 0 else (2 * TILE, mask[1]))
            cur = []
            for u in range(edge_mix):
                j = k * edge_mix + u
                inner = _choose(slots, incoming, j, 1 if s == 0 else last - 1)
                three = [below[j], first[j], inner] if s == 0 else [inner, final[j], above[j]]
                cur.append(_blend(_spread(work, u, three),
                                  lambda t: [_widen(taper3[s, c, t], width) for c in range(3)], mask3))
            res = _steps(cur, lambda t: ends[s, t], mask3)
            for u in range(edge_mix):
                edges[s, k * edge_mix + u] = _collect(work, u, res[u], [1])[0]
        return carry

    lax.fori_loop(0, half // edge_mix, edge, 0)
    v = jnp.concatenate([edges[s, j] for s in range(2) for j in range(half)], axis=0)
    v = _reorder(v, order) * (1.0 / SCALE)
    for s in range(2):
        for j in range(half):
            at = (s * half + j) * TILE
            edges[s, j] = v[at:at + TILE]
    for s in range(2):
        finish(s).start()

    def copy(k):
        return pltpu.make_async_copy(
            done.at[pl.ds(k * mix, mix)], out.at[pl.ds(half + k * mix, mix)], sems.at[k])

    def compute(k):
        masks = _border(count, width, (TILE - 1, mask[0]), (TILE + rows, mask[1]))
        cur = []
        for u in range(mix):
            j = half + k * mix + u
            mine = [below[j], first[j]]
            mine += [_choose(slots, incoming, j, t) for t in range(1, last)]
            mine += [final[j], above[j]]
            cur.append(_blend(_spread(work, u, mine), lambda t: [_widen(taper[c, t], width) for c in range(3)],
                              masks))
        res = _steps(cur, lambda t: scaled[t], masks)
        return [_collect(work, u, res[u], range(1, count - 1)) for u in range(mix)]

    _pipeline(steps, mix, compute, pend, order, done, copy)
    for s in range(2):
        finish(s).wait()


def _pin(x):
    return pltpu.with_memory_space_constraint(x, pltpu.HBM)


def _call(kernel, name, outs, scratch, spaces, out_spaces, alias=None):
    def spec(kind):
        return pl.BlockSpec(memory_space={"v": pltpu.VMEM, "s": pltpu.SMEM, "a": pl.ANY, "h": pltpu.HBM}[kind])

    specs = [spec(k) for k in out_spaces]
    single = len(outs) == 1
    return pl.pallas_call(
        kernel,
        in_specs=[spec(k) for k in spaces],
        out_specs=specs[0] if single else specs,
        out_shape=outs[0] if single else outs,
        scratch_shapes=scratch,
        input_output_aliases=alias or {},
        compiler_params=pltpu.CompilerParams(vmem_limit_bytes=40 * 1024 * 1024),
        name=name,
    )


def on_device(state, forcing, parents, taper_index):
    per, rows, width = state.shape
    tiles = rows // TILE
    groups = lax.axis_size("pgroup")
    bands = lax.axis_size("band")
    f32 = jnp.float32
    forward = [(i, i + 1) for i in range(bands - 1)]
    backward = [(b, a) for a, b in forward]
    info = jnp.stack([lax.axis_index("pgroup"), lax.axis_index("band")]).astype(jnp.int32)
    state4 = state.reshape(per, tiles, TILE, width)
    pinned = _pin(state4)
    drive = forcing.reshape(tiles, TILE, width)
    entries = groups * CAP
    dma = pltpu.SemaphoreType.DMA
    vmem = pltpu.VMEM

    def shape(*dims, dtype=f32):
        return jax.ShapeDtypeStruct(dims, dtype)

    patches, count = parents.shape
    i32 = jnp.int32
    head, tail, kinds, ends, own, state4, drive = _call(
        functools.partial(_prep_kernel, per=per, tiles=tiles), "prepare",
        [shape(per + 2, TILE, width), shape(per + 2, TILE, width), shape(tiles, TILE, 128),
         shape(CAP, patches + TILE, count, dtype=i32), shape(patches + TILE, LANES, dtype=i32),
         shape(per, tiles, TILE, width), shape(tiles, TILE, width)],
        [pltpu.SMEM((rows,), i32), vmem((patches, count), i32), dma((8,))], "shhhh", "vvvvvvv",
    )(info, _pin(taper_index), pinned, _pin(drive), _pin(parents))
    low = lax.ppermute(tail, "band", forward)
    high = lax.ppermute(head, "band", backward)

    half = per // 2

    def work(count, height):
        return vmem((count, width // LANES, height * TILE, LANES), f32)

    extra = [vmem((tiles + 2, TILE, width), f32), vmem((2, 3, TILE, width), f32)]
    square = shape(width, width, dtype=jnp.bfloat16)
    state4, order, back = _call(
        functools.partial(_order_kernel, mix=4), "reorder", [shape(per, tiles, TILE, width), square, square], [], "v", "vvv",
    )(state4)
    message, natural, every = _call(
        functools.partial(_advance_kernel, mix=2, groups=groups, bands=bands), "advance",
        [shape(groups, CAP, tiles, TILE, width), shape(tiles + 2, TILE, width), shape(tiles + 2, TILE, LANES)],
        [vmem((per, tiles, TILE, width), f32), vmem((per + 1, TILE, width), f32), vmem((per + 1, TILE, width), f32),
         extra[0], work(2, tiles + 2)], "svvvvvv", "vvv",
    )(ends, state4, low, high, drive, kinds, order)

    incoming = lax.all_to_all(message, "pgroup", split_axis=0, concat_axis=0, tiled=True)
    incoming = incoming.reshape(entries, tiles, TILE, width)

    first, final = _call(
        _pick_kernel, "pick_edge", [shape(per, TILE, width), shape(per, TILE, width)], [], "sv", "vv",
    )(own, incoming)
    below = lax.ppermute(final, "band", forward)
    above = lax.ppermute(first, "band", backward)

    pairs = half // 2
    field = _call(
        functools.partial(_final_inner_kernel, half=half, mix=2), "final_inner", [shape(per, tiles, TILE, width)],
        [vmem((half, tiles - 2, TILE, width), f32), vmem((2, 2, tiles - 2, TILE, width), f32),
         vmem((tiles, TILE, width), f32), vmem((3, tiles, TILE, LANES), f32), work(2, tiles),
         dma((pairs,))], "svvvv", "a",
    )(own, incoming, natural, every, back)
    field = _call(
        functools.partial(_final_rest_kernel, per=per, half=half, mix=2, edge_mix=4, bands=bands), "final_rest",
        [shape(per, tiles, TILE, width)],
        [vmem((2, half, TILE, width), f32), vmem((per - half, tiles, TILE, width), f32),
         vmem((2, 2, tiles, TILE, width), f32), extra[0], vmem((3, tiles + 2, TILE, LANES), f32), extra[1],
         vmem((2, 3, 3, TILE, LANES), f32), work(4, tiles + 2), dma((pairs + 2,))],
        "svvvvvvvva", "a", {9: 0},
    )(own, incoming, first, final, below, above, natural, every, back, field)
    return field.reshape(per, rows, width)


def solution(mesh):
    return jax.shard_map(
        on_device,
        mesh=mesh,
        in_specs=(P("pgroup", "band", None), P("band", None), P("band", None), P("band")),
        out_specs=P("pgroup", "band", None),
        check_vma=False,
    )
```

```python
import functools

import jax
import jax.numpy as jnp
from jax import lax
from jax.experimental import pallas as pl
from jax.experimental.pallas import tpu as pltpu
from jax.sharding import PartitionSpec as P

PATCH_ROWS = 4
STEPS = 6
CAP = 2
TILE = 8
SCALE = 0.05


def _sub(shape):
    return lax.broadcasted_iota(jnp.int32, shape, 0)


def _north(tiles, i, k):
    count = len(tiles)
    return tiles[i + k] if i + k < count else pltpu.roll(tiles[i + k - count], TILE - 1, 0)


def _south(tiles, i, k):
    return tiles[i - k] if i >= k else pltpu.roll(tiles[i - k + len(tiles)], 1, 0)


def _step(tiles, i, drive):
    m = tiles[i]
    width = m.shape[1]
    e = jnp.concatenate([m[:, LANES:], pltpu.roll(m[:, :LANES], LANES - 1, 1)], axis=1)
    w = jnp.concatenate([pltpu.roll(m[:, width - LANES:], 1, 1), m[:, :width - LANES]], axis=1)
    n = _north(tiles, i, 1)
    s = _south(tiles, i, 1)
    return (m * (0.4 - (e - w)) + 0.15 * (e + w)) + (0.05 * n + 0.25 * s) + drive


def _steps(groups, drive, masks):
    for repeat in range(STEPS):
        fresh = [list(tiles) for tiles in groups]
        for i in range(len(groups[0])):
            source = drive(i)
            for tiles, new in zip(groups, fresh):
                v = _step(tiles, i, source)
                new[i] = v * masks[i] if i in masks else v
        groups = fresh
    return groups


def _blend(tiles, weights, masks):
    fresh = []
    for i in range(len(tiles)):
        w0, w1, w2 = weights(i)
        total = w0 * tiles[i]
        total = total + w1 * (_north(tiles, i, 1) + _south(tiles, i, 1))
        total = total + w2 * (_north(tiles, i, 2) + _south(tiles, i, 2))
        fresh.append(total * masks[i] if i in masks else total)
    return fresh


LANES = 128


def _fill_order(ref, back):
    size = ref.shape[0]
    chunks = size // LANES
    step = 64
    for r in range(0, size, step):
        row = lax.broadcasted_iota(jnp.int32, (step, size), 0) + r
        column = lax.broadcasted_iota(jnp.int32, (step, size), 1)
        natural, mixed = (column, row) if back else (row, column)
        hit = natural == chunks * (mixed % LANES) + mixed // LANES
        ref[r:r + step, :] = jnp.where(hit, 1.0, 0.0).astype(jnp.bfloat16)


def _reorder(v, order):
    rows = v.shape[0]
    high = v.astype(jnp.bfloat16)
    rest = (v - high.astype(jnp.float32)).astype(jnp.bfloat16)
    both = jnp.dot(jnp.concatenate([high, rest], axis=0), order[...], preferred_element_type=jnp.float32)
    return both[:rows] + both[rows:]


def _spread(scratch, u, natural):
    count = len(natural)
    chunks = natural[0].shape[1] // LANES
    for t, v in enumerate(natural):
        for c in range(chunks):
            scratch[u, c, t * TILE:(t + 1) * TILE, :] = v[:, c * LANES:(c + 1) * LANES]
    return [jnp.concatenate([scratch[u, c, pl.ds(i, TILE, count), :] for c in range(chunks)], axis=1)
            for i in range(count)]


def _collect(scratch, u, tiles, keep):
    count = len(tiles)
    chunks = tiles[0].shape[1] // LANES
    for i, v in enumerate(tiles):
        for c in range(chunks):
            scratch[u, c, pl.ds(i, TILE, count), :] = v[:, c * LANES:(c + 1) * LANES]
    return [jnp.concatenate([scratch[u, c, t * TILE:(t + 1) * TILE, :] for c in range(chunks)], axis=1) for t in keep]


def _border(count, width, *rows):
    return {at % count: jnp.where(_sub((TILE, width)) == at // count, factor, jnp.float32(1.0)) for at, factor in rows}


def _taper(kind):
    rate = 0.2 * (kind + 1.0)
    near = jnp.exp(-rate)
    far = jnp.exp(-4.0 * rate)
    inv = 1.0 / (far + near + 1.0 + near + far)
    return inv, near * inv, far * inv


def _halves(a, b):
    return jnp.where(_sub(a.shape) < PATCH_ROWS, a, b)


def _widen(v, width):
    return jnp.concatenate([v] * (width // v.shape[1]), axis=1)


def _prep_kernel(taper_in, state, forcing, head, tail, taper, sems, *, per, tiles):
    last = tiles - 1
    first = pltpu.make_async_copy(taper_in, taper, sems.at[4])
    copies = [
        pltpu.make_async_copy(state.at[:, 0], head.at[pl.ds(0, per)], sems.at[0]),
        pltpu.make_async_copy(state.at[:, last], tail.at[pl.ds(0, per)], sems.at[1]),
        pltpu.make_async_copy(forcing.at[0], head.at[per], sems.at[2]),
        pltpu.make_async_copy(forcing.at[last], tail.at[per], sems.at[3]),
    ]
    for c in [first] + copies:
        c.start()
    first.wait()
    width = head.shape[2]
    for r in range(TILE):
        for out, t in ((head, 0), (tail, last)):
            value = taper[t * TILE + r].astype(jnp.float32)
            out[per + 1, r:r + 1, :] = jnp.full((1, width), value, jnp.float32)
    for c in copies:
        c.wait()


def _order_kernel(info, taper, state, forcing, parents, out, order, back, kinds, ends, own, drive, local, sems, *, mix):
    per, tiles, _, width = out.shape
    steps = per // mix

    def load(k):
        return pltpu.make_async_copy(state.at[pl.ds(k * mix, mix)], local.at[pl.ds(k * mix, mix)], sems.at[k])

    for k in range(steps):
        load(k).start()
    drive[...] = forcing[...]
    for t in range(tiles):
        for r in range(TILE):
            value = taper[t * TILE + r].astype(jnp.float32)
            kinds[t, r:r + 1, :] = jnp.full((1, kinds.shape[2]), value, jnp.float32)
    p = parents[...]
    count = p.shape[1]
    owner = p // per
    inside = p - owner * per
    mine = owner == info[0]
    lo = jnp.where(mine, inside, per - 1)
    hi = jnp.where(mine, inside, 0)
    shift = 1
    while shift < per:
        lo = jnp.minimum(lo, pltpu.roll(lo, count - shift, 1))
        hi = jnp.maximum(hi, pltpu.roll(hi, count - shift, 1))
        shift *= 2
    patches = p.shape[0]
    for slot, v in enumerate((lo, hi)):
        ends[slot, pl.ds(0, patches), :] = v
        ends[slot, pl.ds(patches, TILE), :] = jnp.full((TILE, count), info[1], jnp.int32)
    lane = lax.broadcasted_iota(jnp.int32, p.shape, 1) % per
    rank = jnp.zeros_like(p)
    for shift in range(1, per):
        other = jnp.where(lane + shift < per, pltpu.roll(p, count - shift, 1), pltpu.roll(p, per - shift, 1))
        rank = jnp.where((other // per == owner) & (other < p), 1, rank)
    turn = (count - info[0] * per) % count
    own[pl.ds(0, patches), :] = pltpu.roll(owner * CAP + rank, turn, 1)[:, :LANES]
    own[pl.ds(patches, TILE), :] = jnp.full((TILE, LANES), info[1], jnp.int32)
    _fill_order(order, False)
    _fill_order(back, True)

    def body(k, carry):
        load(k).wait()
        v = jnp.concatenate([local[k * mix + u, t] for u in range(mix) for t in range(tiles)], axis=0) * SCALE
        v = _reorder(v, order)
        for u in range(mix):
            for t in range(tiles):
                at = (u * tiles + t) * TILE
                out[k * mix + u, t] = v[at:at + TILE]
        return carry

    lax.fori_loop(0, steps, body, 0)


def _advance_kernel(table, state, low_in, high_in, drive, kinds, order, out, natural, every, field, low, high,
                    scaled, work, *, mix, groups, bands):
    per, tiles = state.shape[0], state.shape[1]
    count = tiles + 2
    rows = tiles * TILE
    width = state.shape[3]
    both = [low_in[j] for j in range(per + 1)] + [high_in[j] for j in range(per + 1)] + [drive[t] for t in range(tiles)]
    v = _reorder(jnp.concatenate(both, axis=0) * SCALE, order)
    for j in range(per + 1):
        low[j] = v[j * TILE:(j + 1) * TILE]
        high[j] = v[(per + 1 + j) * TILE:(per + 2 + j) * TILE]
    natural[0] = low[per]
    natural[count - 1] = high[per]
    every[0] = low_in[per + 1, :, :LANES]
    every[count - 1] = high_in[per + 1, :, :LANES]
    for t in range(tiles):
        at = (2 * per + 2 + t) * TILE
        natural[t + 1] = v[at:at + TILE]
        every[t + 1] = kinds[t]
    for t, v in enumerate(_spread(work, 0, [natural[t] for t in range(count)])):
        scaled[t] = v
    mask = _masks(table[0, table.shape[1] - 1, 0], bands)

    def whole(k, carry):
        masks = _border(count, width, (TILE - 1, mask[0]), (TILE + rows, mask[1]))
        at = [k * mix + u for u in range(mix)]
        cur = [_spread(work, u, [low[j]] + [state[j, t] for t in range(tiles)] + [high[j]]) for u, j in enumerate(at)]
        res = _steps(cur, lambda t: scaled[t], masks)
        keep = range(1, count - 1)
        for u, j in enumerate(at):
            for t, v in zip(keep, _collect(work, u, res[u], keep)):
                field[j, t - 1] = v
        return carry

    lax.fori_loop(0, per // mix, whole, 0)

    def pack(g, carry):
        for q in range(tiles):
            for slot in range(CAP):
                first = table[slot, 2 * q, g * per]
                second = table[slot, 2 * q + 1, g * per]
                out[g, slot, q] = _halves(field[first, q], field[second, q])
        return carry

    lax.fori_loop(0, groups, pack, 0)


def _masks(band, bands):
    one = jnp.float32(1.0)
    zero = jnp.float32(0.0)
    return [jnp.where(band > 0, one, zero), jnp.where(band < bands - 1, one, zero)]


def _choose(slots, incoming, column, q):
    a = incoming[slots[2 * q, column], q]
    b = incoming[slots[2 * q + 1, column], q]
    return _halves(a, b)


def _pick_kernel(slots, incoming, first, final):
    per, tiles = first.shape[0], incoming.shape[1]

    def body(j, carry):
        first[j] = _choose(slots, incoming, j, 0)
        final[j] = _choose(slots, incoming, j, tiles - 1)
        return carry

    lax.fori_loop(0, per, body, 0)


def _spread_kinds(scratch, kinds, taper):
    for t, v in enumerate(_spread(scratch, 0, kinds)):
        for c, part in enumerate(_taper(v)):
            taper[c, t] = part


def _natural(pend, hold, order):
    mix, count = pend.shape[1], pend.shape[2]
    v = jnp.concatenate([pend[hold, u, t] for u in range(mix) for t in range(count)], axis=0)
    v = _reorder(v, order) * (1.0 / SCALE)
    return [[v[(u * count + t) * TILE:(u * count + t + 1) * TILE] for t in range(count)] for u in range(mix)]


def _pipeline(steps, mix, compute, pend, order, done, copy):
    def flush(k):
        for u, column in enumerate(_natural(pend, k % 2, order)):
            for t, v in enumerate(column):
                done[k * mix + u, t] = v

    def first(k):
        for u, column in enumerate(compute(k)):
            for t, v in enumerate(column):
                pend[k % 2, u, t] = v

    first(0)

    def body(k, carry):
        flush(k - 1)
        first(k)
        copy(k - 1).start()
        return carry

    lax.fori_loop(1, steps, body, 0)
    flush(steps - 1)
    copy(steps - 1).start()
    for k in range(steps):
        copy(k).wait()


def _final_inner_kernel(slots, incoming, natural, every, order, out, done, pend, scaled, taper, work, sems, *, half, mix):
    tiles, width = natural.shape[0] - 2, natural.shape[2]
    for t, v in enumerate(_spread(work, 0, [natural[t + 1] for t in range(tiles)])):
        scaled[t] = v
    _spread_kinds(work, [every[t + 1] for t in range(tiles)], taper)

    def weights(t):
        return [_widen(taper[c, t], width) for c in range(3)]

    def copy(k):
        return pltpu.make_async_copy(
            done.at[pl.ds(k * mix, mix)], out.at[pl.ds(k * mix, mix), pl.ds(1, tiles - 2)], sems.at[k])

    def compute(k):
        cur = []
        for u in range(mix):
            mine = _spread(work, u, [_choose(slots, incoming, k * mix + u, t) for t in range(tiles)])
            cur.append(_blend(mine, weights, {}))
        res = _steps(cur, lambda t: scaled[t], {})
        return [_collect(work, u, res[u], range(1, tiles - 1)) for u in range(mix)]

    _pipeline(half // mix, mix, compute, pend, order, done, copy)


def _final_rest_kernel(slots, incoming, first, final, below, above, natural, every, order, prior, out,
                       edges, done, pend, scaled, taper, ends, taper3, work, sems, *, per, half, mix, edge_mix, bands):
    count, width = natural.shape[0], natural.shape[2]
    tiles = count - 2
    last = tiles - 1
    rows = tiles * TILE
    for s in range(2):
        for t, v in enumerate(_spread(work, s, [natural[last * s + t] for t in range(3)])):
            ends[s, t] = v
        _spread_kinds(work, [every[last * s + t] for t in range(3)], taper3.at[s])
    for t, v in enumerate(_spread(work, 2, [natural[t] for t in range(count)])):
        scaled[t] = v
    _spread_kinds(work, [every[t] for t in range(count)], taper)
    mask = _masks(slots[slots.shape[0] - 1, 0], bands)
    steps = (per - half) // mix

    def finish(s):
        return pltpu.make_async_copy(edges.at[s], out.at[pl.ds(0, half), last * s], sems.at[steps + s])

    def edge(k, carry):
        for s in range(2):
            mask3 = _border(3, width, (TILE - 1, mask[0]) if s == 0 else (2 * TILE, mask[1]))
            cur = []
            for u in range(edge_mix):
                j = k * edge_mix + u
                inner = _choose(slots, incoming, j, 1 if s == 0 else last - 1)
                three = [below[j], first[j], inner] if s == 0 else [inner, final[j], above[j]]
                cur.append(_blend(_spread(work, u, three),
                                  lambda t: [_widen(taper3[s, c, t], width) for c in range(3)], mask3))
            res = _steps(cur, lambda t: ends[s, t], mask3)
            for u in range(edge_mix):
                edges[s, k * edge_mix + u] = _collect(work, u, res[u], [1])[0]
        return carry

    lax.fori_loop(0, half // edge_mix, edge, 0)
    v = jnp.concatenate([edges[s, j] for s in range(2) for j in range(half)], axis=0)
    v = _reorder(v, order) * (1.0 / SCALE)
    for s in range(2):
        for j in range(half):
            at = (s * half + j) * TILE
            edges[s, j] = v[at:at + TILE]
    for s in range(2):
        finish(s).start()

    def copy(k):
        return pltpu.make_async_copy(
            done.at[pl.ds(k * mix, mix)], out.at[pl.ds(half + k * mix, mix)], sems.at[k])

    def compute(k):
        masks = _border(count, width, (TILE - 1, mask[0]), (TILE + rows, mask[1]))
        cur = []
        for u in range(mix):
            j = half + k * mix + u
            mine = [below[j], first[j]]
            mine += [_choose(slots, incoming, j, t) for t in range(1, last)]
            mine += [final[j], above[j]]
            cur.append(_blend(_spread(work, u, mine), lambda t: [_widen(taper[c, t], width) for c in range(3)],
                              masks))
        res = _steps(cur, lambda t: scaled[t], masks)
        return [_collect(work, u, res[u], range(1, count - 1)) for u in range(mix)]

    _pipeline(steps, mix, compute, pend, order, done, copy)
    for s in range(2):
        finish(s).wait()


def _pin(x):
    return pltpu.with_memory_space_constraint(x, pltpu.HBM)


def _call(kernel, name, outs, scratch, spaces, out_spaces, alias=None):
    def spec(kind):
        return pl.BlockSpec(memory_space={"v": pltpu.VMEM, "s": pltpu.SMEM, "a": pl.ANY, "h": pltpu.HBM}[kind])

    specs = [spec(k) for k in out_spaces]
    single = len(outs) == 1
    return pl.pallas_call(
        kernel,
        in_specs=[spec(k) for k in spaces],
        out_specs=specs[0] if single else specs,
        out_shape=outs[0] if single else outs,
        scratch_shapes=scratch,
        input_output_aliases=alias or {},
        compiler_params=pltpu.CompilerParams(vmem_limit_bytes=40 * 1024 * 1024),
        name=name,
    )


def on_device(state, forcing, parents, taper_index):
    per, rows, width = state.shape
    tiles = rows // TILE
    groups = lax.axis_size("pgroup")
    bands = lax.axis_size("band")
    f32 = jnp.float32
    forward = [(i, i + 1) for i in range(bands - 1)]
    backward = [(b, a) for a, b in forward]
    info = jnp.stack([lax.axis_index("pgroup"), lax.axis_index("band")]).astype(jnp.int32)
    state4 = state.reshape(per, tiles, TILE, width)
    pinned = _pin(state4)
    drive = forcing.reshape(tiles, TILE, width)
    entries = groups * CAP
    dma = pltpu.SemaphoreType.DMA
    vmem = pltpu.VMEM

    def shape(*dims, dtype=f32):
        return jax.ShapeDtypeStruct(dims, dtype)

    patches, count = parents.shape
    i32 = jnp.int32
    head, tail = _call(
        functools.partial(_prep_kernel, per=per, tiles=tiles), "prepare",
        [shape(per + 2, TILE, width), shape(per + 2, TILE, width)],
        [pltpu.SMEM((rows,), i32), dma((5,))], "hhh", "vv",
    )(_pin(taper_index), pinned, _pin(drive))
    low = lax.ppermute(tail, "band", forward)
    high = lax.ppermute(head, "band", backward)

    half = per // 2

    def work(count, height):
        return vmem((count, width // LANES, height * TILE, LANES), f32)

    extra = [vmem((tiles + 2, TILE, width), f32), vmem((2, 3, TILE, width), f32)]
    square = shape(width, width, dtype=jnp.bfloat16)
    state4, order, back, kinds, ends, own, drive = _call(
        functools.partial(_order_kernel, mix=4), "reorder",
        [shape(per, tiles, TILE, width), square, square, shape(tiles, TILE, LANES),
         shape(CAP, patches + TILE, count, dtype=i32), shape(patches + TILE, LANES, dtype=i32),
         shape(tiles, TILE, width)],
        [vmem((per, tiles, TILE, width), f32), dma((per // 4,))], "sshvv", "v" * 7,
    )(info, taper_index, pinned, drive, parents)
    message, natural, every = _call(
        functools.partial(_advance_kernel, mix=2, groups=groups, bands=bands), "advance",
        [shape(groups, CAP, tiles, TILE, width), shape(tiles + 2, TILE, width), shape(tiles + 2, TILE, LANES)],
        [vmem((per, tiles, TILE, width), f32), vmem((per + 1, TILE, width), f32), vmem((per + 1, TILE, width), f32),
         extra[0], work(2, tiles + 2)], "svvvvvv", "vvv",
    )(ends, state4, low, high, drive, kinds, order)

    incoming = lax.all_to_all(message, "pgroup", split_axis=0, concat_axis=0, tiled=True)
    incoming = incoming.reshape(entries, tiles, TILE, width)

    first, final = _call(
        _pick_kernel, "pick_edge", [shape(per, TILE, width), shape(per, TILE, width)], [], "sv", "vv",
    )(own, incoming)
    below = lax.ppermute(final, "band", forward)
    above = lax.ppermute(first, "band", backward)

    pairs = half // 2
    field = _call(
        functools.partial(_final_inner_kernel, half=half, mix=2), "final_inner", [shape(per, tiles, TILE, width)],
        [vmem((half, tiles - 2, TILE, width), f32), vmem((2, 2, tiles - 2, TILE, width), f32),
         vmem((tiles, TILE, width), f32), vmem((3, tiles, TILE, LANES), f32), work(2, tiles),
         dma((pairs,))], "svvvv", "a",
    )(own, incoming, natural, every, back)
    field = _call(
        functools.partial(_final_rest_kernel, per=per, half=half, mix=2, edge_mix=4, bands=bands), "final_rest",
        [shape(per, tiles, TILE, width)],
        [vmem((2, half, TILE, width), f32), vmem((per - half, tiles, TILE, width), f32),
         vmem((2, 2, tiles, TILE, width), f32), extra[0], vmem((3, tiles + 2, TILE, LANES), f32), extra[1],
         vmem((2, 3, 3, TILE, LANES), f32), work(4, tiles + 2), dma((pairs + 2,))],
        "svvvvvvvva", "a", {9: 0},
    )(own, incoming, first, final, below, above, natural, every, back, field)
    return field.reshape(per, rows, width)


def solution(mesh):
    return jax.shard_map(
        on_device,
        mesh=mesh,
        in_specs=(P("pgroup", "band", None), P("band", None), P("band", None), P("band")),
        out_specs=P("pgroup", "band", None),
        check_vma=False,
    )
```

```python
import functools

import jax
import jax.numpy as jnp
from jax import lax
from jax.experimental import pallas as pl
from jax.experimental.pallas import tpu as pltpu
from jax.sharding import PartitionSpec as P

PATCH_ROWS = 4
STEPS = 6
CAP = 2
TILE = 8
SCALE = 0.05


def _sub(shape):
    return lax.broadcasted_iota(jnp.int32, shape, 0)


def _north(tiles, i, k):
    count = len(tiles)
    return tiles[i + k] if i + k < count else pltpu.roll(tiles[i + k - count], TILE - 1, 0)


def _south(tiles, i, k):
    return tiles[i - k] if i >= k else pltpu.roll(tiles[i - k + len(tiles)], 1, 0)


def _step(tiles, i, drive):
    m = tiles[i]
    width = m.shape[1]
    e = jnp.concatenate([m[:, LANES:], pltpu.roll(m[:, :LANES], LANES - 1, 1)], axis=1)
    w = jnp.concatenate([pltpu.roll(m[:, width - LANES:], 1, 1), m[:, :width - LANES]], axis=1)
    n = _north(tiles, i, 1)
    s = _south(tiles, i, 1)
    return (m * (0.4 - (e - w)) + 0.15 * (e + w)) + (0.05 * n + 0.25 * s) + drive


def _steps(groups, drive, masks):
    for repeat in range(STEPS):
        fresh = [list(tiles) for tiles in groups]
        for i in range(len(groups[0])):
            source = drive(i)
            for tiles, new in zip(groups, fresh):
                v = _step(tiles, i, source)
                new[i] = v * masks[i] if i in masks else v
        groups = fresh
    return groups


def _blend(tiles, weights, masks):
    fresh = []
    for i in range(len(tiles)):
        w0, w1, w2 = weights(i)
        total = w0 * tiles[i]
        total = total + w1 * (_north(tiles, i, 1) + _south(tiles, i, 1))
        total = total + w2 * (_north(tiles, i, 2) + _south(tiles, i, 2))
        fresh.append(total * masks[i] if i in masks else total)
    return fresh


LANES = 128


def _fill_order(ref, back):
    size = ref.shape[0]
    chunks = size // LANES
    step = 64
    for r in range(0, size, step):
        row = lax.broadcasted_iota(jnp.int32, (step, size), 0) + r
        column = lax.broadcasted_iota(jnp.int32, (step, size), 1)
        natural, mixed = (column, row) if back else (row, column)
        hit = natural == chunks * (mixed % LANES) + mixed // LANES
        ref[r:r + step, :] = jnp.where(hit, 1.0, 0.0).astype(jnp.bfloat16)


def _reorder(v, order):
    rows = v.shape[0]
    high = v.astype(jnp.bfloat16)
    rest = (v - high.astype(jnp.float32)).astype(jnp.bfloat16)
    both = jnp.dot(jnp.concatenate([high, rest], axis=0), order[...], preferred_element_type=jnp.float32)
    return both[:rows] + both[rows:]


def _spread(scratch, u, natural):
    count = len(natural)
    chunks = natural[0].shape[1] // LANES
    for t, v in enumerate(natural):
        for c in range(chunks):
            scratch[u, c, t * TILE:(t + 1) * TILE, :] = v[:, c * LANES:(c + 1) * LANES]
    return [jnp.concatenate([scratch[u, c, pl.ds(i, TILE, count), :] for c in range(chunks)], axis=1)
            for i in range(count)]


def _collect(scratch, u, tiles, keep):
    count = len(tiles)
    chunks = tiles[0].shape[1] // LANES
    for i, v in enumerate(tiles):
        for c in range(chunks):
            scratch[u, c, pl.ds(i, TILE, count), :] = v[:, c * LANES:(c + 1) * LANES]
    return [jnp.concatenate([scratch[u, c, t * TILE:(t + 1) * TILE, :] for c in range(chunks)], axis=1) for t in keep]


def _border(count, width, *rows):
    return {at % count: jnp.where(_sub((TILE, width)) == at // count, factor, jnp.float32(1.0)) for at, factor in rows}


def _taper(kind):
    rate = 0.2 * (kind + 1.0)
    near = jnp.exp(-rate)
    far = jnp.exp(-4.0 * rate)
    inv = 1.0 / (far + near + 1.0 + near + far)
    return inv, near * inv, far * inv


def _halves(a, b):
    return jnp.where(_sub(a.shape) < PATCH_ROWS, a, b)


def _widen(v, width):
    return jnp.concatenate([v] * (width // v.shape[1]), axis=1)


def _prep_kernel(taper_in, state, forcing, head, tail, taper, sems, *, per, tiles):
    last = tiles - 1
    first = pltpu.make_async_copy(taper_in, taper, sems.at[4])
    copies = [
        pltpu.make_async_copy(state.at[:, 0], head.at[pl.ds(0, per)], sems.at[0]),
        pltpu.make_async_copy(state.at[:, last], tail.at[pl.ds(0, per)], sems.at[1]),
        pltpu.make_async_copy(forcing.at[0], head.at[per], sems.at[2]),
        pltpu.make_async_copy(forcing.at[last], tail.at[per], sems.at[3]),
    ]
    for c in [first] + copies:
        c.start()
    first.wait()
    width = head.shape[2]
    for r in range(TILE):
        for out, t in ((head, 0), (tail, last)):
            value = taper[t * TILE + r].astype(jnp.float32)
            out[per + 1, r:r + 1, :] = jnp.full((1, width), value, jnp.float32)
    for c in copies:
        c.wait()


def _order_kernel(info, taper, state, forcing, parents, out, order, back, kinds, ends, own, drive, local, sems, *, mix):
    per, tiles, _, width = out.shape
    steps = per // mix

    def load(k):
        return pltpu.make_async_copy(state.at[pl.ds(k * mix, mix)], local.at[pl.ds(k * mix, mix)], sems.at[k])

    for k in range(steps):
        load(k).start()
    drive[...] = forcing[...]
    for t in range(tiles):
        for r in range(TILE):
            value = taper[t * TILE + r].astype(jnp.float32)
            kinds[t, r:r + 1, :] = jnp.full((1, kinds.shape[2]), value, jnp.float32)
    p = parents[...]
    count = p.shape[1]
    owner = p // per
    inside = p - owner * per
    mine = owner == info[0]
    lo = jnp.where(mine, inside, per - 1)
    hi = jnp.where(mine, inside, 0)
    shift = 1
    while shift < per:
        lo = jnp.minimum(lo, pltpu.roll(lo, count - shift, 1))
        hi = jnp.maximum(hi, pltpu.roll(hi, count - shift, 1))
        shift *= 2
    patches = p.shape[0]
    for slot, v in enumerate((lo, hi)):
        ends[slot] = v
    lane = lax.broadcasted_iota(jnp.int32, p.shape, 1) % per
    rank = jnp.zeros_like(p)
    for shift in range(1, per):
        other = jnp.where(lane + shift < per, pltpu.roll(p, count - shift, 1), pltpu.roll(p, per - shift, 1))
        rank = jnp.where((other // per == owner) & (other < p), 1, rank)
    turn = (count - info[0] * per) % count
    own[pl.ds(0, patches), :] = pltpu.roll(owner * CAP + rank, turn, 1)[:, :LANES]
    own[pl.ds(patches, TILE), :] = jnp.full((TILE, LANES), info[1], jnp.int32)
    _fill_order(order, False)
    _fill_order(back, True)

    def body(k, carry):
        load(k).wait()
        v = jnp.concatenate([local[k * mix + u, t] for u in range(mix) for t in range(tiles)], axis=0) * SCALE
        v = _reorder(v, order)
        for u in range(mix):
            for t in range(tiles):
                at = (u * tiles + t) * TILE
                out[k * mix + u, t] = v[at:at + TILE]
        return carry

    lax.fori_loop(0, steps, body, 0)


def _advance_kernel(info, ends, state, low_in, high_in, drive, kinds, order, out, natural, every, field, low, high,
                    scaled, work, table, sem, *, mix, groups, bands):
    per, tiles = state.shape[0], state.shape[1]
    count = tiles + 2
    rows = tiles * TILE
    width = state.shape[3]
    fetch = pltpu.make_async_copy(ends, table, sem.at[0])
    fetch.start()
    both = [low_in[j] for j in range(per + 1)] + [high_in[j] for j in range(per + 1)] + [drive[t] for t in range(tiles)]
    v = _reorder(jnp.concatenate(both, axis=0) * SCALE, order)
    for j in range(per + 1):
        low[j] = v[j * TILE:(j + 1) * TILE]
        high[j] = v[(per + 1 + j) * TILE:(per + 2 + j) * TILE]
    natural[0] = low[per]
    natural[count - 1] = high[per]
    every[0] = low_in[per + 1, :, :LANES]
    every[count - 1] = high_in[per + 1, :, :LANES]
    for t in range(tiles):
        at = (2 * per + 2 + t) * TILE
        natural[t + 1] = v[at:at + TILE]
        every[t + 1] = kinds[t]
    for t, v in enumerate(_spread(work, 0, [natural[t] for t in range(count)])):
        scaled[t] = v
    mask = _masks(info[1], bands)

    def whole(k, carry):
        masks = _border(count, width, (TILE - 1, mask[0]), (TILE + rows, mask[1]))
        at = [k * mix + u for u in range(mix)]
        cur = [_spread(work, u, [low[j]] + [state[j, t] for t in range(tiles)] + [high[j]]) for u, j in enumerate(at)]
        res = _steps(cur, lambda t: scaled[t], masks)
        keep = range(1, count - 1)
        for u, j in enumerate(at):
            for t, v in zip(keep, _collect(work, u, res[u], keep)):
                field[j, t - 1] = v
        return carry

    lax.fori_loop(0, per // mix, whole, 0)
    fetch.wait()

    def pack(g, carry):
        for q in range(tiles):
            for slot in range(CAP):
                first = table[slot, 2 * q, g * per]
                second = table[slot, 2 * q + 1, g * per]
                out[g, slot, q] = _halves(field[first, q], field[second, q])
        return carry

    lax.fori_loop(0, groups, pack, 0)


def _masks(band, bands):
    one = jnp.float32(1.0)
    zero = jnp.float32(0.0)
    return [jnp.where(band > 0, one, zero), jnp.where(band < bands - 1, one, zero)]


def _choose(slots, incoming, column, q):
    a = incoming[slots[2 * q, column], q]
    b = incoming[slots[2 * q + 1, column], q]
    return _halves(a, b)


def _pick_kernel(slots, incoming, first, final):
    per, tiles = first.shape[0], incoming.shape[1]

    def body(j, carry):
        first[j] = _choose(slots, incoming, j, 0)
        final[j] = _choose(slots, incoming, j, tiles - 1)
        return carry

    lax.fori_loop(0, per, body, 0)


def _spread_kinds(scratch, kinds, taper):
    for t, v in enumerate(_spread(scratch, 0, kinds)):
        for c, part in enumerate(_taper(v)):
            taper[c, t] = part


def _natural(pend, hold, order):
    mix, count = pend.shape[1], pend.shape[2]
    v = jnp.concatenate([pend[hold, u, t] for u in range(mix) for t in range(count)], axis=0)
    v = _reorder(v, order) * (1.0 / SCALE)
    return [[v[(u * count + t) * TILE:(u * count + t + 1) * TILE] for t in range(count)] for u in range(mix)]


def _pipeline(steps, mix, compute, pend, order, done, copy=None):
    def flush(k):
        for u, column in enumerate(_natural(pend, k % 2, order)):
            for t, v in enumerate(column):
                done[k * mix + u, t] = v

    def first(k):
        for u, column in enumerate(compute(k)):
            for t, v in enumerate(column):
                pend[k % 2, u, t] = v

    first(0)

    def body(k, carry):
        flush(k - 1)
        first(k)
        if copy:
            copy(k - 1).start()
        return carry

    lax.fori_loop(1, steps, body, 0)
    flush(steps - 1)
    if copy:
        copy(steps - 1).start()
        for k in range(steps):
            copy(k).wait()


def _final_inner_kernel(slots, incoming, natural, every, order, done, pend, scaled, taper, work, *, half, mix):
    tiles, width = natural.shape[0] - 2, natural.shape[2]
    for t, v in enumerate(_spread(work, 0, [natural[t + 1] for t in range(tiles)])):
        scaled[t] = v
    _spread_kinds(work, [every[t + 1] for t in range(tiles)], taper)

    def weights(t):
        return [_widen(taper[c, t], width) for c in range(3)]

    def compute(k):
        cur = []
        for u in range(mix):
            mine = _spread(work, u, [_choose(slots, incoming, k * mix + u, t) for t in range(tiles)])
            cur.append(_blend(mine, weights, {}))
        res = _steps(cur, lambda t: scaled[t], {})
        return [_collect(work, u, res[u], range(1, tiles - 1)) for u in range(mix)]

    _pipeline(half // mix, mix, compute, pend, order, done)


def _final_rest_kernel(slots, incoming, first, final, below, above, natural, every, order, prior, out,
                       edges, done, pend, scaled, taper, ends, taper3, work, sems, *, per, half, mix, edge_mix, bands):
    count, width = natural.shape[0], natural.shape[2]
    tiles = count - 2
    last = tiles - 1
    rows = tiles * TILE
    for s in range(2):
        for t, v in enumerate(_spread(work, s, [natural[last * s + t] for t in range(3)])):
            ends[s, t] = v
        _spread_kinds(work, [every[last * s + t] for t in range(3)], taper3.at[s])
    for t, v in enumerate(_spread(work, 2, [natural[t] for t in range(count)])):
        scaled[t] = v
    _spread_kinds(work, [every[t] for t in range(count)], taper)
    mask = _masks(slots[slots.shape[0] - 1, 0], bands)
    steps = (per - half) // mix

    def finish(s):
        return pltpu.make_async_copy(edges.at[s], out.at[pl.ds(0, half), last * s], sems.at[steps + s])

    inner_rows = pltpu.make_async_copy(prior, out.at[pl.ds(0, half), pl.ds(1, tiles - 2)], sems.at[steps + 2])
    inner_rows.start()

    def edge(k, carry):
        for s in range(2):
            mask3 = _border(3, width, (TILE - 1, mask[0]) if s == 0 else (2 * TILE, mask[1]))
            cur = []
            for u in range(edge_mix):
                j = k * edge_mix + u
                inner = _choose(slots, incoming, j, 1 if s == 0 else last - 1)
                three = [below[j], first[j], inner] if s == 0 else [inner, final[j], above[j]]
                cur.append(_blend(_spread(work, u, three),
                                  lambda t: [_widen(taper3[s, c, t], width) for c in range(3)], mask3))
            res = _steps(cur, lambda t: ends[s, t], mask3)
            for u in range(edge_mix):
                edges[s, k * edge_mix + u] = _collect(work, u, res[u], [1])[0]
        return carry

    lax.fori_loop(0, half // edge_mix, edge, 0)
    v = jnp.concatenate([edges[s, j] for s in range(2) for j in range(half)], axis=0)
    v = _reorder(v, order) * (1.0 / SCALE)
    for s in range(2):
        for j in range(half):
            at = (s * half + j) * TILE
            edges[s, j] = v[at:at + TILE]
    for s in range(2):
        finish(s).start()

    def copy(k):
        return pltpu.make_async_copy(
            done.at[pl.ds(k * mix, mix)], out.at[pl.ds(half + k * mix, mix)], sems.at[k])

    def compute(k):
        masks = _border(count, width, (TILE - 1, mask[0]), (TILE + rows, mask[1]))
        cur = []
        for u in range(mix):
            j = half + k * mix + u
            mine = [below[j], first[j]]
            mine += [_choose(slots, incoming, j, t) for t in range(1, last)]
            mine += [final[j], above[j]]
            cur.append(_blend(_spread(work, u, mine), lambda t: [_widen(taper[c, t], width) for c in range(3)],
                              masks))
        res = _steps(cur, lambda t: scaled[t], masks)
        return [_collect(work, u, res[u], range(1, count - 1)) for u in range(mix)]

    _pipeline(steps, mix, compute, pend, order, done, copy)
    for s in range(2):
        finish(s).wait()
    inner_rows.wait()


def _pin(x):
    return pltpu.with_memory_space_constraint(x, pltpu.HBM)


def _call(kernel, name, outs, scratch, spaces, out_spaces, alias=None):
    def spec(kind):
        return pl.BlockSpec(memory_space={"v": pltpu.VMEM, "s": pltpu.SMEM, "a": pl.ANY, "h": pltpu.HBM}[kind])

    specs = [spec(k) for k in out_spaces]
    single = len(outs) == 1
    return pl.pallas_call(
        kernel,
        in_specs=[spec(k) for k in spaces],
        out_specs=specs[0] if single else specs,
        out_shape=outs[0] if single else outs,
        scratch_shapes=scratch,
        input_output_aliases=alias or {},
        compiler_params=pltpu.CompilerParams(vmem_limit_bytes=40 * 1024 * 1024),
        name=name,
    )


def on_device(state, forcing, parents, taper_index):
    per, rows, width = state.shape
    tiles = rows // TILE
    groups = lax.axis_size("pgroup")
    bands = lax.axis_size("band")
    f32 = jnp.float32
    forward = [(i, i + 1) for i in range(bands - 1)]
    backward = [(b, a) for a, b in forward]
    info = jnp.stack([lax.axis_index("pgroup"), lax.axis_index("band")]).astype(jnp.int32)
    state4 = state.reshape(per, tiles, TILE, width)
    pinned = _pin(state4)
    drive = forcing.reshape(tiles, TILE, width)
    entries = groups * CAP
    dma = pltpu.SemaphoreType.DMA
    vmem = pltpu.VMEM

    def shape(*dims, dtype=f32):
        return jax.ShapeDtypeStruct(dims, dtype)

    patches, count = parents.shape
    i32 = jnp.int32
    head, tail = _call(
        functools.partial(_prep_kernel, per=per, tiles=tiles), "prepare",
        [shape(per + 2, TILE, width), shape(per + 2, TILE, width)],
        [pltpu.SMEM((rows,), i32), dma((5,))], "hhh", "vv",
    )(_pin(taper_index), pinned, _pin(drive))
    low = lax.ppermute(tail, "band", forward)
    high = lax.ppermute(head, "band", backward)

    half = per // 2

    def work(count, height):
        return vmem((count, width // LANES, height * TILE, LANES), f32)

    extra = [vmem((tiles + 2, TILE, width), f32), vmem((2, 3, TILE, width), f32)]
    square = shape(width, width, dtype=jnp.bfloat16)
    state4, order, back, kinds, ends, own, drive = _call(
        functools.partial(_order_kernel, mix=4), "reorder",
        [shape(per, tiles, TILE, width), square, square, shape(tiles, TILE, LANES),
         shape(CAP, patches, count, dtype=i32), shape(patches + TILE, LANES, dtype=i32),
         shape(tiles, TILE, width)],
        [vmem((per, tiles, TILE, width), f32), dma((per // 4,))], "sshvv", "v" * 7,
    )(info, taper_index, pinned, drive, parents)
    message, natural, every = _call(
        functools.partial(_advance_kernel, mix=2, groups=groups, bands=bands), "advance",
        [shape(groups, CAP, tiles, TILE, width), shape(tiles + 2, TILE, width), shape(tiles + 2, TILE, LANES)],
        [vmem((per, tiles, TILE, width), f32), vmem((per + 1, TILE, width), f32), vmem((per + 1, TILE, width), f32),
         extra[0], work(2, tiles + 2), pltpu.SMEM((CAP, patches, count), i32), dma((1,))], "svvvvvvv", "vvv",
    )(info, ends, state4, low, high, drive, kinds, order)

    incoming = lax.all_to_all(message, "pgroup", split_axis=0, concat_axis=0, tiled=True)
    incoming = incoming.reshape(entries, tiles, TILE, width)

    first, final = _call(
        _pick_kernel, "pick_edge", [shape(per, TILE, width), shape(per, TILE, width)], [], "sv", "vv",
    )(own, incoming)
    below = lax.ppermute(final, "band", forward)
    above = lax.ppermute(first, "band", backward)

    pairs = half // 2
    middle = _call(
        functools.partial(_final_inner_kernel, half=half, mix=2), "final_inner", [shape(half, tiles - 2, TILE, width)],
        [vmem((2, 2, tiles - 2, TILE, width), f32), vmem((tiles, TILE, width), f32),
         vmem((3, tiles, TILE, LANES), f32), work(2, tiles)], "svvvv", "v",
    )(own, incoming, natural, every, back)
    field = _call(
        functools.partial(_final_rest_kernel, per=per, half=half, mix=2, edge_mix=4, bands=bands), "final_rest",
        [shape(per, tiles, TILE, width)],
        [vmem((2, half, TILE, width), f32), vmem((per - half, tiles, TILE, width), f32),
         vmem((2, 2, tiles, TILE, width), f32), extra[0], vmem((3, tiles + 2, TILE, LANES), f32), extra[1],
         vmem((2, 3, 3, TILE, LANES), f32), work(4, tiles + 2), dma((pairs + 3,))],
        "svvvvvvvvv", "a",
    )(own, incoming, first, final, below, above, natural, every, back, middle)
    return field.reshape(per, rows, width)


def solution(mesh):
    return jax.shard_map(
        on_device,
        mesh=mesh,
        in_specs=(P("pgroup", "band", None), P("band", None), P("band", None), P("band")),
        out_specs=P("pgroup", "band", None),
        check_vma=False,
    )
```

```python
import functools

import jax
import jax.numpy as jnp
from jax import lax
from jax.experimental import pallas as pl
from jax.experimental.pallas import tpu as pltpu
from jax.sharding import PartitionSpec as P

PATCH_ROWS = 4
STEPS = 6
CAP = 2
TILE = 8
SCALE = 0.05


def _sub(shape):
    return lax.broadcasted_iota(jnp.int32, shape, 0)


def _north(tiles, i, k):
    count = len(tiles)
    return tiles[i + k] if i + k < count else pltpu.roll(tiles[i + k - count], TILE - 1, 0)


def _south(tiles, i, k):
    return tiles[i - k] if i >= k else pltpu.roll(tiles[i - k + len(tiles)], 1, 0)


def _step(tiles, i, drive):
    m = tiles[i]
    width = m.shape[1]
    e = jnp.concatenate([m[:, LANES:], pltpu.roll(m[:, :LANES], LANES - 1, 1)], axis=1)
    w = jnp.concatenate([pltpu.roll(m[:, width - LANES:], 1, 1), m[:, :width - LANES]], axis=1)
    n = _north(tiles, i, 1)
    s = _south(tiles, i, 1)
    return (m * (0.4 - (e - w)) + 0.15 * (e + w)) + (0.05 * n + 0.25 * s) + drive


def _steps(groups, drive, masks):
    for repeat in range(STEPS):
        fresh = [list(tiles) for tiles in groups]
        for i in range(len(groups[0])):
            source = drive(i)
            for tiles, new in zip(groups, fresh):
                v = _step(tiles, i, source)
                new[i] = v * masks[i] if i in masks else v
        groups = fresh
    return groups


def _blend(tiles, weights, masks):
    fresh = []
    for i in range(len(tiles)):
        w0, w1, w2 = weights(i)
        total = w0 * tiles[i]
        total = total + w1 * (_north(tiles, i, 1) + _south(tiles, i, 1))
        total = total + w2 * (_north(tiles, i, 2) + _south(tiles, i, 2))
        fresh.append(total * masks[i] if i in masks else total)
    return fresh


LANES = 128


def _fill_order(ref, back):
    size = ref.shape[0]
    chunks = size // LANES
    step = 64
    for r in range(0, size, step):
        row = lax.broadcasted_iota(jnp.int32, (step, size), 0) + r
        column = lax.broadcasted_iota(jnp.int32, (step, size), 1)
        natural, mixed = (column, row) if back else (row, column)
        hit = natural == chunks * (mixed % LANES) + mixed // LANES
        ref[r:r + step, :] = jnp.where(hit, 1.0, 0.0).astype(jnp.bfloat16)


def _reorder(v, order):
    rows = v.shape[0]
    high = v.astype(jnp.bfloat16)
    rest = (v - high.astype(jnp.float32)).astype(jnp.bfloat16)
    both = jnp.dot(jnp.concatenate([high, rest], axis=0), order[...], preferred_element_type=jnp.float32)
    return both[:rows] + both[rows:]


def _spread(scratch, u, natural):
    count = len(natural)
    chunks = natural[0].shape[1] // LANES
    for t, v in enumerate(natural):
        for c in range(chunks):
            scratch[u, c, t * TILE:(t + 1) * TILE, :] = v[:, c * LANES:(c + 1) * LANES]
    return [jnp.concatenate([scratch[u, c, pl.ds(i, TILE, count), :] for c in range(chunks)], axis=1)
            for i in range(count)]


def _collect(scratch, u, tiles, keep):
    count = len(tiles)
    chunks = tiles[0].shape[1] // LANES
    for i, v in enumerate(tiles):
        for c in range(chunks):
            scratch[u, c, pl.ds(i, TILE, count), :] = v[:, c * LANES:(c + 1) * LANES]
    return [jnp.concatenate([scratch[u, c, t * TILE:(t + 1) * TILE, :] for c in range(chunks)], axis=1) for t in keep]


def _border(count, width, *rows):
    return {at % count: jnp.where(_sub((TILE, width)) == at // count, factor, jnp.float32(1.0)) for at, factor in rows}


def _taper(kind):
    rate = 0.2 * (kind + 1.0)
    near = jnp.exp(-rate)
    far = jnp.exp(-4.0 * rate)
    inv = 1.0 / (far + near + 1.0 + near + far)
    return inv, near * inv, far * inv


def _halves(a, b):
    return jnp.where(_sub(a.shape) < PATCH_ROWS, a, b)


def _widen(v, width):
    return jnp.concatenate([v] * (width // v.shape[1]), axis=1)


def _prep_kernel(taper_in, state, forcing, head, tail, taper, sems, *, per, tiles):
    last = tiles - 1
    first = pltpu.make_async_copy(taper_in, taper, sems.at[4])
    copies = [
        pltpu.make_async_copy(state.at[:, 0], head.at[pl.ds(0, per)], sems.at[0]),
        pltpu.make_async_copy(state.at[:, last], tail.at[pl.ds(0, per)], sems.at[1]),
        pltpu.make_async_copy(forcing.at[0], head.at[per], sems.at[2]),
        pltpu.make_async_copy(forcing.at[last], tail.at[per], sems.at[3]),
    ]
    for c in [first] + copies:
        c.start()
    first.wait()
    width = head.shape[2]
    for r in range(TILE):
        for out, t in ((head, 0), (tail, last)):
            value = taper[t * TILE + r].astype(jnp.float32)
            out[per + 1, r:r + 1, :] = jnp.full((1, width), value, jnp.float32)
    for c in copies:
        c.wait()


def _order_kernel(info, taper, state, forcing, parents, out, order, back, kinds, ends, own, drive, local, sems, *, mix):
    per, tiles, _, width = out.shape
    steps = per // mix

    def load(k):
        return pltpu.make_async_copy(state.at[pl.ds(k * mix, mix)], local.at[pl.ds(k * mix, mix)], sems.at[k])

    for k in range(steps):
        load(k).start()
    for t in range(tiles):
        for r in range(TILE):
            value = taper[t * TILE + r].astype(jnp.float32)
            kinds[t, r:r + 1, :] = jnp.full((1, kinds.shape[2]), value, jnp.float32)
    p = parents[...]
    count = p.shape[1]
    owner = p // per
    inside = p - owner * per
    mine = owner == info[0]
    lo = jnp.where(mine, inside, per - 1)
    hi = jnp.where(mine, inside, 0)
    shift = 1
    while shift < per:
        lo = jnp.minimum(lo, pltpu.roll(lo, count - shift, 1))
        hi = jnp.maximum(hi, pltpu.roll(hi, count - shift, 1))
        shift *= 2
    patches = p.shape[0]
    for slot, v in enumerate((lo, hi)):
        ends[slot] = v
    lane = lax.broadcasted_iota(jnp.int32, p.shape, 1) % per
    rank = jnp.zeros_like(p)
    for shift in range(1, per):
        other = jnp.where(lane + shift < per, pltpu.roll(p, count - shift, 1), pltpu.roll(p, per - shift, 1))
        rank = jnp.where((other // per == owner) & (other < p), 1, rank)
    turn = (count - info[0] * per) % count
    own[pl.ds(0, patches), :] = pltpu.roll(owner * CAP + rank, turn, 1)[:, :LANES]
    own[pl.ds(patches, TILE), :] = jnp.full((TILE, LANES), info[1], jnp.int32)
    _fill_order(order, False)
    _fill_order(back, True)
    v = _reorder(jnp.concatenate([forcing[t] for t in range(tiles)], axis=0) * SCALE, order)
    for t in range(tiles):
        drive[t] = v[t * TILE:(t + 1) * TILE]

    def body(k, carry):
        load(k).wait()
        v = jnp.concatenate([local[k * mix + u, t] for u in range(mix) for t in range(tiles)], axis=0) * SCALE
        v = _reorder(v, order)
        for u in range(mix):
            for t in range(tiles):
                at = (u * tiles + t) * TILE
                out[k * mix + u, t] = v[at:at + TILE]
        return carry

    lax.fori_loop(0, steps, body, 0)


def _advance_kernel(info, ends, state, low_in, high_in, drive, kinds, order, out, natural, every, field, low, high,
                    scaled, work, table, sem, *, mix, groups, bands):
    per, tiles = state.shape[0], state.shape[1]
    count = tiles + 2
    rows = tiles * TILE
    width = state.shape[3]
    fetch = pltpu.make_async_copy(ends, table, sem.at[0])
    fetch.start()
    v = _reorder(jnp.concatenate([low_in[per], high_in[per]], axis=0) * SCALE, order)
    natural[0] = v[:TILE]
    natural[count - 1] = v[TILE:]
    every[0] = low_in[per + 1, :, :LANES]
    every[count - 1] = high_in[per + 1, :, :LANES]
    for t in range(tiles):
        natural[t + 1] = drive[t]
        every[t + 1] = kinds[t]

    def order_pair(k):
        at = [k * mix + u for u in range(mix)]
        v = _reorder(jnp.concatenate([low_in[j] for j in at] + [high_in[j] for j in at], axis=0) * SCALE, order)
        for u, j in enumerate(at):
            low[j] = v[u * TILE:(u + 1) * TILE]
            high[j] = v[(mix + u) * TILE:(mix + u + 1) * TILE]

    order_pair(0)
    for t, v in enumerate(_spread(work, 0, [natural[t] for t in range(count)])):
        scaled[t] = v
    mask = _masks(info[1], bands)

    def whole(k, carry):
        masks = _border(count, width, (TILE - 1, mask[0]), (TILE + rows, mask[1]))
        at = [k * mix + u for u in range(mix)]
        cur = [_spread(work, u, [low[j]] + [state[j, t] for t in range(tiles)] + [high[j]]) for u, j in enumerate(at)]
        res = _steps(cur, lambda t: scaled[t], masks)
        keep = range(1, count - 1)
        order_pair(jnp.minimum(k + 1, per // mix - 1))
        for u, j in enumerate(at):
            for t, v in zip(keep, _collect(work, u, res[u], keep)):
                field[j, t - 1] = v
        return carry

    lax.fori_loop(0, per // mix, whole, 0)
    fetch.wait()

    def pack(g, carry):
        for q in range(tiles):
            for slot in range(CAP):
                first = table[slot, 2 * q, g * per]
                second = table[slot, 2 * q + 1, g * per]
                out[g, slot, q] = _halves(field[first, q], field[second, q])
        return carry

    lax.fori_loop(0, groups, pack, 0)


def _masks(band, bands):
    one = jnp.float32(1.0)
    zero = jnp.float32(0.0)
    return [jnp.where(band > 0, one, zero), jnp.where(band < bands - 1, one, zero)]


def _choose(slots, incoming, column, q):
    a = incoming[slots[2 * q, column], q]
    b = incoming[slots[2 * q + 1, column], q]
    return _halves(a, b)


def _pick_kernel(slots, incoming, first, final):
    per, tiles = first.shape[0], incoming.shape[1]

    def body(j, carry):
        first[j] = _choose(slots, incoming, j, 0)
        final[j] = _choose(slots, incoming, j, tiles - 1)
        return carry

    lax.fori_loop(0, per, body, 0)


def _spread_kinds(scratch, kinds, taper):
    for t, v in enumerate(_spread(scratch, 0, kinds)):
        for c, part in enumerate(_taper(v)):
            taper[c, t] = part


def _natural(pend, hold, order):
    mix, count = pend.shape[1], pend.shape[2]
    v = jnp.concatenate([pend[hold, u, t] for u in range(mix) for t in range(count)], axis=0)
    v = _reorder(v, order) * (1.0 / SCALE)
    return [[v[(u * count + t) * TILE:(u * count + t + 1) * TILE] for t in range(count)] for u in range(mix)]


def _pipeline(steps, mix, compute, pend, order, done, copy=None, beside=None):
    def flush(k):
        for u, column in enumerate(_natural(pend, k % 2, order)):
            for t, v in enumerate(column):
                done[k * mix + u, t] = v

    def first(k):
        for u, column in enumerate(compute(k)):
            for t, v in enumerate(column):
                pend[k % 2, u, t] = v

    first(0)
    if beside:
        beside()

    def body(k, carry):
        flush(k - 1)
        first(k)
        if copy:
            copy(k - 1).start()
        return carry

    lax.fori_loop(1, steps, body, 0)
    flush(steps - 1)
    if copy:
        copy(steps - 1).start()
        for k in range(steps):
            copy(k).wait()


def _final_inner_kernel(slots, incoming, natural, every, order, done, pend, scaled, taper, work, *, half, mix):
    tiles, width = natural.shape[0] - 2, natural.shape[2]
    for t, v in enumerate(_spread(work, 0, [natural[t + 1] for t in range(tiles)])):
        scaled[t] = v
    _spread_kinds(work, [every[t + 1] for t in range(tiles)], taper)

    def weights(t):
        return [_widen(taper[c, t], width) for c in range(3)]

    def compute(k):
        cur = []
        for u in range(mix):
            mine = _spread(work, u, [_choose(slots, incoming, k * mix + u, t) for t in range(tiles)])
            cur.append(_blend(mine, weights, {}))
        res = _steps(cur, lambda t: scaled[t], {})
        return [_collect(work, u, res[u], range(1, tiles - 1)) for u in range(mix)]

    _pipeline(half // mix, mix, compute, pend, order, done)


def _final_rest_kernel(slots, incoming, first, final, below, above, natural, every, order, prior, out,
                       edges, done, pend, scaled, taper, ends, taper3, work, sems, *, per, half, mix, edge_mix, bands):
    count, width = natural.shape[0], natural.shape[2]
    tiles = count - 2
    last = tiles - 1
    rows = tiles * TILE
    for s in range(2):
        for t, v in enumerate(_spread(work, s, [natural[last * s + t] for t in range(3)])):
            ends[s, t] = v
        _spread_kinds(work, [every[last * s + t] for t in range(3)], taper3.at[s])
    for t, v in enumerate(_spread(work, 2, [natural[t] for t in range(count)])):
        scaled[t] = v
    _spread_kinds(work, [every[t] for t in range(count)], taper)
    mask = _masks(slots[slots.shape[0] - 1, 0], bands)
    steps = (per - half) // mix

    def finish(s):
        return pltpu.make_async_copy(edges.at[s], out.at[pl.ds(0, half), last * s], sems.at[steps + s])

    inner_rows = pltpu.make_async_copy(prior, out.at[pl.ds(0, half), pl.ds(1, tiles - 2)], sems.at[steps + 2])
    inner_rows.start()

    def edge(k, carry):
        for s in range(2):
            mask3 = _border(3, width, (TILE - 1, mask[0]) if s == 0 else (2 * TILE, mask[1]))
            cur = []
            for u in range(edge_mix):
                j = k * edge_mix + u
                inner = _choose(slots, incoming, j, 1 if s == 0 else last - 1)
                three = [below[j], first[j], inner] if s == 0 else [inner, final[j], above[j]]
                cur.append(_blend(_spread(work, u, three),
                                  lambda t: [_widen(taper3[s, c, t], width) for c in range(3)], mask3))
            res = _steps(cur, lambda t: ends[s, t], mask3)
            for u in range(edge_mix):
                edges[s, k * edge_mix + u] = _collect(work, u, res[u], [1])[0]
        return carry

    lax.fori_loop(0, half // edge_mix, edge, 0)

    def edge_rows():
        v = jnp.concatenate([edges[s, j] for s in range(2) for j in range(half)], axis=0)
        v = _reorder(v, order) * (1.0 / SCALE)
        for s in range(2):
            for j in range(half):
                at = (s * half + j) * TILE
                edges[s, j] = v[at:at + TILE]
        for s in range(2):
            finish(s).start()

    def copy(k):
        return pltpu.make_async_copy(
            done.at[pl.ds(k * mix, mix)], out.at[pl.ds(half + k * mix, mix)], sems.at[k])

    def compute(k):
        masks = _border(count, width, (TILE - 1, mask[0]), (TILE + rows, mask[1]))
        cur = []
        for u in range(mix):
            j = half + k * mix + u
            mine = [below[j], first[j]]
            mine += [_choose(slots, incoming, j, t) for t in range(1, last)]
            mine += [final[j], above[j]]
            cur.append(_blend(_spread(work, u, mine), lambda t: [_widen(taper[c, t], width) for c in range(3)],
                              masks))
        res = _steps(cur, lambda t: scaled[t], masks)
        return [_collect(work, u, res[u], range(1, count - 1)) for u in range(mix)]

    _pipeline(steps, mix, compute, pend, order, done, copy, edge_rows)
    for s in range(2):
        finish(s).wait()
    inner_rows.wait()


def _pin(x):
    return pltpu.with_memory_space_constraint(x, pltpu.HBM)


def _call(kernel, name, outs, scratch, spaces, out_spaces, alias=None):
    def spec(kind):
        return pl.BlockSpec(memory_space={"v": pltpu.VMEM, "s": pltpu.SMEM, "a": pl.ANY, "h": pltpu.HBM}[kind])

    specs = [spec(k) for k in out_spaces]
    single = len(outs) == 1
    return pl.pallas_call(
        kernel,
        in_specs=[spec(k) for k in spaces],
        out_specs=specs[0] if single else specs,
        out_shape=outs[0] if single else outs,
        scratch_shapes=scratch,
        input_output_aliases=alias or {},
        compiler_params=pltpu.CompilerParams(vmem_limit_bytes=40 * 1024 * 1024),
        name=name,
    )


def on_device(state, forcing, parents, taper_index):
    per, rows, width = state.shape
    tiles = rows // TILE
    groups = lax.axis_size("pgroup")
    bands = lax.axis_size("band")
    f32 = jnp.float32
    forward = [(i, i + 1) for i in range(bands - 1)]
    backward = [(b, a) for a, b in forward]
    info = jnp.stack([lax.axis_index("pgroup"), lax.axis_index("band")]).astype(jnp.int32)
    state4 = state.reshape(per, tiles, TILE, width)
    pinned = _pin(state4)
    drive = forcing.reshape(tiles, TILE, width)
    entries = groups * CAP
    dma = pltpu.SemaphoreType.DMA
    vmem = pltpu.VMEM

    def shape(*dims, dtype=f32):
        return jax.ShapeDtypeStruct(dims, dtype)

    patches, count = parents.shape
    i32 = jnp.int32
    head, tail = _call(
        functools.partial(_prep_kernel, per=per, tiles=tiles), "prepare",
        [shape(per + 2, TILE, width), shape(per + 2, TILE, width)],
        [pltpu.SMEM((rows,), i32), dma((5,))], "hhh", "vv",
    )(_pin(taper_index), pinned, _pin(drive))
    low = lax.ppermute(tail, "band", forward)
    high = lax.ppermute(head, "band", backward)

    half = per // 2

    def work(count, height):
        return vmem((count, width // LANES, height * TILE, LANES), f32)

    extra = [vmem((tiles + 2, TILE, width), f32), vmem((2, 3, TILE, width), f32)]
    square = shape(width, width, dtype=jnp.bfloat16)
    state4, order, back, kinds, ends, own, drive = _call(
        functools.partial(_order_kernel, mix=4), "reorder",
        [shape(per, tiles, TILE, width), square, square, shape(tiles, TILE, LANES),
         shape(CAP, patches, count, dtype=i32), shape(patches + TILE, LANES, dtype=i32),
         shape(tiles, TILE, width)],
        [vmem((per, tiles, TILE, width), f32), dma((per // 4,))], "sshvv", "v" * 7,
    )(info, taper_index, pinned, drive, parents)
    message, natural, every = _call(
        functools.partial(_advance_kernel, mix=2, groups=groups, bands=bands), "advance",
        [shape(groups, CAP, tiles, TILE, width), shape(tiles + 2, TILE, width), shape(tiles + 2, TILE, LANES)],
        [vmem((per, tiles, TILE, width), f32), vmem((per + 1, TILE, width), f32), vmem((per + 1, TILE, width), f32),
         extra[0], work(2, tiles + 2), pltpu.SMEM((CAP, patches, count), i32), dma((1,))], "svvvvvvv", "vvv",
    )(info, ends, state4, low, high, drive, kinds, order)

    incoming = lax.all_to_all(message, "pgroup", split_axis=0, concat_axis=0, tiled=True)
    incoming = incoming.reshape(entries, tiles, TILE, width)

    first, final = _call(
        _pick_kernel, "pick_edge", [shape(per, TILE, width), shape(per, TILE, width)], [], "sv", "vv",
    )(own, incoming)
    below = lax.ppermute(final, "band", forward)
    above = lax.ppermute(first, "band", backward)

    pairs = half // 2
    middle = _call(
        functools.partial(_final_inner_kernel, half=half, mix=2), "final_inner", [shape(half, tiles - 2, TILE, width)],
        [vmem((2, 2, tiles - 2, TILE, width), f32), vmem((tiles, TILE, width), f32),
         vmem((3, tiles, TILE, LANES), f32), work(2, tiles)], "svvvv", "v",
    )(own, incoming, natural, every, back)
    field = _call(
        functools.partial(_final_rest_kernel, per=per, half=half, mix=2, edge_mix=4, bands=bands), "final_rest",
        [shape(per, tiles, TILE, width)],
        [vmem((2, half, TILE, width), f32), vmem((per - half, tiles, TILE, width), f32),
         vmem((2, 2, tiles, TILE, width), f32), extra[0], vmem((3, tiles + 2, TILE, LANES), f32), extra[1],
         vmem((2, 3, 3, TILE, LANES), f32), work(4, tiles + 2), dma((pairs + 3,))],
        "svvvvvvvvv", "a",
    )(own, incoming, first, final, below, above, natural, every, back, middle)
    return field.reshape(per, rows, width)


def solution(mesh):
    return jax.shard_map(
        on_device,
        mesh=mesh,
        in_specs=(P("pgroup", "band", None), P("band", None), P("band", None), P("band")),
        out_specs=P("pgroup", "band", None),
        check_vma=False,
    )
```

```python
import functools

import jax
import jax.numpy as jnp
from jax import lax
from jax.experimental import pallas as pl
from jax.experimental.pallas import tpu as pltpu
from jax.sharding import PartitionSpec as P

PATCH_ROWS = 4
STEPS = 6
CAP = 2
TILE = 8
SCALE = 0.05


def _sub(shape):
    return lax.broadcasted_iota(jnp.int32, shape, 0)


def _north(tiles, i, k):
    count = len(tiles)
    return tiles[i + k] if i + k < count else pltpu.roll(tiles[i + k - count], TILE - 1, 0)


def _south(tiles, i, k):
    return tiles[i - k] if i >= k else pltpu.roll(tiles[i - k + len(tiles)], 1, 0)


def _step(tiles, i, drive):
    m = tiles[i]
    width = m.shape[1]
    e = jnp.concatenate([m[:, LANES:], pltpu.roll(m[:, :LANES], LANES - 1, 1)], axis=1)
    w = jnp.concatenate([pltpu.roll(m[:, width - LANES:], 1, 1), m[:, :width - LANES]], axis=1)
    n = _north(tiles, i, 1)
    s = _south(tiles, i, 1)
    return (m * (0.4 - (e - w)) + 0.15 * (e + w)) + (0.05 * n + 0.25 * s) + drive


def _steps(groups, drive, masks):
    for repeat in range(STEPS):
        fresh = [list(tiles) for tiles in groups]
        for i in range(len(groups[0])):
            source = drive(i)
            for tiles, new in zip(groups, fresh):
                v = _step(tiles, i, source)
                new[i] = v * masks[i] if i in masks else v
        groups = fresh
    return groups


def _blend(tiles, weights, masks):
    fresh = []
    for i in range(len(tiles)):
        w0, w1, w2 = weights(i)
        total = w0 * tiles[i]
        total = total + w1 * (_north(tiles, i, 1) + _south(tiles, i, 1))
        total = total + w2 * (_north(tiles, i, 2) + _south(tiles, i, 2))
        fresh.append(total * masks[i] if i in masks else total)
    return fresh


LANES = 128


def _fill_order(ref, back):
    size = ref.shape[0]
    chunks = size // LANES
    step = 64
    for r in range(0, size, step):
        row = lax.broadcasted_iota(jnp.int32, (step, size), 0) + r
        column = lax.broadcasted_iota(jnp.int32, (step, size), 1)
        natural, mixed = (column, row) if back else (row, column)
        hit = natural == chunks * (mixed % LANES) + mixed // LANES
        ref[r:r + step, :] = jnp.where(hit, 1.0 / SCALE if back else 1.0, 0.0).astype(jnp.bfloat16)


def _reorder(v, order):
    rows = v.shape[0]
    high = v.astype(jnp.bfloat16)
    rest = (v - high.astype(jnp.float32)).astype(jnp.bfloat16)
    both = jnp.dot(jnp.concatenate([high, rest], axis=0), order[...], preferred_element_type=jnp.float32)
    return both[:rows] + both[rows:]


def _spread(scratch, u, natural):
    count = len(natural)
    chunks = natural[0].shape[1] // LANES
    for t, v in enumerate(natural):
        for c in range(chunks):
            scratch[u, c, t * TILE:(t + 1) * TILE, :] = v[:, c * LANES:(c + 1) * LANES]
    return [jnp.concatenate([scratch[u, c, pl.ds(i, TILE, count), :] for c in range(chunks)], axis=1)
            for i in range(count)]


def _collect(scratch, u, tiles, keep):
    count = len(tiles)
    chunks = tiles[0].shape[1] // LANES
    for i, v in enumerate(tiles):
        for c in range(chunks):
            scratch[u, c, pl.ds(i, TILE, count), :] = v[:, c * LANES:(c + 1) * LANES]
    return [jnp.concatenate([scratch[u, c, t * TILE:(t + 1) * TILE, :] for c in range(chunks)], axis=1) for t in keep]


def _border(count, width, *rows):
    return {at % count: jnp.where(_sub((TILE, width)) == at // count, factor, jnp.float32(1.0)) for at, factor in rows}


def _taper(kind):
    rate = 0.2 * (kind + 1.0)
    near = jnp.exp(-rate)
    far = jnp.exp(-4.0 * rate)
    inv = 1.0 / (far + near + 1.0 + near + far)
    return inv, near * inv, far * inv


def _halves(a, b):
    return jnp.where(_sub(a.shape) < PATCH_ROWS, a, b)


def _widen(v, width):
    return jnp.concatenate([v] * (width // v.shape[1]), axis=1)


def _prep_kernel(taper_in, state, forcing, head, tail, taper, sems, *, per, tiles):
    last = tiles - 1
    first = pltpu.make_async_copy(taper_in, taper, sems.at[4])
    copies = [
        pltpu.make_async_copy(state.at[:, 0], head.at[pl.ds(0, per)], sems.at[0]),
        pltpu.make_async_copy(state.at[:, last], tail.at[pl.ds(0, per)], sems.at[1]),
        pltpu.make_async_copy(forcing.at[0], head.at[per], sems.at[2]),
        pltpu.make_async_copy(forcing.at[last], tail.at[per], sems.at[3]),
    ]
    for c in [first] + copies:
        c.start()
    first.wait()
    width = head.shape[2]
    for r in range(TILE):
        for out, t in ((head, 0), (tail, last)):
            value = taper[t * TILE + r].astype(jnp.float32)
            out[per + 1, r:r + 1, :] = jnp.full((1, width), value, jnp.float32)
    for c in copies:
        c.wait()


def _order_kernel(info, taper, state, forcing, parents, out, order, back, kinds, ends, own, drive, local, sems, *, mix):
    per, tiles, _, width = out.shape
    steps = per // mix

    def load(k):
        return pltpu.make_async_copy(state.at[pl.ds(k * mix, mix)], local.at[pl.ds(k * mix, mix)], sems.at[k])

    for k in range(steps):
        load(k).start()
    for t in range(tiles):
        for r in range(TILE):
            value = taper[t * TILE + r].astype(jnp.float32)
            kinds[t, r:r + 1, :] = jnp.full((1, kinds.shape[2]), value, jnp.float32)
    p = parents[...]
    count = p.shape[1]
    owner = p // per
    inside = p - owner * per
    mine = owner == info[0]
    lo = jnp.where(mine, inside, per - 1)
    hi = jnp.where(mine, inside, 0)
    shift = 1
    while shift < per:
        lo = jnp.minimum(lo, pltpu.roll(lo, count - shift, 1))
        hi = jnp.maximum(hi, pltpu.roll(hi, count - shift, 1))
        shift *= 2
    patches = p.shape[0]
    for slot, v in enumerate((lo, hi)):
        ends[slot] = v
    lane = lax.broadcasted_iota(jnp.int32, p.shape, 1) % per
    rank = jnp.zeros_like(p)
    for shift in range(1, per):
        other = jnp.where(lane + shift < per, pltpu.roll(p, count - shift, 1), pltpu.roll(p, per - shift, 1))
        rank = jnp.where((other // per == owner) & (other < p), 1, rank)
    turn = (count - info[0] * per) % count
    own[pl.ds(0, patches), :] = pltpu.roll(owner * CAP + rank, turn, 1)[:, :LANES]
    own[pl.ds(patches, TILE), :] = jnp.full((TILE, LANES), info[1], jnp.int32)
    _fill_order(order, False)
    _fill_order(back, True)
    v = _reorder(jnp.concatenate([forcing[t] for t in range(tiles)], axis=0) * SCALE, order)
    for t in range(tiles):
        drive[t] = v[t * TILE:(t + 1) * TILE]

    def body(k, carry):
        load(k).wait()
        v = jnp.concatenate([local[k * mix + u, t] for u in range(mix) for t in range(tiles)], axis=0) * SCALE
        v = _reorder(v, order)
        for u in range(mix):
            for t in range(tiles):
                at = (u * tiles + t) * TILE
                out[k * mix + u, t] = v[at:at + TILE]
        return carry

    lax.fori_loop(0, steps, body, 0)


def _advance_kernel(info, ends, state, low_in, high_in, drive, kinds, order, out, natural, every, field, low, high,
                    scaled, work, table, sem, *, mix, groups, bands):
    per, tiles = state.shape[0], state.shape[1]
    count = tiles + 2
    rows = tiles * TILE
    width = state.shape[3]
    fetch = pltpu.make_async_copy(ends, table, sem.at[0])
    fetch.start()
    v = _reorder(jnp.concatenate([low_in[per], high_in[per]], axis=0) * SCALE, order)
    natural[0] = v[:TILE]
    natural[count - 1] = v[TILE:]
    every[0] = low_in[per + 1, :, :LANES]
    every[count - 1] = high_in[per + 1, :, :LANES]
    for t in range(tiles):
        natural[t + 1] = drive[t]
        every[t + 1] = kinds[t]

    def order_pair(k):
        at = [k * mix + u for u in range(mix)]
        v = _reorder(jnp.concatenate([low_in[j] for j in at] + [high_in[j] for j in at], axis=0) * SCALE, order)
        for u, j in enumerate(at):
            low[j] = v[u * TILE:(u + 1) * TILE]
            high[j] = v[(mix + u) * TILE:(mix + u + 1) * TILE]

    order_pair(0)
    for t, v in enumerate(_spread(work, 0, [natural[t] for t in range(count)])):
        scaled[t] = v
    mask = _masks(info[1], bands)

    def whole(k, carry):
        masks = _border(count, width, (TILE - 1, mask[0]), (TILE + rows, mask[1]))
        at = [k * mix + u for u in range(mix)]
        cur = [_spread(work, u, [low[j]] + [state[j, t] for t in range(tiles)] + [high[j]]) for u, j in enumerate(at)]
        res = _steps(cur, lambda t: scaled[t], masks)
        keep = range(1, count - 1)
        order_pair(jnp.minimum(k + 1, per // mix - 1))
        for u, j in enumerate(at):
            for t, v in zip(keep, _collect(work, u, res[u], keep)):
                field[j, t - 1] = v
        return carry

    lax.fori_loop(0, per // mix, whole, 0)
    fetch.wait()

    def pack(g, carry):
        for q in range(tiles):
            for slot in range(CAP):
                first = table[slot, 2 * q, g * per]
                second = table[slot, 2 * q + 1, g * per]
                out[g, slot, q] = _halves(field[first, q], field[second, q])
        return carry

    lax.fori_loop(0, groups, pack, 0, unroll=2)


def _masks(band, bands):
    one = jnp.float32(1.0)
    zero = jnp.float32(0.0)
    return [jnp.where(band > 0, one, zero), jnp.where(band < bands - 1, one, zero)]


def _choose(slots, incoming, column, q):
    a = incoming[slots[2 * q, column], q]
    b = incoming[slots[2 * q + 1, column], q]
    return _halves(a, b)


def _pick_kernel(slots, incoming, first, final):
    per, tiles = first.shape[0], incoming.shape[1]

    def body(j, carry):
        first[j] = _choose(slots, incoming, j, 0)
        final[j] = _choose(slots, incoming, j, tiles - 1)
        return carry

    lax.fori_loop(0, per, body, 0, unroll=4)


def _spread_kinds(scratch, kinds, taper):
    for t, v in enumerate(_spread(scratch, 0, kinds)):
        for c, part in enumerate(_taper(v)):
            taper[c, t] = part


def _natural(pend, hold, order):
    mix, count = pend.shape[1], pend.shape[2]
    v = jnp.concatenate([pend[hold, u, t] for u in range(mix) for t in range(count)], axis=0)
    v = _reorder(v, order)
    return [[v[(u * count + t) * TILE:(u * count + t + 1) * TILE] for t in range(count)] for u in range(mix)]


def _pipeline(steps, mix, compute, pend, order, done, copy=None, beside=None):
    def flush(k):
        for u, column in enumerate(_natural(pend, k % 2, order)):
            for t, v in enumerate(column):
                done[k * mix + u, t] = v

    def first(k):
        for u, column in enumerate(compute(k)):
            for t, v in enumerate(column):
                pend[k % 2, u, t] = v

    first(0)
    if beside:
        beside()

    def body(k, carry):
        flush(k - 1)
        first(k)
        if copy:
            copy(k - 1).start()
        return carry

    lax.fori_loop(1, steps, body, 0)
    flush(steps - 1)
    if copy:
        copy(steps - 1).start()
        for k in range(steps):
            copy(k).wait()


def _final_inner_kernel(slots, incoming, natural, every, order, done, pend, scaled, taper, work, *, half, mix):
    tiles, width = natural.shape[0] - 2, natural.shape[2]
    for t, v in enumerate(_spread(work, 0, [natural[t + 1] for t in range(tiles)])):
        scaled[t] = v
    _spread_kinds(work, [every[t + 1] for t in range(tiles)], taper)

    def weights(t):
        return [_widen(taper[c, t], width) for c in range(3)]

    def compute(k):
        cur = []
        for u in range(mix):
            mine = _spread(work, u, [_choose(slots, incoming, k * mix + u, t) for t in range(tiles)])
            cur.append(_blend(mine, weights, {}))
        res = _steps(cur, lambda t: scaled[t], {})
        return [_collect(work, u, res[u], range(1, tiles - 1)) for u in range(mix)]

    _pipeline(half // mix, mix, compute, pend, order, done)


def _final_rest_kernel(slots, incoming, first, final, below, above, natural, every, order, prior, out,
                       edges, done, pend, scaled, taper, ends, taper3, work, sems, *, per, half, mix, edge_mix, bands):
    count, width = natural.shape[0], natural.shape[2]
    tiles = count - 2
    last = tiles - 1
    rows = tiles * TILE
    for s in range(2):
        for t, v in enumerate(_spread(work, s, [natural[last * s + t] for t in range(3)])):
            ends[s, t] = v
        _spread_kinds(work, [every[last * s + t] for t in range(3)], taper3.at[s])
    for t, v in enumerate(_spread(work, 2, [natural[t] for t in range(count)])):
        scaled[t] = v
    _spread_kinds(work, [every[t] for t in range(count)], taper)
    mask = _masks(slots[slots.shape[0] - 1, 0], bands)
    steps = (per - half) // mix

    def finish(s):
        return pltpu.make_async_copy(edges.at[s], out.at[pl.ds(0, half), last * s], sems.at[steps + s])

    inner_rows = pltpu.make_async_copy(prior, out.at[pl.ds(0, half), pl.ds(1, tiles - 2)], sems.at[steps + 2])
    inner_rows.start()

    def edge(k, carry):
        for s in range(2):
            mask3 = _border(3, width, (TILE - 1, mask[0]) if s == 0 else (2 * TILE, mask[1]))
            cur = []
            for u in range(edge_mix):
                j = k * edge_mix + u
                inner = _choose(slots, incoming, j, 1 if s == 0 else last - 1)
                three = [below[j], first[j], inner] if s == 0 else [inner, final[j], above[j]]
                cur.append(_blend(_spread(work, u, three),
                                  lambda t: [_widen(taper3[s, c, t], width) for c in range(3)], mask3))
            res = _steps(cur, lambda t: ends[s, t], mask3)
            for u in range(edge_mix):
                edges[s, k * edge_mix + u] = _collect(work, u, res[u], [1])[0]
        return carry

    lax.fori_loop(0, half // edge_mix, edge, 0)

    def edge_rows():
        v = jnp.concatenate([edges[s, j] for s in range(2) for j in range(half)], axis=0)
        v = _reorder(v, order)
        for s in range(2):
            for j in range(half):
                at = (s * half + j) * TILE
                edges[s, j] = v[at:at + TILE]
        for s in range(2):
            finish(s).start()

    def copy(k):
        return pltpu.make_async_copy(
            done.at[pl.ds(k * mix, mix)], out.at[pl.ds(half + k * mix, mix)], sems.at[k])

    def compute(k):
        masks = _border(count, width, (TILE - 1, mask[0]), (TILE + rows, mask[1]))
        cur = []
        for u in range(mix):
            j = half + k * mix + u
            mine = [below[j], first[j]]
            mine += [_choose(slots, incoming, j, t) for t in range(1, last)]
            mine += [final[j], above[j]]
            cur.append(_blend(_spread(work, u, mine), lambda t: [_widen(taper[c, t], width) for c in range(3)],
                              masks))
        res = _steps(cur, lambda t: scaled[t], masks)
        return [_collect(work, u, res[u], range(1, count - 1)) for u in range(mix)]

    _pipeline(steps, mix, compute, pend, order, done, copy, edge_rows)
    for s in range(2):
        finish(s).wait()
    inner_rows.wait()


def _pin(x):
    return pltpu.with_memory_space_constraint(x, pltpu.HBM)


def _call(kernel, name, outs, scratch, spaces, out_spaces, alias=None):
    def spec(kind):
        return pl.BlockSpec(memory_space={"v": pltpu.VMEM, "s": pltpu.SMEM, "a": pl.ANY, "h": pltpu.HBM}[kind])

    specs = [spec(k) for k in out_spaces]
    single = len(outs) == 1
    return pl.pallas_call(
        kernel,
        in_specs=[spec(k) for k in spaces],
        out_specs=specs[0] if single else specs,
        out_shape=outs[0] if single else outs,
        scratch_shapes=scratch,
        input_output_aliases=alias or {},
        compiler_params=pltpu.CompilerParams(vmem_limit_bytes=40 * 1024 * 1024),
        name=name,
    )


def on_device(state, forcing, parents, taper_index):
    per, rows, width = state.shape
    tiles = rows // TILE
    groups = lax.axis_size("pgroup")
    bands = lax.axis_size("band")
    f32 = jnp.float32
    forward = [(i, i + 1) for i in range(bands - 1)]
    backward = [(b, a) for a, b in forward]
    info = jnp.stack([lax.axis_index("pgroup"), lax.axis_index("band")]).astype(jnp.int32)
    state4 = state.reshape(per, tiles, TILE, width)
    pinned = _pin(state4)
    drive = forcing.reshape(tiles, TILE, width)
    entries = groups * CAP
    dma = pltpu.SemaphoreType.DMA
    vmem = pltpu.VMEM

    def shape(*dims, dtype=f32):
        return jax.ShapeDtypeStruct(dims, dtype)

    patches, count = parents.shape
    i32 = jnp.int32
    head, tail = _call(
        functools.partial(_prep_kernel, per=per, tiles=tiles), "prepare",
        [shape(per + 2, TILE, width), shape(per + 2, TILE, width)],
        [pltpu.SMEM((rows,), i32), dma((5,))], "hhh", "vv",
    )(_pin(taper_index), pinned, _pin(drive))
    low = lax.ppermute(tail, "band", forward)
    high = lax.ppermute(head, "band", backward)

    half = per // 2

    def work(count, height):
        return vmem((count, width // LANES, height * TILE, LANES), f32)

    extra = [vmem((tiles + 2, TILE, width), f32), vmem((2, 3, TILE, width), f32)]
    square = shape(width, width, dtype=jnp.bfloat16)
    state4, order, back, kinds, ends, own, drive = _call(
        functools.partial(_order_kernel, mix=4), "reorder",
        [shape(per, tiles, TILE, width), square, square, shape(tiles, TILE, LANES),
         shape(CAP, patches, count, dtype=i32), shape(patches + TILE, LANES, dtype=i32),
         shape(tiles, TILE, width)],
        [vmem((per, tiles, TILE, width), f32), dma((per // 4,))], "sshvv", "v" * 7,
    )(info, taper_index, pinned, drive, parents)
    message, natural, every = _call(
        functools.partial(_advance_kernel, mix=2, groups=groups, bands=bands), "advance",
        [shape(groups, CAP, tiles, TILE, width), shape(tiles + 2, TILE, width), shape(tiles + 2, TILE, LANES)],
        [vmem((per, tiles, TILE, width), f32), vmem((per + 1, TILE, width), f32), vmem((per + 1, TILE, width), f32),
         extra[0], work(2, tiles + 2), pltpu.SMEM((CAP, patches, count), i32), dma((1,))], "svvvvvvv", "vvv",
    )(info, ends, state4, low, high, drive, kinds, order)

    incoming = lax.all_to_all(message, "pgroup", split_axis=0, concat_axis=0, tiled=True)
    incoming = incoming.reshape(entries, tiles, TILE, width)

    first, final = _call(
        _pick_kernel, "pick_edge", [shape(per, TILE, width), shape(per, TILE, width)], [], "sv", "vv",
    )(own, incoming)
    below = lax.ppermute(final, "band", forward)
    above = lax.ppermute(first, "band", backward)

    pairs = half // 2
    middle = _call(
        functools.partial(_final_inner_kernel, half=half, mix=2), "final_inner", [shape(half, tiles - 2, TILE, width)],
        [vmem((2, 2, tiles - 2, TILE, width), f32), vmem((tiles, TILE, width), f32),
         vmem((3, tiles, TILE, LANES), f32), work(2, tiles)], "svvvv", "v",
    )(own, incoming, natural, every, back)
    field = _call(
        functools.partial(_final_rest_kernel, per=per, half=half, mix=2, edge_mix=4, bands=bands), "final_rest",
        [shape(per, tiles, TILE, width)],
        [vmem((2, half, TILE, width), f32), vmem((per - half, tiles, TILE, width), f32),
         vmem((2, 2, tiles, TILE, width), f32), extra[0], vmem((3, tiles + 2, TILE, LANES), f32), extra[1],
         vmem((2, 3, 3, TILE, LANES), f32), work(4, tiles + 2), dma((pairs + 3,))],
        "svvvvvvvvv", "a",
    )(own, incoming, first, final, below, above, natural, every, back, middle)
    return field.reshape(per, rows, width)


def solution(mesh):
    return jax.shard_map(
        on_device,
        mesh=mesh,
        in_specs=(P("pgroup", "band", None), P("band", None), P("band", None), P("band")),
        out_specs=P("pgroup", "band", None),
        check_vma=False,
    )
```

```python
import functools

import jax
import jax.numpy as jnp
from jax import lax
from jax.experimental import pallas as pl
from jax.experimental.pallas import tpu as pltpu
from jax.sharding import PartitionSpec as P

PATCH_ROWS = 4
STEPS = 6
CAP = 2
TILE = 8
SCALE = 0.05


def _sub(shape):
    return lax.broadcasted_iota(jnp.int32, shape, 0)


def _north(tiles, i, k):
    count = len(tiles)
    return tiles[i + k] if i + k < count else pltpu.roll(tiles[i + k - count], TILE - 1, 0)


def _south(tiles, i, k):
    return tiles[i - k] if i >= k else pltpu.roll(tiles[i - k + len(tiles)], 1, 0)


def _step(tiles, i, drive):
    m = tiles[i]
    width = m.shape[1]
    e = jnp.concatenate([m[:, LANES:], pltpu.roll(m[:, :LANES], LANES - 1, 1)], axis=1)
    w = jnp.concatenate([pltpu.roll(m[:, width - LANES:], 1, 1), m[:, :width - LANES]], axis=1)
    n = _north(tiles, i, 1)
    s = _south(tiles, i, 1)
    return (m * (0.4 - (e - w)) + 0.15 * (e + w)) + (0.05 * n + 0.25 * s) + drive


def _steps(groups, drive, masks):
    for repeat in range(STEPS):
        fresh = [list(tiles) for tiles in groups]
        for i in range(len(groups[0])):
            source = drive(i)
            for tiles, new in zip(groups, fresh):
                v = _step(tiles, i, source)
                new[i] = v * masks[i] if i in masks else v
        groups = fresh
    return groups


def _blend(tiles, weights, masks):
    fresh = []
    for i in range(len(tiles)):
        w0, w1, w2 = weights(i)
        total = w0 * tiles[i]
        total = total + w1 * (_north(tiles, i, 1) + _south(tiles, i, 1))
        total = total + w2 * (_north(tiles, i, 2) + _south(tiles, i, 2))
        fresh.append(total * masks[i] if i in masks else total)
    return fresh


LANES = 128


def _fill_order(ref, back):
    size = ref.shape[0]
    chunks = size // LANES
    step = 64
    for r in range(0, size, step):
        row = lax.broadcasted_iota(jnp.int32, (step, size), 0) + r
        column = lax.broadcasted_iota(jnp.int32, (step, size), 1)
        natural, mixed = (column, row) if back else (row, column)
        hit = natural == chunks * (mixed % LANES) + mixed // LANES
        ref[r:r + step, :] = jnp.where(hit, 1.0, 0.0).astype(jnp.bfloat16)


def _reorder(v, order):
    rows = v.shape[0]
    high = v.astype(jnp.bfloat16)
    rest = (v - high.astype(jnp.float32)).astype(jnp.bfloat16)
    both = jnp.dot(jnp.concatenate([high, rest], axis=0), order[...], preferred_element_type=jnp.float32)
    return both[:rows] + both[rows:]


def _spread(scratch, u, natural):
    count = len(natural)
    chunks = natural[0].shape[1] // LANES
    for t, v in enumerate(natural):
        for c in range(chunks):
            scratch[u, c, t * TILE:(t + 1) * TILE, :] = v[:, c * LANES:(c + 1) * LANES]
    return [jnp.concatenate([scratch[u, c, pl.ds(i, TILE, count), :] for c in range(chunks)], axis=1)
            for i in range(count)]


def _collect(scratch, u, tiles, keep):
    count = len(tiles)
    chunks = tiles[0].shape[1] // LANES
    for i, v in enumerate(tiles):
        for c in range(chunks):
            scratch[u, c, pl.ds(i, TILE, count), :] = v[:, c * LANES:(c + 1) * LANES]
    return [jnp.concatenate([scratch[u, c, t * TILE:(t + 1) * TILE, :] for c in range(chunks)], axis=1) for t in keep]


def _border(count, width, *rows):
    return {at % count: jnp.where(_sub((TILE, width)) == at // count, factor, jnp.float32(1.0)) for at, factor in rows}


def _taper(kind):
    rate = 0.2 * (kind + 1.0)
    near = jnp.exp(-rate)
    far = jnp.exp(-4.0 * rate)
    inv = 1.0 / (far + near + 1.0 + near + far)
    return inv, near * inv, far * inv


def _halves(a, b):
    return jnp.where(_sub(a.shape) < PATCH_ROWS, a, b)


def _widen(v, width):
    return jnp.concatenate([v] * (width // v.shape[1]), axis=1)


def _prep_kernel(taper_in, state, forcing, head, tail, taper, sems, *, per, tiles):
    last = tiles - 1
    first = pltpu.make_async_copy(taper_in, taper, sems.at[4])
    copies = [
        pltpu.make_async_copy(state.at[:, 0], head.at[pl.ds(0, per)], sems.at[0]),
        pltpu.make_async_copy(state.at[:, last], tail.at[pl.ds(0, per)], sems.at[1]),
        pltpu.make_async_copy(forcing.at[0], head.at[per], sems.at[2]),
        pltpu.make_async_copy(forcing.at[last], tail.at[per], sems.at[3]),
    ]
    for c in [first] + copies:
        c.start()
    first.wait()
    width = head.shape[2]
    for r in range(TILE):
        for out, t in ((head, 0), (tail, last)):
            value = taper[t * TILE + r].astype(jnp.float32)
            out[per + 1, r:r + 1, :] = jnp.full((1, width), value, jnp.float32)
    for c in copies:
        c.wait()


def _order_kernel(info, taper, state, forcing, parents, out, order, back, kinds, ends, own, drive, local, sems, *, mix):
    per, tiles, _, width = out.shape
    steps = per // mix

    def load(k):
        return pltpu.make_async_copy(state.at[pl.ds(k * mix, mix)], local.at[pl.ds(k * mix, mix)], sems.at[k])

    for k in range(steps):
        load(k).start()
    for t in range(tiles):
        for r in range(TILE):
            value = taper[t * TILE + r].astype(jnp.float32)
            kinds[t, r:r + 1, :] = jnp.full((1, kinds.shape[2]), value, jnp.float32)
    p = parents[...]
    count = p.shape[1]
    owner = p // per
    inside = p - owner * per
    mine = owner == info[0]
    lo = jnp.where(mine, inside, per - 1)
    hi = jnp.where(mine, inside, 0)
    shift = 1
    while shift < per:
        lo = jnp.minimum(lo, pltpu.roll(lo, count - shift, 1))
        hi = jnp.maximum(hi, pltpu.roll(hi, count - shift, 1))
        shift *= 2
    patches = p.shape[0]
    for slot, v in enumerate((lo, hi)):
        ends[slot] = v
    lane = lax.broadcasted_iota(jnp.int32, p.shape, 1) % per
    rank = jnp.zeros_like(p)
    for shift in range(1, per):
        other = jnp.where(lane + shift < per, pltpu.roll(p, count - shift, 1), pltpu.roll(p, per - shift, 1))
        rank = jnp.where((other // per == owner) & (other < p), 1, rank)
    turn = (count - info[0] * per) % count
    own[pl.ds(0, patches), :] = pltpu.roll(owner * CAP + rank, turn, 1)[:, :LANES]
    own[pl.ds(patches, TILE), :] = jnp.full((TILE, LANES), info[1], jnp.int32)
    _fill_order(order, False)
    _fill_order(back, True)
    v = _reorder(jnp.concatenate([forcing[t] for t in range(tiles)], axis=0) * SCALE, order)
    for t in range(tiles):
        drive[t] = v[t * TILE:(t + 1) * TILE]

    def body(k, carry):
        load(k).wait()
        v = jnp.concatenate([local[k * mix + u, t] for u in range(mix) for t in range(tiles)], axis=0) * SCALE
        v = _reorder(v, order)
        for u in range(mix):
            for t in range(tiles):
                at = (u * tiles + t) * TILE
                out[k * mix + u, t] = v[at:at + TILE]
        return carry

    lax.fori_loop(0, steps, body, 0)


def _advance_kernel(info, ends, state, low_in, high_in, drive, kinds, order, out, natural, every, field, low, high,
                    scaled, work, table, sem, *, mix, groups, bands):
    per, tiles = state.shape[0], state.shape[1]
    count = tiles + 2
    rows = tiles * TILE
    width = state.shape[3]
    fetch = pltpu.make_async_copy(ends, table, sem.at[0])
    fetch.start()
    v = _reorder(jnp.concatenate([low_in[per], high_in[per]], axis=0) * SCALE, order)
    natural[0] = v[:TILE]
    natural[count - 1] = v[TILE:]
    every[0] = low_in[per + 1, :, :LANES]
    every[count - 1] = high_in[per + 1, :, :LANES]
    for t in range(tiles):
        natural[t + 1] = drive[t]
        every[t + 1] = kinds[t]

    v = _reorder(jnp.concatenate([low_in[j] for j in range(per)] + [high_in[j] for j in range(per)], axis=0) * SCALE, order)
    for j in range(per):
        low[j] = v[j * TILE:(j + 1) * TILE]
        high[j] = v[(per + j) * TILE:(per + j + 1) * TILE]
    for t, v in enumerate(_spread(work, 0, [natural[t] for t in range(count)])):
        scaled[t] = v
    mask = _masks(info[1], bands)

    def whole(k, carry):
        masks = _border(count, width, (TILE - 1, mask[0]), (TILE + rows, mask[1]))
        at = [k * mix + u for u in range(mix)]
        cur = [_spread(work, u, [low[j]] + [state[j, t] for t in range(tiles)] + [high[j]]) for u, j in enumerate(at)]
        res = _steps(cur, lambda t: scaled[t], masks)
        keep = range(1, count - 1)
        for u, j in enumerate(at):
            for t, v in zip(keep, _collect(work, u, res[u], keep)):
                field[j, t - 1] = v
        return carry

    lax.fori_loop(0, per // mix, whole, 0)
    fetch.wait()

    def pack(g, carry):
        for q in range(tiles):
            for slot in range(CAP):
                first = table[slot, 2 * q, g * per]
                second = table[slot, 2 * q + 1, g * per]
                out[g, slot, q] = _halves(field[first, q], field[second, q])
        return carry

    lax.fori_loop(0, groups, pack, 0)


def _masks(band, bands):
    one = jnp.float32(1.0)
    zero = jnp.float32(0.0)
    return [jnp.where(band > 0, one, zero), jnp.where(band < bands - 1, one, zero)]


def _choose(slots, incoming, column, q):
    a = incoming[slots[2 * q, column], q]
    b = incoming[slots[2 * q + 1, column], q]
    return _halves(a, b)


def _pick_kernel(slots, incoming, first, final):
    per, tiles = first.shape[0], incoming.shape[1]

    def body(j, carry):
        first[j] = _choose(slots, incoming, j, 0)
        final[j] = _choose(slots, incoming, j, tiles - 1)
        return carry

    lax.fori_loop(0, per, body, 0)


def _spread_kinds(scratch, kinds, taper):
    for t, v in enumerate(_spread(scratch, 0, kinds)):
        for c, part in enumerate(_taper(v)):
            taper[c, t] = part


def _natural(pend, hold, order):
    mix, count = pend.shape[1], pend.shape[2]
    v = jnp.concatenate([pend[hold, u, t] for u in range(mix) for t in range(count)], axis=0)
    v = _reorder(v, order) * (1.0 / SCALE)
    return [[v[(u * count + t) * TILE:(u * count + t + 1) * TILE] for t in range(count)] for u in range(mix)]


def _pipeline(steps, mix, compute, pend, order, done, copy=None, beside=None):
    def flush(k):
        for u, column in enumerate(_natural(pend, k % 2, order)):
            for t, v in enumerate(column):
                done[k * mix + u, t] = v

    def first(k):
        for u, column in enumerate(compute(k)):
            for t, v in enumerate(column):
                pend[k % 2, u, t] = v

    first(0)
    if beside:
        beside()

    def body(k, carry):
        flush(k - 1)
        first(k)
        if copy:
            copy(k - 1).start()
        return carry

    lax.fori_loop(1, steps, body, 0)
    flush(steps - 1)
    if copy:
        copy(steps - 1).start()
        for k in range(steps):
            copy(k).wait()


def _final_inner_kernel(slots, incoming, natural, every, order, done, pend, scaled, taper, work, *, half, mix):
    tiles, width = natural.shape[0] - 2, natural.shape[2]
    for t, v in enumerate(_spread(work, 0, [natural[t + 1] for t in range(tiles)])):
        scaled[t] = v
    _spread_kinds(work, [every[t + 1] for t in range(tiles)], taper)

    def weights(t):
        return [_widen(taper[c, t], width) for c in range(3)]

    def compute(k):
        cur = []
        for u in range(mix):
            mine = _spread(work, u, [_choose(slots, incoming, k * mix + u, t) for t in range(tiles)])
            cur.append(_blend(mine, weights, {}))
        res = _steps(cur, lambda t: scaled[t], {})
        return [_collect(work, u, res[u], range(1, tiles - 1)) for u in range(mix)]

    _pipeline(half // mix, mix, compute, pend, order, done)


def _final_rest_kernel(slots, incoming, first, final, below, above, natural, every, order, prior, out,
                       edges, done, pend, scaled, taper, ends, taper3, work, sems, *, per, half, mix, edge_mix, bands):
    count, width = natural.shape[0], natural.shape[2]
    tiles = count - 2
    last = tiles - 1
    rows = tiles * TILE
    for s in range(2):
        for t, v in enumerate(_spread(work, s, [natural[last * s + t] for t in range(3)])):
            ends[s, t] = v
        _spread_kinds(work, [every[last * s + t] for t in range(3)], taper3.at[s])
    for t, v in enumerate(_spread(work, 2, [natural[t] for t in range(count)])):
        scaled[t] = v
    _spread_kinds(work, [every[t] for t in range(count)], taper)
    mask = _masks(slots[slots.shape[0] - 1, 0], bands)
    steps = (per - half) // mix

    def finish(s):
        return pltpu.make_async_copy(edges.at[s], out.at[pl.ds(0, half), last * s], sems.at[steps + s])

    inner_rows = pltpu.make_async_copy(prior, out.at[pl.ds(0, half), pl.ds(1, tiles - 2)], sems.at[steps + 2])
    inner_rows.start()

    def edge(k, carry):
        for s in range(2):
            mask3 = _border(3, width, (TILE - 1, mask[0]) if s == 0 else (2 * TILE, mask[1]))
            cur = []
            for u in range(edge_mix):
                j = k * edge_mix + u
                inner = _choose(slots, incoming, j, 1 if s == 0 else last - 1)
                three = [below[j], first[j], inner] if s == 0 else [inner, final[j], above[j]]
                cur.append(_blend(_spread(work, u, three),
                                  lambda t: [_widen(taper3[s, c, t], width) for c in range(3)], mask3))
            res = _steps(cur, lambda t: ends[s, t], mask3)
            for u in range(edge_mix):
                edges[s, k * edge_mix + u] = _collect(work, u, res[u], [1])[0]
        return carry

    lax.fori_loop(0, half // edge_mix, edge, 0)

    def edge_rows():
        v = jnp.concatenate([edges[s, j] for s in range(2) for j in range(half)], axis=0)
        v = _reorder(v, order) * (1.0 / SCALE)
        for s in range(2):
            for j in range(half):
                at = (s * half + j) * TILE
                edges[s, j] = v[at:at + TILE]
        for s in range(2):
            finish(s).start()

    def copy(k):
        return pltpu.make_async_copy(
            done.at[pl.ds(k * mix, mix)], out.at[pl.ds(half + k * mix, mix)], sems.at[k])

    def compute(k):
        masks = _border(count, width, (TILE - 1, mask[0]), (TILE + rows, mask[1]))
        cur = []
        for u in range(mix):
            j = half + k * mix + u
            mine = [below[j], first[j]]
            mine += [_choose(slots, incoming, j, t) for t in range(1, last)]
            mine += [final[j], above[j]]
            cur.append(_blend(_spread(work, u, mine), lambda t: [_widen(taper[c, t], width) for c in range(3)],
                              masks))
        res = _steps(cur, lambda t: scaled[t], masks)
        return [_collect(work, u, res[u], range(1, count - 1)) for u in range(mix)]

    _pipeline(steps, mix, compute, pend, order, done, copy, edge_rows)
    for s in range(2):
        finish(s).wait()
    inner_rows.wait()


def _pin(x):
    return pltpu.with_memory_space_constraint(x, pltpu.HBM)


def _call(kernel, name, outs, scratch, spaces, out_spaces, alias=None):
    def spec(kind):
        return pl.BlockSpec(memory_space={"v": pltpu.VMEM, "s": pltpu.SMEM, "a": pl.ANY, "h": pltpu.HBM}[kind])

    specs = [spec(k) for k in out_spaces]
    single = len(outs) == 1
    return pl.pallas_call(
        kernel,
        in_specs=[spec(k) for k in spaces],
        out_specs=specs[0] if single else specs,
        out_shape=outs[0] if single else outs,
        scratch_shapes=scratch,
        input_output_aliases=alias or {},
        compiler_params=pltpu.CompilerParams(vmem_limit_bytes=40 * 1024 * 1024),
        name=name,
    )


def on_device(state, forcing, parents, taper_index):
    per, rows, width = state.shape
    tiles = rows // TILE
    groups = lax.axis_size("pgroup")
    bands = lax.axis_size("band")
    f32 = jnp.float32
    forward = [(i, i + 1) for i in range(bands - 1)]
    backward = [(b, a) for a, b in forward]
    info = jnp.stack([lax.axis_index("pgroup"), lax.axis_index("band")]).astype(jnp.int32)
    state4 = state.reshape(per, tiles, TILE, width)
    pinned = _pin(state4)
    drive = forcing.reshape(tiles, TILE, width)
    entries = groups * CAP
    dma = pltpu.SemaphoreType.DMA
    vmem = pltpu.VMEM

    def shape(*dims, dtype=f32):
        return jax.ShapeDtypeStruct(dims, dtype)

    patches, count = parents.shape
    i32 = jnp.int32
    head, tail = _call(
        functools.partial(_prep_kernel, per=per, tiles=tiles), "prepare",
        [shape(per + 2, TILE, width), shape(per + 2, TILE, width)],
        [pltpu.SMEM((rows,), i32), dma((5,))], "hhh", "vv",
    )(_pin(taper_index), pinned, _pin(drive))
    low = lax.ppermute(tail, "band", forward)
    high = lax.ppermute(head, "band", backward)

    half = per // 2

    def work(count, height):
        return vmem((count, width // LANES, height * TILE, LANES), f32)

    extra = [vmem((tiles + 2, TILE, width), f32), vmem((2, 3, TILE, width), f32)]
    square = shape(width, width, dtype=jnp.bfloat16)
    state4, order, back, kinds, ends, own, drive = _call(
        functools.partial(_order_kernel, mix=4), "reorder",
        [shape(per, tiles, TILE, width), square, square, shape(tiles, TILE, LANES),
         shape(CAP, patches, count, dtype=i32), shape(patches + TILE, LANES, dtype=i32),
         shape(tiles, TILE, width)],
        [vmem((per, tiles, TILE, width), f32), dma((per // 4,))], "sshvv", "v" * 7,
    )(info, taper_index, pinned, drive, parents)
    message, natural, every = _call(
        functools.partial(_advance_kernel, mix=2, groups=groups, bands=bands), "advance",
        [shape(groups, CAP, tiles, TILE, width), shape(tiles + 2, TILE, width), shape(tiles + 2, TILE, LANES)],
        [vmem((per, tiles, TILE, width), f32), vmem((per + 1, TILE, width), f32), vmem((per + 1, TILE, width), f32),
         extra[0], work(2, tiles + 2), pltpu.SMEM((CAP, patches, count), i32), dma((1,))], "svvvvvvv", "vvv",
    )(info, ends, state4, low, high, drive, kinds, order)

    incoming = lax.all_to_all(message, "pgroup", split_axis=0, concat_axis=0, tiled=True)
    incoming = incoming.reshape(entries, tiles, TILE, width)

    first, final = _call(
        _pick_kernel, "pick_edge", [shape(per, TILE, width), shape(per, TILE, width)], [], "sv", "vv",
    )(own, incoming)
    below = lax.ppermute(final, "band", forward)
    above = lax.ppermute(first, "band", backward)

    pairs = half // 2
    middle = _call(
        functools.partial(_final_inner_kernel, half=half, mix=2), "final_inner", [shape(half, tiles - 2, TILE, width)],
        [vmem((2, 2, tiles - 2, TILE, width), f32), vmem((tiles, TILE, width), f32),
         vmem((3, tiles, TILE, LANES), f32), work(2, tiles)], "svvvv", "v",
    )(own, incoming, natural, every, back)
    field = _call(
        functools.partial(_final_rest_kernel, per=per, half=half, mix=2, edge_mix=4, bands=bands), "final_rest",
        [shape(per, tiles, TILE, width)],
        [vmem((2, half, TILE, width), f32), vmem((per - half, tiles, TILE, width), f32),
         vmem((2, 2, tiles, TILE, width), f32), extra[0], vmem((3, tiles + 2, TILE, LANES), f32), extra[1],
         vmem((2, 3, 3, TILE, LANES), f32), work(4, tiles + 2), dma((pairs + 3,))],
        "svvvvvvvvv", "a",
    )(own, incoming, first, final, below, above, natural, every, back, middle)
    return field.reshape(per, rows, width)


def solution(mesh):
    return jax.shard_map(
        on_device,
        mesh=mesh,
        in_specs=(P("pgroup", "band", None), P("band", None), P("band", None), P("band")),
        out_specs=P("pgroup", "band", None),
        check_vma=False,
    )
```
